32 devices in a mesh: grp: 4 (over y, x), sub: 8 (over z, core).
Axes of the slice: x: 2, y: 2, z: 4, core: 2. Of those that a mesh axis runs over, the one named last changes fastest.
Arguments:
- initial_field: float32 [4, 16, 16384], P('grp', 'sub'), may hold values from -6 to 6
- conduct: float32 [4, 16, 16384], P('grp', 'sub'), may hold values from 0.02 to 0.12
- velocity: float32 [4, 16, 16384], P('grp', 'sub'), may hold values from 0 to 0.25
- heat_release: float32 [4, 16, 16384], P('grp', 'sub'), may hold values from 0.01 to 0.1
- group_kind: int32 [4], replicated, may hold values from 0 to 1, as said below
- partner: int32 [4], replicated, may hold values from 0 to 3, as said below
- surface_cell: int32 [4, 4096], P('grp', 'sub'), may hold values from 0 to 32767
- patch_count: int32 [4, 8], P('grp'), may hold values from 1 to 24, 64 in all within a row
- patch_centres: int32 [4, 192, 128], P('grp', 'sub'), may hold values from 0 to 4095, as said below
- patch_targets: int32 [4, 192, 128], P('grp', 'sub'), may hold values from 0 to 4095
- patch_maps: float32 [4, 192, 128, 128], P('grp', 'sub'), may hold values from -0.25 to 0.95
Outputs:
- temperature: float32 [4, 16, 16384], P('grp', 'sub')
- interface: float32 [4, 2, 4096], P('grp', None, 'sub')
The draws below stay inside these ranges and needn't reach their ends.
Inputs may be any that keep to these rules, and one draw needn't show every extreme that they name: `group_kind`: both kinds occur. partner[g] is a group of the other kind than g. Slots 0 to patch_count[g, j] - 1 of device j of group g are live; each group's counts sum to 64; in each group some device holds 24. `patch_centres`: the centres of slot s of group g lie in the cyclic window of 1024 consecutive nodes that starts at (s // 24) * 512 - 512 // 2 + h[g], for one shift h[g] of each group.
All inputs are finite; a program needn't handle non-finite values.
Results may differ from the reference program's by a relative error of at most 0.00013.
Values sent between devices are 32-bit elements; how exact they have to be, the bound alone decides.
A program may use at most 64 MiB of HBM per device.

```python
import math
import jax
import jax.numpy as jnp
import numpy as np
from jax import lax

PLANES = 2
CELLS = 16384
SURF_DEV = 512
PATCH = 128
STEPS = 4
COUPLE = 4
GROUPS = 4
STACK = 16
NODES = 4096
CAP = 24
SLOTS = 192
PATCH_ROW = 64
N_SUB = 8


def kinds_partners(key):
    base_key = jax.random.fold_in(key, 17)
    order_key, count_key, score_key = jax.random.split(base_key, 3)
    shuffled = jax.random.permutation(order_key, GROUPS)
    gas_count = jax.random.randint(count_key, (), 1, GROUPS)
    position = jnp.argsort(shuffled, stable=True)
    kinds = (position >= gas_count).astype(jnp.int32)
    scores = jax.random.randint(score_key, (GROUPS, GROUPS), 0, 1000) * GROUPS + jnp.arange(GROUPS)[None, :]
    scores = scores + (kinds[:, None] == kinds[None, :]).astype(jnp.int32) * 1000000
    partners = jnp.argsort(scores, axis=1, stable=True)[:, 0].astype(jnp.int32)
    return (kinds, partners)


def draw_group_kind(key, part):
    return kinds_partners(key)[0]


def draw_partner(key, part):
    return kinds_partners(key)[1]


def window_nodes(key, group_shift):
    owner = (jnp.arange(SLOTS, dtype=jnp.int32) // CAP)[None, :, None]
    start = owner * SURF_DEV - SURF_DEV // 2 + group_shift[:, None, None]
    offset = jax.random.randint(key, (GROUPS, SLOTS, PATCH), 0, 2 * SURF_DEV)
    return ((start + offset) % NODES).astype(jnp.int32)


def draw_patch_targets(key, part):
    target_key = jax.random.fold_in(key, 31)
    return jax.random.randint(target_key, (GROUPS, SLOTS, PATCH), 0, NODES).astype(jnp.int32)


def draw_patch_centres(key, part):
    centre_key = jax.random.fold_in(key, 47)
    shift_key, node_key = jax.random.split(centre_key)
    group_shift = jax.random.randint(shift_key, (GROUPS,), 0, NODES)
    return window_nodes(node_key, group_shift)


def draw_patch_maps(key, part):
    off_key, diag_key = jax.random.split(key)
    full_shape = (GROUPS, SLOTS, PATCH, PATCH)
    spread = jax.random.normal(off_key, full_shape, jnp.float32) * (0.5 / math.sqrt(PATCH))
    spread = jnp.clip(spread, -0.25, 0.25)
    diagonal = jax.random.uniform(diag_key, (GROUPS, SLOTS, PATCH), jnp.float32, 0.3, 0.7)
    return spread + diagonal[..., None] * jnp.eye(PATCH, dtype=jnp.float32)


def set_ends(result, own_key, low, top_value):
    longest = result.shape.index(max(result.shape))
    spots = []
    for shift in (0, 1):
        where = [jax.random.randint(jax.random.fold_in(own_key, axis), (), 0, length) for axis, length in enumerate(result.shape)]
        where[longest] = (where[longest] + shift) % result.shape[longest]
        spots.append(tuple(where))
    return result.at[spots[0]].set(low).at[spots[1]].set(top_value)


def steps_of(key, dims, cuts, low, high):
    loudness, own = 1.0, jax.random.fold_in(key, 6)
    for axis_at, shards_of in cuts:
        steps = jnp.exp(jax.random.uniform(jax.random.fold_in(own, axis_at), (shards_of,), jnp.float32, low / len(cuts), high / len(cuts)))
        loudness = loudness * jnp.repeat(steps, dims[axis_at] // shards_of).reshape([-1 if axis == axis_at else 1 for axis in range(len(dims))])
    return loudness


def length_profile(number_of, total, most, lean):
    weights = [(1 << 20) // math.isqrt(standing ** lean) + 1 for standing in range(2, number_of + 1)]
    spare, holding = total - most - (number_of - 1), [1] * (number_of - 1)
    while spare > 0:
        candidates = [i for i in range(number_of - 1) if holding[i] < most]
        whole, left = sum([weights[i] for i in candidates]), spare
        for i in candidates:
            addition = min(most - holding[i], max(1, left * weights[i] // whole), spare)
            holding[i] = holding[i] + addition
            spare = spare - addition
    return np.array([most] + holding)


def ragged(own_key, count, total, limit, slope):
    if count == 2:
        one = jax.random.randint(own_key, (), max(1, total - limit), min(limit, total - 1) + 1)
        return jnp.stack([one, total - one])
    sizes = jnp.asarray(length_profile(count, total, limit, slope), jnp.int32)
    pairs = (count - 1) // 2
    source_of, sink = sizes[1:1 + 2 * pairs:2], sizes[2:2 + 2 * pairs:2]
    room = jnp.minimum(source_of - 1, limit - sink)
    moved = jax.random.randint(jax.random.fold_in(own_key, 1), (pairs,), 0, 1 << 20) % (room + 1)
    sizes = sizes.at[1:1 + 2 * pairs:2].set(source_of - moved).at[2:2 + 2 * pairs:2].set(sink + moved)
    return sizes[jax.random.permutation(jax.random.fold_in(own_key, 2), count)]


def scatter_about(own_key, dims, deviation, reach, pieces=(), kind=jnp.bfloat16):
    result = deviation * jax.random.normal(own_key, dims, jnp.float32)
    if pieces:
        result = result * steps_of(own_key, dims, pieces, -0.22, 0.18)
    return jnp.clip(result, -reach, reach).astype(kind)


def setup_inputs(seed: int = 0) -> dict:
    key_list = jax.random.split(jax.random.key(seed), 12)
    initial_field = scatter_about(key_list[0], (GROUPS, STACK, CELLS), 1.0, 6.0, ((0, 4), (1, 8)), jnp.float32)
    conduct = jnp.clip(jnp.exp(math.log(0.12) - 1.7917595 * jax.random.uniform(key_list[1], (GROUPS, STACK, CELLS), jnp.float32) ** steps_of(key_list[1], (GROUPS, STACK, CELLS), ((0, 4), (1, 8)), -0.2, 0.2)), 0.02, 0.12)
    velocity = jnp.clip(0.25 * jax.random.uniform(key_list[2], (GROUPS, STACK, CELLS), jnp.float32) ** steps_of(key_list[2], (GROUPS, STACK, CELLS), ((0, 4), (1, 8)), -0.2, 0.2), 0.0, 0.25)
    heat_release = jnp.clip(jnp.exp(math.log(0.1) - 2.3025851 * jax.random.uniform(key_list[3], (GROUPS, STACK, CELLS), jnp.float32) ** steps_of(key_list[3], (GROUPS, STACK, CELLS), ((0, 4), (1, 8)), -0.2, 0.2)), 0.01, 0.1)
    group_kind = draw_group_kind(jax.random.fold_in(key_list[11], 71), 0)
    partner = draw_partner(jax.random.fold_in(key_list[11], 71), 0)
    surface_cell = set_ends(jax.random.randint(key_list[6], (GROUPS, NODES), 0, PLANES * CELLS), jax.random.fold_in(key_list[6], 1), 0, (PLANES * CELLS) - 1).astype(jnp.int32)
    patch_count = jax.vmap(lambda own: ragged(own, N_SUB, PATCH_ROW, CAP, 2))(jax.random.split(key_list[7], GROUPS)).reshape((GROUPS, N_SUB)).astype(jnp.int32)
    patch_centres = draw_patch_centres(jax.random.fold_in(key_list[11], 71), 0)
    patch_targets = draw_patch_targets(jax.random.fold_in(key_list[11], 71), 0)
    patch_maps = draw_patch_maps(jax.random.fold_in(key_list[11], 71), 0)
    return dict(initial_field=initial_field, conduct=conduct, velocity=velocity, heat_release=heat_release, group_kind=group_kind, partner=partner, surface_cell=surface_cell, patch_count=patch_count, patch_centres=patch_centres, patch_targets=patch_targets, patch_maps=patch_maps)


def in_plane(current):
    return (jnp.roll(current, 1, -2) + jnp.roll(current, -1, -2)
            + jnp.roll(current, 1, -1) + jnp.roll(current, -1, -1))


def advance(current, conduct, velocity, heat_release, gas_mask):
    zero_plane = jnp.zeros_like(current[:, :1])
    upper_plane = jnp.concatenate([current[:, 1:], zero_plane], axis=1)
    lower_plane = jnp.concatenate([zero_plane, current[:, :-1]], axis=1)
    laplace = upper_plane + lower_plane + in_plane(current) - 6.0 * current
    return (current + conduct * laplace - gas_mask * velocity * (current - lower_plane)
            + gas_mask * heat_release * jax.nn.sigmoid(2.0 * current))


def reference(initial_field, conduct, velocity, heat_release, group_kind, partner, surface_cell,
              patch_count, patch_centres, patch_targets, patch_maps):
    groups = initial_field.shape[0]
    slab_shape = (groups, N_SUB * PLANES, CELLS // 128, 128)
    current = initial_field.reshape(slab_shape)
    conduct_slab = conduct.reshape(slab_shape)
    velocity_slab = velocity.reshape(slab_shape)
    heat_slab = heat_release.reshape(slab_shape)
    gas_mask = (group_kind == 0).astype(jnp.float32)[:, None, None, None]
    gain_temp = jnp.where(group_kind == 0, 0.5, 0.25).astype(jnp.float32)[:, None]
    gain_flux = jnp.where(group_kind == 0, -0.25, 0.25).astype(jnp.float32)[:, None]
    node_ids = jnp.arange(N_SUB * SURF_DEV, dtype=jnp.int32)
    cell_ids = (node_ids // SURF_DEV)[None, :] * (PLANES * CELLS) + surface_cell
    slot_ids = jnp.arange(N_SUB * CAP, dtype=jnp.int32)
    live_mask = ((slot_ids % CAP)[None, :] < patch_count[:, slot_ids // CAP]).astype(jnp.float32)
    group_ids = jnp.arange(groups, dtype=jnp.int32)[:, None]
    interface = jnp.zeros((groups, 2, N_SUB * SURF_DEV), jnp.float32)
    for iteration in range(COUPLE):
        for substep in range(STEPS):
            current = advance(current, conduct_slab, velocity_slab, heat_slab, gas_mask)
        flux_field = conduct_slab * (4.0 * current - in_plane(current))
        flat_temp = current.reshape(groups, -1)
        flat_flux = flux_field.reshape(groups, -1)
        export = jnp.stack([jnp.take_along_axis(flat_temp, cell_ids, 1),
                            jnp.take_along_axis(flat_flux, cell_ids, 1)], axis=1)
        source = export[partner]
        row_sums = []
        for group in range(groups):
            centre_vals = source[group][:, patch_centres[group]]
            contrib = jnp.einsum("stk,qsk->qst", patch_maps[group], centre_vals,
                                 precision=lax.Precision.HIGHEST) * live_mask[group][None, :, None]
            row_sum = jnp.zeros((2, N_SUB * SURF_DEV), jnp.float32).at[:, patch_targets[group]].add(contrib)
            row_sums.append(row_sum)
        interface = jnp.stack(row_sums)
        increment = gain_temp * (interface[:, 0] - export[:, 0]) + gain_flux * interface[:, 1]
        flat_temp = flat_temp.at[group_ids, cell_ids].add(increment)
        current = flat_temp.reshape(slab_shape)
    return current.reshape(initial_field.shape), interface
```

```python
import jax
import jax.numpy as jnp
from jax import lax
from jax.experimental import pallas as pl
from jax.experimental.pallas import tpu as pltpu
from jax.sharding import PartitionSpec as P

STEPS = 4
COUPLE = 4
LANES = 128
F32 = jnp.float32
BF16 = jnp.bfloat16


def split(x):
    hi = x.astype(BF16).astype(F32)
    return hi, x - hi


def dot_nt(a, b):
    return lax.dot_general(a, b, (((1,), (1,)), ((), ())), preferred_element_type=F32)


def dot_nn(a, b):
    return lax.dot_general(a, b, (((1,), (0,)), ((), ())), preferred_element_type=F32)


def iota(shape, dim):
    return lax.broadcasted_iota(jnp.int32, shape, dim)


def in_plane(c):
    rows, cols = c.shape
    return (
        pltpu.roll(c, 1, 0)
        + pltpu.roll(c, rows - 1, 0)
        + pltpu.roll(c, 1, 1)
        + pltpu.roll(c, cols - 1, 1)
    )


def kernel(
    n,
    groups,
    kind_ref,
    partner_ref,
    count_ref,
    field_ref,
    cond_ref,
    vel_ref,
    heat_ref,
    surf_ref,
    cent_ref,
    targ_ref,
    maps_ref,
    out_ref,
    iface_ref,
    fa,
    fb,
    cx,
    vx,
    hx,
    land,
    surf_all,
    oh_surf,
    hot_surf,
    oh_lane,
    oh_cent,
    oh_targ,
    hot_targ,
    maps2,
    exp_one,
    exp_two,
    own_temp,
    land_one,
    land_two,
    part_one,
    part_two,
    rs_one,
    rs_two,
    set_send,
    set_recv,
    ex_send,
    ex_recv,
    rs_send,
    rs_recv,
    halo_send,
    halo_recv,
    maps,
    load_sem,
):
    planes = field_ref.shape[1]
    rows = fa.shape[1]
    near = STEPS // 2
    assert near % 2 == 0 and near <= planes
    surf_here = surf_ref.shape[1]
    cap = cent_ref.shape[0]
    reach = -(-STEPS // planes)
    depth = reach * planes
    ext = planes + 2 * depth
    offs = [d for d in range(-reach, reach + 1) if d != 0]
    at = {d: i for i, d in enumerate(offs)}
    half = surf_here // LANES
    span = 2 * reach + 1
    blocks = n * half
    me = lax.axis_index("sub")
    grp = lax.axis_index("grp")

    def there(d):
        return jnp.logical_and(me + d >= 0, me + d < n)

    def rcopy(src, dst, ss, rs, dev):
        return pltpu.make_async_remote_copy(
            src_ref=src,
            dst_ref=dst,
            send_sem=ss,
            recv_sem=rs,
            device_id=dev,
            device_id_type=pl.DeviceIdType.MESH,
        )

    load = pltpu.make_async_copy(maps_ref, maps, load_sem)
    load.start()

    for buf in (fa, cx, vx, hx):
        buf[...] = jnp.zeros(buf.shape, F32)
    land[...] = jnp.zeros(land.shape, F32)
    part_one[...] = jnp.zeros(part_one.shape, F32)
    surf_all[...] = jnp.zeros(surf_all.shape, jnp.int32)

    barrier = pltpu.get_barrier_semaphore()
    for k in range(1, n):
        pl.semaphore_signal(
            barrier, inc=1, device_id={"sub": lax.rem(me + k, n)}, device_id_type=pl.DeviceIdType.MESH
        )
    for k in range(1, groups):
        for j in range(n):
            pl.semaphore_signal(
                barrier,
                inc=1,
                device_id={"grp": lax.rem(grp + k, groups), "sub": lax.rem(me + j, n)},
                device_id_type=pl.DeviceIdType.MESH,
            )

    own = pl.ds(depth, planes)
    kind = kind_ref[grp]
    gas = jnp.where(kind == 0, 1.0, 0.0).astype(F32)
    gain_t = jnp.where(kind == 0, 0.5, 0.25).astype(F32)
    gain_f = jnp.where(kind == 0, -0.25, 0.25).astype(F32)
    away_t = jnp.where(kind == 0, 0.25, 0.5).astype(F32)
    away_f = jnp.where(kind == 0, 0.25, -0.25).astype(F32)
    fetch = ((field_ref, fa, None), (cond_ref, cx, None), (vel_ref, vx, gas), (heat_ref, hx, 0.5 * gas))

    def unfold(b, carry):
        chunk = pl.ds(pl.multiple_of(b * 8 * LANES, LANES), 8 * LANES)
        for src, dst, scale in fetch:
            x = src[0, :, chunk]
            if scale is not None:
                x = x * scale
            for p in range(planes):
                dst[depth + p, pl.ds(pl.multiple_of(b * 8, 8), 8), :] = jnp.concatenate(
                    [x[p : p + 1, i * LANES : (i + 1) * LANES] for i in range(8)], axis=0
                )
        return carry

    lax.fori_loop(0, rows // 8, unfold, 0)
    pl.semaphore_wait(barrier, n * groups - 1)

    def send_planes(buf, lo, hi, to, j):
        slot = -to
        shift = depth - (depth + planes * slot)
        return rcopy(
            buf.at[pl.ds(lo + shift, hi - lo)],
            buf.at[pl.ds(lo, hi - lo)],
            set_send.at[j, at[to]],
            set_recv.at[j, at[slot]],
            {"sub": me + to},
        )

    def first_copies(to):
        base = depth - planes * to
        lo, hi = max(base, depth - near), min(base + planes, depth + planes + near)
        out = [send_planes(fa, lo, hi, to, 0)]
        lo, hi = max(base, depth - near + 1), min(base + planes, depth + planes + near - 1)
        if hi > lo:
            out += [send_planes(buf, lo, hi, to, j + 1) for j, buf in enumerate((cx, vx, hx))]
        return out

    def rest_copies(to, which):
        base = depth - planes * to
        lo, hi = max(base, 1), min(base + planes, ext - 1)
        if to == 1:
            hi = min(hi, depth - near + 1)
        if to == -1:
            lo = max(lo, depth + planes + near - 1)
        if hi <= lo:
            return []
        return [send_planes((cx, vx, hx)[j], lo, hi, to, j + 4) for j in which]

    def surf_copies(to):
        return [
            rcopy(
                surf_ref,
                surf_all.at[reach - to],
                set_send.at[7, at[to]],
                set_recv.at[7, at[-to]],
                {"sub": me + to},
            )
        ]

    def mid_copy(to):
        return rcopy(
            fa.at[own],
            land.at[1, at[-to]],
            set_send.at[8, at[to]],
            set_recv.at[8, at[-to]],
            {"sub": me + to},
        )

    def each(ds, act):
        for d in ds:

            @pl.when(there(d))
            def _():
                act(d)

    def starts(copies):
        for c in copies:
            c.start()

    def arrivals(copies):
        for c in copies:
            c.wait_recv()

    def departures(copies):
        for c in copies:
            c.wait_send()

    beside = (-1, 1)
    each(beside, lambda d: starts(first_copies(d)))

    partner = partner_ref[grp]
    count = count_ref[0, me]
    surf_all[reach] = surf_ref[...]
    block_row = iota((blocks, LANES), 0)
    lane_row = iota((LANES, LANES), 0)

    def hot(mask):
        return jnp.where(mask, 1.0, 0.0).astype(F32)

    load.wait()
    for s in range(cap):
        lanes = pl.ds(s * LANES, LANES)
        oh_cent[:, lanes] = hot(lane_row == cent_ref[s : s + 1, :] % LANES).astype(BF16)
        oh_targ[:, lanes] = hot(block_row == targ_ref[s : s + 1, :] // LANES).astype(BF16)
        hot_targ[lanes, :] = hot(lane_row == targ_ref[s : s + 1, :] % LANES).T.astype(BF16)
        live = jnp.where(s < count, 1.0, 0.0).astype(F32)
        hi, lo = split((maps[s] * live).T)
        maps2[s, :, pl.ds(0, LANES)] = hi.astype(BF16)
        maps2[s, :, pl.ds(LANES, LANES)] = lo.astype(BF16)

    cell_row = iota((planes * rows, surf_here), 0)

    def hot_rows(j):
        oh_surf[j] = hot(cell_row == surf_all[j] // LANES).astype(BF16)
        lane = surf_all[j] % LANES
        for i in range(half):
            cols = slice(i * LANES, (i + 1) * LANES)
            hot_surf[j, cols, :] = hot(lane_row == lane[:, cols]).T.astype(BF16)

    hot_rows(reach)
    own_lane = hot(iota((LANES, surf_here), 0) == surf_all[reach] % LANES).astype(BF16)
    oh_lane[pl.ds(0, LANES)] = own_lane
    oh_lane[pl.ds(LANES, LANES)] = own_lane

    group_of_slots = 4 if cap % 4 == 0 else 1
    width = group_of_slots * LANES
    block_of_chunk = iota((blocks, width), 0)

    def step(src, dst, k):
        for z in range(k + 1, ext - k - 1):
            c = src[z]
            dn = src[z - 1]
            lap = src[z + 1] + dn + in_plane(c) - 6.0 * c
            dst[z] = c + cx[z] * lap - vx[z] * (c - dn) + hx[z] * (1.0 + jnp.tanh(c))

    def spread(slot, inc):
        packed = []
        for x in split(inc):
            wide = [jnp.broadcast_to(x[i : i + 1, :], (16, LANES)).astype(BF16) for i in range(half)]
            packed.append(jnp.concatenate(wide, axis=1))
        out = None
        for x in packed:
            lhs = jnp.concatenate(
                [oh_surf[slot, r * 16 : (r + 1) * 16, :] * x for r in range(planes * rows // 16)], axis=0
            )
            r = dot_nn(lhs, hot_surf[slot])
            out = r if out is None else out + r
        return out.reshape(planes, rows, LANES)

    def halo_copy(par, to, slot):
        return rcopy(
            fa.at[own],
            land.at[par, at[slot]],
            halo_send.at[par, at[to]],
            halo_recv.at[par, at[slot]],
            {"sub": me + to},
        )

    def ex_copy(two, par, k, j, sender):
        src, dst = (exp_two, land_two.at[k - 1, sender]) if two else (exp_one, land_one.at[par, k - 1, sender])
        return rcopy(
            src,
            dst,
            ex_send.at[par, k - 1, j],
            ex_recv.at[par, k - 1, j],
            {"grp": lax.rem(grp + k, groups), "sub": lax.rem(me + j, n)},
        )

    def rs_copy(two, par, k, sender):
        peer = lax.rem(me + k, n)
        if two:
            src, dst = part_two.at[peer], rs_two.at[sender]
        else:
            src, dst = part_one.at[pl.ds(peer, span)], rs_one.at[par, sender]
        return rcopy(src, dst, rs_send.at[par, k - 1], rs_recv.at[par, k - 1], {"sub": peer})

    def sample(values):
        lhs = []
        for x in values:
            hi, lo = split(jnp.concatenate(x, axis=0))
            lhs.append(jnp.concatenate([hi, lo], axis=1).astype(BF16))
        got = dot_nn(jnp.concatenate(lhs, axis=0), oh_lane[...])
        hit = cell_row == surf_all[reach] // LANES
        size = planes * rows
        return [
            jnp.sum(jnp.where(hit, got[q * size : (q + 1) * size], 0.0), axis=0, keepdims=True)
            for q in range(len(values))
        ]

    def patches(srcs):
        count_q = len(srcs)
        lhs = jnp.concatenate([x for v in srcs for x in split(v)], axis=0).astype(BF16)
        acc = None
        for s0 in range(0, cap, group_of_slots):
            lanes = slice(s0 * LANES, s0 * LANES + width)
            slots = range(s0, s0 + group_of_slots)
            cent = jnp.concatenate([cent_ref[s : s + 1, :] for s in slots], axis=1) // LANES
            vals = dot_nn(lhs, oh_cent[:, lanes])
            hit = block_of_chunk == cent
            cv = []
            for q in range(count_q):
                v = vals[2 * q * blocks : (2 * q + 1) * blocks] + vals[(2 * q + 1) * blocks : (2 * q + 2) * blocks]
                cv.append(jnp.sum(jnp.where(hit, v, 0.0), axis=0, keepdims=True))
            c4 = jnp.concatenate([x for v in cv for x in split(v)], axis=0).astype(BF16)
            contrib = []
            for i, s in enumerate(slots):
                r = dot_nn(c4[:, i * LANES : (i + 1) * LANES], maps2[s])
                contrib.append(r[:, :LANES] + r[:, LANES:])
            r = jnp.concatenate(contrib, axis=1)
            rows_of = []
            for q in range(count_q):
                for x in split(r[2 * q : 2 * q + 1] + r[2 * q + 1 : 2 * q + 2]):
                    wide = jnp.broadcast_to(x, (16, width)).astype(BF16)
                    rows_of += [oh_targ[b * 16 : (b + 1) * 16, lanes] * wide for b in range(blocks // 16)]
            r = dot_nn(jnp.concatenate(rows_of, axis=0), hot_targ[lanes, :])
            acc = r if acc is None else acc + r
        return [
            acc[2 * q * blocks : (2 * q + 1) * blocks] + acc[(2 * q + 1) * blocks : (2 * q + 2) * blocks]
            for q in range(count_q)
        ]

    def advance():
        for k in range(STEPS):
            step(pair[k % 2], pair[(k + 1) % 2], k)

    def surface():
        temp = [fa[depth + p] for p in range(planes)]
        flux = [cx[depth + p] * (4.0 * t - in_plane(t)) for p, t in enumerate(temp)]
        return temp, flux

    def exchange(two, par):
        for j in range(n - 1, -1, -1):
            for k in range(1, groups):
                ex_copy(two, par, k, j, me).start()

    def chosen(two, par):
        for j in range(n):
            for k in range(1, groups):
                ex_copy(two, par, k, j, lax.rem(me + n - j, n)).wait_recv()
        out = None
        for k in range(1, groups):
            got = land_two[k - 1] if two else land_one[par, k - 1]
            source = lax.rem(grp + groups - k, groups)
            out = got if out is None else jnp.where(partner == source, got, out)
        return out

    def finish(two, par):
        for j in range(n):
            for k in range(1, groups):
                ex_copy(two, par, k, j, me).wait_send()
        for k in range(1, n):
            rs_copy(two, par, k, me).wait_send()

    def couple(it, carry):
        par = lax.rem(it, 2)
        first = it == 0

        @pl.when(jnp.logical_not(first))
        def _():
            advance()

        temp, flux = surface()
        mixed = sample([[away_t * t + away_f * f for t, f in zip(temp, flux)]])[0]
        for i in range(half):
            exp_one[i : i + 1, :] = mixed[:, i * LANES : (i + 1) * LANES]
        exchange(False, par)
        for d in offs:

            @pl.when(there(d))
            def _():
                halo_copy(par, d, -d).start()

        here = sample([temp])[0]
        for i in range(half):
            own_temp[i : i + 1, :] = here[:, i * LANES : (i + 1) * LANES]

        srcs = chosen(False, par)
        part = patches([srcs.reshape(blocks, LANES)])[0].reshape(n, half, LANES)
        mine = iota((n, half, LANES), 0) == me
        part_one[pl.ds(reach, n)] = part - jnp.where(mine, gain_t * own_temp[...], 0.0)
        for k in range(1, n):
            rs_copy(False, par, k, me).start()

        @pl.when(first)
        def _():
            each(offs, lambda d: starts(rest_copies(d, (2,))))

        rs_one[par, me] = part_one[pl.ds(me, span)]

        @pl.when(first)
        def _():
            each(offs, lambda d: arrivals(surf_copies(-d)))
            for d in offs:
                hot_rows(d + reach)

        for d in offs:

            @pl.when(there(d))
            def _():
                halo_copy(par, d, -d).wait_send()
                halo_copy(par, -d, d).wait_recv()

        for k in range(1, n):
            rs_copy(False, par, k, lax.rem(me + n - k, n)).wait_recv()
        inc = rs_one[par, 0]
        for j in range(1, n):
            inc = inc + rs_one[par, j]
        fa[own] = fa[own] + spread(reach, inc[reach])
        for d in offs:
            fa[pl.ds(depth + planes * d, planes)] = land[par, at[d]] + spread(d + reach, inc[d + reach])

        @pl.when(first)
        def _():
            each(offs, lambda d: arrivals(rest_copies(-d, (0, 1, 2))))
            each(offs, lambda d: departures(rest_copies(d, (0, 1, 2)) + surf_copies(d)))

        finish(False, par)
        return carry

    def final():
        par = (COUPLE - 1) % 2
        advance()
        got = sample(surface())
        for q in range(2):
            for i in range(half):
                exp_two[q * half + i : q * half + i + 1, :] = got[q][:, i * LANES : (i + 1) * LANES]
        exchange(True, par)
        src = chosen(True, par)
        parts = patches([src[:, q * half : (q + 1) * half].reshape(blocks, LANES) for q in range(2)])
        part_two[...] = jnp.concatenate([x.reshape(n, half, LANES) for x in parts], axis=1)
        for k in range(1, n):
            rs_copy(True, par, k, me).start()
        rs_two[me] = part_two[me]
        for k in range(1, n):
            rs_copy(True, par, k, lax.rem(me + n - k, n)).wait_recv()
        iface = rs_two[0]
        for j in range(1, n):
            iface = iface + rs_two[j]
        for q in range(2):
            for i in range(half):
                iface_ref[0, q : q + 1, i * LANES : (i + 1) * LANES] = iface[q * half + i : q * half + i + 1, :]
        inc = gain_t * (iface[:half] - exp_two[:half]) + gain_f * iface[half:]
        fa[own] = fa[own] + spread(reach, inc)
        finish(True, par)

    pair = (fa, fb)
    each(beside, lambda d: arrivals(first_copies(-d)))
    each(beside, lambda d: departures(first_copies(d)))
    for k in range(near):
        step(pair[k % 2], pair[(k + 1) % 2], depth - near + k)
    each(beside, lambda d: mid_copy(d).start())
    each(offs, lambda d: starts(surf_copies(d) + rest_copies(d, (0, 1))))
    each(beside, lambda d: mid_copy(-d).wait_recv())
    for d in beside:
        fa[pl.ds(depth + planes * d, planes)] = land[1, at[d]]
    each(beside, lambda d: mid_copy(d).wait_send())
    for k in range(near):
        step(pair[k % 2], pair[(k + 1) % 2], depth - near + k)

    lax.fori_loop(0, COUPLE - 1, couple, 0)
    final()

    def fold(b, carry):
        chunk = pl.ds(pl.multiple_of(b * 8 * LANES, LANES), 8 * LANES)
        rws = []
        for p in range(planes):
            x = fa[depth + p, pl.ds(pl.multiple_of(b * 8, 8), 8), :]
            rws.append(jnp.concatenate([x[i : i + 1, :] for i in range(8)], axis=1))
        out_ref[0, :, chunk] = jnp.concatenate(rws, axis=0)
        return carry

    lax.fori_loop(0, rows // 8, fold, 0)


def local_of(n, groups):
    def local(
        initial_field,
        conduct,
        velocity,
        heat_release,
        group_kind,
        partner,
        surface_cell,
        patch_count,
        patch_centres,
        patch_targets,
        patch_maps,
    ):
        _, planes, cells = initial_field.shape
        rows = cells // LANES
        surf_here = surface_cell.shape[1]
        cap = patch_centres.shape[1]
        reach = -(-STEPS // planes)
        ext = planes + 2 * reach * planes
        half = surf_here // LANES
        vmem = pl.BlockSpec(memory_space=pltpu.VMEM)
        smem = pl.BlockSpec(memory_space=pltpu.SMEM)
        dma = pltpu.SemaphoreType.DMA
        nd = 2 * reach
        scratch = [
            pltpu.VMEM((ext, rows, LANES), F32),
            pltpu.VMEM((ext, rows, LANES), F32),
            pltpu.VMEM((ext, rows, LANES), F32),
            pltpu.VMEM((ext, rows, LANES), F32),
            pltpu.VMEM((ext, rows, LANES), F32),
            pltpu.VMEM((2, nd, planes, rows, LANES), F32),
            pltpu.VMEM((nd + 1, 1, surf_here), jnp.int32),
            pltpu.VMEM((nd + 1, planes * rows, surf_here), BF16),
            pltpu.VMEM((nd + 1, surf_here, LANES), BF16),
            pltpu.VMEM((2 * LANES, surf_here), BF16),
            pltpu.VMEM((LANES, cap * LANES), BF16),
            pltpu.VMEM((n * half, cap * LANES), BF16),
            pltpu.VMEM((cap * LANES, LANES), BF16),
            pltpu.VMEM((cap, LANES, 2 * LANES), BF16),
            pltpu.VMEM((half, LANES), F32),
            pltpu.VMEM((2 * half, LANES), F32),
            pltpu.VMEM((half, LANES), F32),
            pltpu.VMEM((2, groups - 1, n, half, LANES), F32),
            pltpu.VMEM((groups - 1, n, 2 * half, LANES), F32),
            pltpu.VMEM((n + nd, half, LANES), F32),
            pltpu.VMEM((n, 2 * half, LANES), F32),
            pltpu.VMEM((2, n, nd + 1, half, LANES), F32),
            pltpu.VMEM((n, 2 * half, LANES), F32),
            dma((9, nd)),
            dma((9, nd)),
            dma((2, groups - 1, n)),
            dma((2, groups - 1, n)),
            dma((2, n - 1)),
            dma((2, n - 1)),
            dma((2, nd)),
            dma((2, nd)),
            pltpu.VMEM((cap, LANES, LANES), F32),
            dma(()),
        ]

        def body(*refs):
            kernel(n, groups, *refs)

        field, iface = pl.pallas_call(
            body,
            name="coupled",
            out_shape=(
                jax.ShapeDtypeStruct(initial_field.shape, F32),
                jax.ShapeDtypeStruct((1, 2, surf_here), F32),
            ),
            in_specs=[smem] * 3 + [vmem] * 7 + [pl.BlockSpec(memory_space=pl.ANY)],
            out_specs=(vmem, vmem),
            scratch_shapes=scratch,
            compiler_params=pltpu.CompilerParams(
                collective_id=0, has_side_effects=True, vmem_limit_bytes=56 * 1024 * 1024
            ),
        )(
            group_kind,
            partner,
            patch_count,
            initial_field,
            conduct,
            velocity,
            heat_release,
            surface_cell,
            patch_centres[0],
            patch_targets[0],
            patch_maps[0],
        )
        return field, iface

    return local


def solution(mesh):
    placed = (
        P("grp", "sub", None),
        P("grp", "sub", None),
        P("grp", "sub", None),
        P("grp", "sub", None),
        P(),
        P(),
        P("grp", "sub"),
        P("grp", None),
        P("grp", "sub", None),
        P("grp", "sub", None),
        P("grp", "sub", None, None),
    )
    return jax.shard_map(
        local_of(mesh.shape["sub"], mesh.shape["grp"]),
        mesh=mesh,
        in_specs=placed,
        out_specs=(P("grp", "sub", None), P("grp", None, "sub")),
        check_vma=False,
    )
```

```python
import jax
import jax.numpy as jnp
from jax import lax
from jax.experimental import pallas as pl
from jax.experimental.pallas import tpu as pltpu
from jax.sharding import PartitionSpec as P

STEPS = 4
COUPLE = 4
LANES = 128
F32 = jnp.float32
BF16 = jnp.bfloat16


def split(x):
    hi = x.astype(BF16).astype(F32)
    return hi, x - hi


def dot_nt(a, b):
    return lax.dot_general(a, b, (((1,), (1,)), ((), ())), preferred_element_type=F32)


def dot_nn(a, b):
    return lax.dot_general(a, b, (((1,), (0,)), ((), ())), preferred_element_type=F32)


def iota(shape, dim):
    return lax.broadcasted_iota(jnp.int32, shape, dim)


def in_plane(c):
    rows, cols = c.shape
    return (
        pltpu.roll(c, 1, 0)
        + pltpu.roll(c, rows - 1, 0)
        + pltpu.roll(c, 1, 1)
        + pltpu.roll(c, cols - 1, 1)
    )


def kernel(
    n,
    groups,
    kind_ref,
    partner_ref,
    count_ref,
    field_ref,
    cond_ref,
    vel_ref,
    heat_ref,
    surf_ref,
    cent_ref,
    targ_ref,
    maps_ref,
    out_ref,
    iface_ref,
    fa,
    fb,
    cx,
    vx,
    hx,
    land,
    surf_all,
    oh_surf,
    hot_surf,
    oh_lane,
    oh_cent,
    oh_targ,
    hot_targ,
    maps2,
    exp_one,
    exp_two,
    own_temp,
    land_one,
    land_two,
    part_one,
    part_two,
    rs_one,
    rs_two,
    set_send,
    set_recv,
    ex_send,
    ex_recv,
    rs_send,
    rs_recv,
    halo_send,
    halo_recv,
    maps,
    load_sem,
):
    planes = field_ref.shape[1]
    rows = fa.shape[1]
    near = STEPS // 2
    assert near % 2 == 0 and near <= planes
    surf_here = surf_ref.shape[1]
    cap = cent_ref.shape[0]
    reach = -(-STEPS // planes)
    depth = reach * planes
    ext = planes + 2 * depth
    offs = [d for d in range(-reach, reach + 1) if d != 0]
    at = {d: i for i, d in enumerate(offs)}
    half = surf_here // LANES
    span = 2 * reach + 1
    blocks = n * half
    me = lax.axis_index("sub")
    grp = lax.axis_index("grp")

    def there(d):
        return jnp.logical_and(me + d >= 0, me + d < n)

    def rcopy(src, dst, ss, rs, dev):
        return pltpu.make_async_remote_copy(
            src_ref=src,
            dst_ref=dst,
            send_sem=ss,
            recv_sem=rs,
            device_id=dev,
            device_id_type=pl.DeviceIdType.MESH,
        )

    load = pltpu.make_async_copy(maps_ref, maps, load_sem)
    load.start()

    for buf in (fa, cx, vx, hx):
        buf[...] = jnp.zeros(buf.shape, F32)
    land[...] = jnp.zeros(land.shape, F32)
    part_one[...] = jnp.zeros(part_one.shape, F32)
    surf_all[...] = jnp.zeros(surf_all.shape, jnp.int32)

    barrier = pltpu.get_barrier_semaphore()
    for k in range(1, n):
        pl.semaphore_signal(
            barrier, inc=1, device_id={"sub": lax.rem(me + k, n)}, device_id_type=pl.DeviceIdType.MESH
        )
    for k in range(1, groups):
        for j in range(n):
            pl.semaphore_signal(
                barrier,
                inc=1,
                device_id={"grp": lax.rem(grp + k, groups), "sub": lax.rem(me + j, n)},
                device_id_type=pl.DeviceIdType.MESH,
            )

    own = pl.ds(depth, planes)
    kind = kind_ref[grp]
    gas = jnp.where(kind == 0, 1.0, 0.0).astype(F32)
    gain_t = jnp.where(kind == 0, 0.5, 0.25).astype(F32)
    gain_f = jnp.where(kind == 0, -0.25, 0.25).astype(F32)
    away_t = jnp.where(kind == 0, 0.25, 0.5).astype(F32)
    away_f = jnp.where(kind == 0, 0.25, -0.25).astype(F32)
    fetch = ((field_ref, fa, None), (cond_ref, cx, None), (vel_ref, vx, gas), (heat_ref, hx, 0.5 * gas))

    def unfold(b, carry):
        chunk = pl.ds(pl.multiple_of(b * 8 * LANES, LANES), 8 * LANES)
        for src, dst, scale in fetch:
            x = src[0, :, chunk]
            if scale is not None:
                x = x * scale
            for p in range(planes):
                dst[depth + p, pl.ds(pl.multiple_of(b * 8, 8), 8), :] = jnp.concatenate(
                    [x[p : p + 1, i * LANES : (i + 1) * LANES] for i in range(8)], axis=0
                )
        return carry

    lax.fori_loop(0, rows // 8, unfold, 0)
    pl.semaphore_wait(barrier, n * groups - 1)

    def send_planes(buf, lo, hi, to, j):
        slot = -to
        shift = depth - (depth + planes * slot)
        return rcopy(
            buf.at[pl.ds(lo + shift, hi - lo)],
            buf.at[pl.ds(lo, hi - lo)],
            set_send.at[j, at[to]],
            set_recv.at[j, at[slot]],
            {"sub": me + to},
        )

    def first_copies(to):
        base = depth - planes * to
        lo, hi = max(base, depth - near), min(base + planes, depth + planes + near)
        out = [send_planes(fa, lo, hi, to, 0)]
        lo, hi = max(base, depth - near + 1), min(base + planes, depth + planes + near - 1)
        if hi > lo:
            out += [send_planes(buf, lo, hi, to, j + 1) for j, buf in enumerate((cx, vx, hx))]
        return out

    def rest_copies(to, which):
        base = depth - planes * to
        lo, hi = max(base, 1), min(base + planes, ext - 1)
        if to == 1:
            hi = min(hi, depth - near + 1)
        if to == -1:
            lo = max(lo, depth + planes + near - 1)
        if hi <= lo:
            return []
        return [send_planes((cx, vx, hx)[j], lo, hi, to, j + 4) for j in which]

    def surf_copies(to):
        return [
            rcopy(
                surf_ref,
                surf_all.at[reach - to],
                set_send.at[7, at[to]],
                set_recv.at[7, at[-to]],
                {"sub": me + to},
            )
        ]

    def mid_copy(to):
        return rcopy(
            fa.at[own],
            land.at[1, at[-to]],
            set_send.at[8, at[to]],
            set_recv.at[8, at[-to]],
            {"sub": me + to},
        )

    def each(ds, act):
        for d in ds:

            @pl.when(there(d))
            def _():
                act(d)

    def starts(copies):
        for c in copies:
            c.start()

    def arrivals(copies):
        for c in copies:
            c.wait_recv()

    def departures(copies):
        for c in copies:
            c.wait_send()

    beside = (-1, 1)
    each(beside, lambda d: starts(first_copies(d)))

    partner = partner_ref[grp]
    count = count_ref[0, me]
    surf_all[reach] = surf_ref[...]
    block_row = iota((blocks, LANES), 0)
    lane_row = iota((LANES, LANES), 0)

    def hot(mask):
        return jnp.where(mask, 1.0, 0.0).astype(F32)

    load.wait()
    for s in range(cap):
        lanes = pl.ds(s * LANES, LANES)
        oh_cent[:, lanes] = hot(lane_row == cent_ref[s : s + 1, :] % LANES).astype(BF16)
        oh_targ[:, lanes] = hot(block_row == targ_ref[s : s + 1, :] // LANES).astype(BF16)
        hot_targ[lanes, :] = hot(lane_row == targ_ref[s : s + 1, :] % LANES).T.astype(BF16)
        live = jnp.where(s < count, 1.0, 0.0).astype(F32)
        hi, lo = split((maps[s] * live).T)
        maps2[s, :, pl.ds(0, LANES)] = hi.astype(BF16)
        maps2[s, :, pl.ds(LANES, LANES)] = lo.astype(BF16)

    cell_row = iota((rows, surf_here), 0)

    def row_of(cell):
        return (cell // LANES) % rows

    def spot_of(cell):
        return cell // (rows * LANES) * LANES + cell % LANES

    def hot_rows(j):
        oh_surf[j] = hot(cell_row == row_of(surf_all[j])).astype(BF16)
        spot = spot_of(surf_all[j])
        for i in range(half):
            cols = slice(i * LANES, (i + 1) * LANES)
            for p in range(planes):
                hot_surf[j, cols, pl.ds(p * LANES, LANES)] = hot(lane_row + p * LANES == spot[:, cols]).T.astype(BF16)

    hot_rows(reach)
    oh_lane[...] = hot(iota((planes * LANES, surf_here), 0) == spot_of(surf_all[reach])).astype(BF16)

    group_of_slots = 4 if cap % 4 == 0 else 1
    width = group_of_slots * LANES
    block_of_chunk = iota((blocks, width), 0)

    def step(src, dst, k):
        for z in range(k + 1, ext - k - 1):
            c = src[z]
            dn = src[z - 1]
            lap = src[z + 1] + dn + in_plane(c) - 6.0 * c
            dst[z] = c + cx[z] * lap - vx[z] * (c - dn) + hx[z] * (1.0 + jnp.tanh(c))

    def spread(slot, inc):
        lhs = []
        for x in split(inc):
            wide = [jnp.broadcast_to(x[i : i + 1, :], (16, LANES)).astype(BF16) for i in range(half)]
            wide = jnp.concatenate(wide, axis=1)
            lhs += [oh_surf[slot, r * 16 : (r + 1) * 16, :] * wide for r in range(rows // 16)]
        r = dot_nn(jnp.concatenate(lhs, axis=0), hot_surf[slot])
        r = r[:rows] + r[rows:]
        return [r[:, p * LANES : (p + 1) * LANES] for p in range(planes)]

    def halo_copy(par, to, slot):
        return rcopy(
            fa.at[own],
            land.at[par, at[slot]],
            halo_send.at[par, at[to]],
            halo_recv.at[par, at[slot]],
            {"sub": me + to},
        )

    upper = 2 * me >= n

    def ex_copy(two, par, k, peer, sender):
        src, dst = (exp_two, land_two.at[k - 1, sender]) if two else (exp_one, land_one.at[par, k - 1, sender])
        return rcopy(
            src,
            dst,
            ex_send.at[par, k - 1, peer],
            ex_recv.at[par, k - 1, sender],
            {"grp": lax.rem(grp + k, groups), "sub": peer},
        )

    def rs_copy(two, par, k, sender):
        peer = lax.rem(me + k, n)
        if two:
            src, dst = part_two.at[peer], rs_two.at[sender]
        else:
            src, dst = part_one.at[pl.ds(peer, span)], rs_one.at[par, sender]
        return rcopy(src, dst, rs_send.at[par, k - 1], rs_recv.at[par, k - 1], {"sub": peer})

    def sample(values):
        lhs = []
        for x in values:
            lhs += split(jnp.concatenate(x, axis=1))
        got = dot_nn(jnp.concatenate(lhs, axis=0).astype(BF16), oh_lane[...])
        hit = cell_row == row_of(surf_all[reach])
        out = []
        for q in range(len(values)):
            v = got[2 * q * rows : (2 * q + 1) * rows] + got[(2 * q + 1) * rows : (2 * q + 2) * rows]
            out.append(jnp.sum(jnp.where(hit, v, 0.0), axis=0, keepdims=True))
        return out

    def patches(srcs):
        count_q = len(srcs)
        lhs = jnp.concatenate([x for v in srcs for x in split(v)], axis=0).astype(BF16)
        acc = None
        for s0 in range(0, cap, group_of_slots):
            lanes = slice(s0 * LANES, s0 * LANES + width)
            slots = range(s0, s0 + group_of_slots)
            cent = jnp.concatenate([cent_ref[s : s + 1, :] for s in slots], axis=1) // LANES
            vals = dot_nn(lhs, oh_cent[:, lanes])
            hit = block_of_chunk == cent
            cv = []
            for q in range(count_q):
                v = vals[2 * q * blocks : (2 * q + 1) * blocks] + vals[(2 * q + 1) * blocks : (2 * q + 2) * blocks]
                cv.append(jnp.sum(jnp.where(hit, v, 0.0), axis=0, keepdims=True))
            c4 = jnp.concatenate([x for v in cv for x in split(v)], axis=0).astype(BF16)
            contrib = []
            for i, s in enumerate(slots):
                r = dot_nn(c4[:, i * LANES : (i + 1) * LANES], maps2[s])
                contrib.append(r[:, :LANES] + r[:, LANES:])
            r = jnp.concatenate(contrib, axis=1)
            rows_of = []
            for q in range(count_q):
                for x in split(r[2 * q : 2 * q + 1] + r[2 * q + 1 : 2 * q + 2]):
                    wide = jnp.broadcast_to(x, (16, width)).astype(BF16)
                    rows_of += [oh_targ[b * 16 : (b + 1) * 16, lanes] * wide for b in range(blocks // 16)]
            r = dot_nn(jnp.concatenate(rows_of, axis=0), hot_targ[lanes, :])
            acc = r if acc is None else acc + r
        return [
            acc[2 * q * blocks : (2 * q + 1) * blocks] + acc[(2 * q + 1) * blocks : (2 * q + 2) * blocks]
            for q in range(count_q)
        ]

    def advance():
        for k in range(STEPS):
            step(pair[k % 2], pair[(k + 1) % 2], k)

    def surface():
        temp = [fa[depth + p] for p in range(planes)]
        flux = [cx[depth + p] * (4.0 * t - in_plane(t)) for p, t in enumerate(temp)]
        return temp, flux

    def exchange(two, par):
        for j in range(n):
            peer = jnp.where(upper, j, n - 1 - j)
            for k in range(1, groups):
                ex_copy(two, par, k, peer, me).start()

    def chosen(two, par):
        for j in range(n):
            for k in range(1, groups):
                ex_copy(two, par, k, me, j).wait_recv()
        out = None
        for k in range(1, groups):
            got = land_two[k - 1] if two else land_one[par, k - 1]
            source = lax.rem(grp + groups - k, groups)
            out = got if out is None else jnp.where(partner == source, got, out)
        return out

    def finish(two, par):
        for j in range(n):
            for k in range(1, groups):
                ex_copy(two, par, k, j, me).wait_send()
        for k in range(1, n):
            rs_copy(two, par, k, me).wait_send()

    def couple(it, carry):
        par = lax.rem(it, 2)
        first = it == 0

        @pl.when(jnp.logical_not(first))
        def _():
            advance()

        temp, flux = surface()
        mixed = sample([[away_t * t + away_f * f for t, f in zip(temp, flux)]])[0]
        for i in range(half):
            exp_one[i : i + 1, :] = mixed[:, i * LANES : (i + 1) * LANES]
        exchange(False, par)
        for d in offs:

            @pl.when(there(d))
            def _():
                halo_copy(par, d, -d).start()

        here = sample([temp])[0]
        for i in range(half):
            own_temp[i : i + 1, :] = here[:, i * LANES : (i + 1) * LANES]

        srcs = chosen(False, par)
        part = patches([srcs.reshape(blocks, LANES)])[0].reshape(n, half, LANES)
        mine = iota((n, half, LANES), 0) == me
        part_one[pl.ds(reach, n)] = part - jnp.where(mine, gain_t * own_temp[...], 0.0)
        for k in range(1, n):
            rs_copy(False, par, k, me).start()

        @pl.when(first)
        def _():
            each(offs, lambda d: starts(rest_copies(d, (2,))))

        rs_one[par, me] = part_one[pl.ds(me, span)]

        @pl.when(first)
        def _():
            each(offs, lambda d: arrivals(surf_copies(-d)))
            for d in offs:
                hot_rows(d + reach)

        for d in offs:

            @pl.when(there(d))
            def _():
                halo_copy(par, d, -d).wait_send()
                halo_copy(par, -d, d).wait_recv()

        for k in range(1, n):
            rs_copy(False, par, k, lax.rem(me + n - k, n)).wait_recv()
        inc = rs_one[par, 0]
        for j in range(1, n):
            inc = inc + rs_one[par, j]
        for p, x in enumerate(spread(reach, inc[reach])):
            fa[depth + p] = fa[depth + p] + x
        for d in offs:
            for p, x in enumerate(spread(d + reach, inc[d + reach])):
                fa[depth + planes * d + p] = land[par, at[d], p] + x

        @pl.when(first)
        def _():
            each(offs, lambda d: arrivals(rest_copies(-d, (0, 1, 2))))
            each(offs, lambda d: departures(rest_copies(d, (0, 1, 2)) + surf_copies(d)))

        finish(False, par)
        return carry

    def final():
        par = (COUPLE - 1) % 2
        advance()
        got = sample(surface())
        for q in range(2):
            for i in range(half):
                exp_two[q * half + i : q * half + i + 1, :] = got[q][:, i * LANES : (i + 1) * LANES]
        exchange(True, par)
        src = chosen(True, par)
        parts = patches([src[:, q * half : (q + 1) * half].reshape(blocks, LANES) for q in range(2)])
        part_two[...] = jnp.concatenate([x.reshape(n, half, LANES) for x in parts], axis=1)
        for k in range(1, n):
            rs_copy(True, par, k, me).start()
        rs_two[me] = part_two[me]
        for k in range(1, n):
            rs_copy(True, par, k, lax.rem(me + n - k, n)).wait_recv()
        iface = rs_two[0]
        for j in range(1, n):
            iface = iface + rs_two[j]
        iface_ref[...] = iface
        inc = gain_t * (iface[:half] - exp_two[:half]) + gain_f * iface[half:]
        for p, x in enumerate(spread(reach, inc)):
            out_ref[p] = fa[depth + p] + x
        finish(True, par)

    pair = (fa, fb)
    each(beside, lambda d: arrivals(first_copies(-d)))
    each(beside, lambda d: departures(first_copies(d)))
    for k in range(near):
        step(pair[k % 2], pair[(k + 1) % 2], depth - near + k)
    each(beside, lambda d: mid_copy(d).start())
    each(offs, lambda d: starts(surf_copies(d) + rest_copies(d, (0, 1))))
    each(beside, lambda d: mid_copy(-d).wait_recv())
    for d in beside:
        fa[pl.ds(depth + planes * d, planes)] = land[1, at[d]]
    each(beside, lambda d: mid_copy(d).wait_send())
    for k in range(near):
        step(pair[k % 2], pair[(k + 1) % 2], depth - near + k)

    lax.fori_loop(0, COUPLE - 1, couple, 0)
    final()


def unpack(planes_ref, rows_ref, out_ref, iface_ref):
    planes, rows, _ = planes_ref.shape
    half = rows_ref.shape[0] // 2
    for b in range(rows // 8):
        rws = []
        for p in range(planes):
            x = planes_ref[p, b * 8 : (b + 1) * 8, :]
            rws.append(jnp.concatenate([x[i : i + 1, :] for i in range(8)], axis=1))
        out_ref[0, :, b * 8 * LANES : (b + 1) * 8 * LANES] = jnp.concatenate(rws, axis=0)
    for q in range(2):
        for i in range(half):
            iface_ref[0, q : q + 1, i * LANES : (i + 1) * LANES] = rows_ref[q * half + i : q * half + i + 1, :]


def local_of(n, groups):
    def local(
        initial_field,
        conduct,
        velocity,
        heat_release,
        group_kind,
        partner,
        surface_cell,
        patch_count,
        patch_centres,
        patch_targets,
        patch_maps,
    ):
        _, planes, cells = initial_field.shape
        rows = cells // LANES
        surf_here = surface_cell.shape[1]
        cap = patch_centres.shape[1]
        reach = -(-STEPS // planes)
        ext = planes + 2 * reach * planes
        half = surf_here // LANES
        vmem = pl.BlockSpec(memory_space=pltpu.VMEM)
        smem = pl.BlockSpec(memory_space=pltpu.SMEM)
        dma = pltpu.SemaphoreType.DMA
        nd = 2 * reach
        scratch = [
            pltpu.VMEM((ext, rows, LANES), F32),
            pltpu.VMEM((ext, rows, LANES), F32),
            pltpu.VMEM((ext, rows, LANES), F32),
            pltpu.VMEM((ext, rows, LANES), F32),
            pltpu.VMEM((ext, rows, LANES), F32),
            pltpu.VMEM((2, nd, planes, rows, LANES), F32),
            pltpu.VMEM((nd + 1, 1, surf_here), jnp.int32),
            pltpu.VMEM((nd + 1, rows, surf_here), BF16),
            pltpu.VMEM((nd + 1, surf_here, planes * LANES), BF16),
            pltpu.VMEM((planes * LANES, surf_here), BF16),
            pltpu.VMEM((LANES, cap * LANES), BF16),
            pltpu.VMEM((n * half, cap * LANES), BF16),
            pltpu.VMEM((cap * LANES, LANES), BF16),
            pltpu.VMEM((cap, LANES, 2 * LANES), BF16),
            pltpu.VMEM((half, LANES), F32),
            pltpu.VMEM((2 * half, LANES), F32),
            pltpu.VMEM((half, LANES), F32),
            pltpu.VMEM((2, groups - 1, n, half, LANES), F32),
            pltpu.VMEM((groups - 1, n, 2 * half, LANES), F32),
            pltpu.VMEM((n + nd, half, LANES), F32),
            pltpu.VMEM((n, 2 * half, LANES), F32),
            pltpu.VMEM((2, n, nd + 1, half, LANES), F32),
            pltpu.VMEM((n, 2 * half, LANES), F32),
            dma((9, nd)),
            dma((9, nd)),
            dma((2, groups - 1, n)),
            dma((2, groups - 1, n)),
            dma((2, n - 1)),
            dma((2, n - 1)),
            dma((2, nd)),
            dma((2, nd)),
            pltpu.VMEM((cap, LANES, LANES), F32),
            dma(()),
        ]

        def body(*refs):
            kernel(n, groups, *refs)

        lying, tops = pl.pallas_call(
            body,
            name="coupled",
            out_shape=(
                pltpu.VMEM((planes, rows, LANES), F32),
                pltpu.VMEM((2 * half, LANES), F32),
            ),
            in_specs=[smem] * 3 + [vmem] * 7 + [pl.BlockSpec(memory_space=pl.ANY)],
            out_specs=(vmem, vmem),
            scratch_shapes=scratch,
            compiler_params=pltpu.CompilerParams(
                collective_id=0, has_side_effects=True, vmem_limit_bytes=56 * 1024 * 1024
            ),
        )(
            group_kind,
            partner,
            patch_count,
            initial_field,
            conduct,
            velocity,
            heat_release,
            surface_cell,
            patch_centres[0],
            patch_targets[0],
            patch_maps[0],
        )
        return pl.pallas_call(
            unpack,
            name="unpack",
            out_shape=(
                jax.ShapeDtypeStruct(initial_field.shape, F32),
                jax.ShapeDtypeStruct((1, 2, surf_here), F32),
            ),
            in_specs=[vmem] * 2,
            out_specs=(vmem, vmem),
        )(*(pltpu.with_memory_space_constraint(x, pltpu.VMEM) for x in (lying, tops)))

    return local


def solution(mesh):
    placed = (
        P("grp", "sub", None),
        P("grp", "sub", None),
        P("grp", "sub", None),
        P("grp", "sub", None),
        P(),
        P(),
        P("grp", "sub"),
        P("grp", None),
        P("grp", "sub", None),
        P("grp", "sub", None),
        P("grp", "sub", None, None),
    )
    return jax.shard_map(
        local_of(mesh.shape["sub"], mesh.shape["grp"]),
        mesh=mesh,
        in_specs=placed,
        out_specs=(P("grp", "sub", None), P("grp", None, "sub")),
        check_vma=False,
    )
```

```python
import jax
import jax.numpy as jnp
from jax import lax
from jax.experimental import pallas as pl
from jax.experimental.pallas import tpu as pltpu
from jax.sharding import PartitionSpec as P

STEPS = 4
COUPLE = 4
LANES = 128
F32 = jnp.float32
BF16 = jnp.bfloat16


def split(x):
    hi = x.astype(BF16).astype(F32)
    return hi, x - hi


def dot_nt(a, b):
    return lax.dot_general(a, b, (((1,), (1,)), ((), ())), preferred_element_type=F32)


def dot_nn(a, b):
    return lax.dot_general(a, b, (((1,), (0,)), ((), ())), preferred_element_type=F32)


def iota(shape, dim):
    return lax.broadcasted_iota(jnp.int32, shape, dim)


def in_plane(c):
    rows, cols = c.shape
    return (
        pltpu.roll(c, 1, 0)
        + pltpu.roll(c, rows - 1, 0)
        + pltpu.roll(c, 1, 1)
        + pltpu.roll(c, cols - 1, 1)
    )


def kernel(
    n,
    groups,
    kind_hbm,
    partner_hbm,
    count_hbm,
    field_hbm,
    cond_hbm,
    vel_hbm,
    heat_hbm,
    surf_hbm,
    cent_hbm,
    targ_hbm,
    maps_hbm,
    out_ref,
    iface_ref,
    fa,
    fb,
    cx,
    vx,
    hx,
    land,
    surf_all,
    oh_surf,
    hot_surf,
    oh_lane,
    oh_cent,
    oh_targ,
    hot_targ,
    maps2,
    exp_one,
    exp_two,
    own_temp,
    land_one,
    land_two,
    part_one,
    part_two,
    rs_one,
    rs_two,
    set_send,
    set_recv,
    ex_send,
    ex_recv,
    rs_send,
    rs_recv,
    halo_send,
    halo_recv,
    kind_ref,
    partner_ref,
    count_ref,
    field_ref,
    cond_ref,
    vel_ref,
    heat_ref,
    cent_ref,
    targ_ref,
    maps,
    load_sem,
):
    planes = field_ref.shape[0]
    rows = fa.shape[1]
    near = STEPS // 2
    assert near % 2 == 0 and near <= planes
    surf_here = surf_all.shape[2]
    cap = cent_ref.shape[0]
    reach = -(-STEPS // planes)
    depth = reach * planes
    ext = planes + 2 * depth
    offs = [d for d in range(-reach, reach + 1) if d != 0]
    at = {d: i for i, d in enumerate(offs)}
    half = surf_here // LANES
    span = 2 * reach + 1
    blocks = n * half
    me = lax.axis_index("sub")
    grp = lax.axis_index("grp")

    def there(d):
        return jnp.logical_and(me + d >= 0, me + d < n)

    def rcopy(src, dst, ss, rs, dev):
        return pltpu.make_async_remote_copy(
            src_ref=src,
            dst_ref=dst,
            send_sem=ss,
            recv_sem=rs,
            device_id=dev,
            device_id_type=pl.DeviceIdType.MESH,
        )

    pairs = (
        (kind_hbm, kind_ref),
        (partner_hbm, partner_ref),
        (count_hbm, count_ref),
        (field_hbm.at[0], field_ref),
        (cond_hbm.at[0], cond_ref),
        (vel_hbm.at[0], vel_ref),
        (heat_hbm.at[0], heat_ref),
        (surf_hbm, surf_all.at[reach]),
        (cent_hbm, cent_ref),
        (targ_hbm, targ_ref),
        (maps_hbm, maps),
    )
    loads = [pltpu.make_async_copy(src, dst, load_sem.at[i]) for i, (src, dst) in enumerate(pairs)]
    for c in loads:
        c.start()

    barrier = pltpu.get_barrier_semaphore()
    for k in range(1, n):
        pl.semaphore_signal(
            barrier, inc=1, device_id={"sub": lax.rem(me + k, n)}, device_id_type=pl.DeviceIdType.MESH
        )
    for k in range(1, groups):
        for j in range(n):
            pl.semaphore_signal(
                barrier,
                inc=1,
                device_id={"grp": lax.rem(grp + k, groups), "sub": lax.rem(me + j, n)},
                device_id_type=pl.DeviceIdType.MESH,
            )

    for border in (pl.ds(0, reach), pl.ds(reach + n, reach)):
        part_one[border] = jnp.zeros((reach, half, LANES), F32)
    for d in offs:

        @pl.when(jnp.logical_not(there(d)))
        def _():
            for buf in (fa, cx, vx, hx):
                buf[pl.ds(depth + planes * d, planes)] = jnp.zeros((planes, rows, LANES), F32)
            for par in range(2):
                land[par, at[d]] = jnp.zeros((planes, rows, LANES), F32)
            surf_all[reach + d] = jnp.zeros((1, surf_here), jnp.int32)

    for c in loads[:7]:
        c.wait()
    own = pl.ds(depth, planes)
    kind = kind_ref[grp]
    gas = jnp.where(kind == 0, 1.0, 0.0).astype(F32)
    gain_t = jnp.where(kind == 0, 0.5, 0.25).astype(F32)
    gain_f = jnp.where(kind == 0, -0.25, 0.25).astype(F32)
    away_t = jnp.where(kind == 0, 0.25, 0.5).astype(F32)
    away_f = jnp.where(kind == 0, 0.25, -0.25).astype(F32)
    fetch = ((field_ref, fa, None), (cond_ref, cx, None), (vel_ref, vx, gas), (heat_ref, hx, 0.5 * gas))

    def unfold(b, carry):
        chunk = pl.ds(pl.multiple_of(b * 8 * LANES, LANES), 8 * LANES)
        for src, dst, scale in fetch:
            x = src[:, chunk]
            if scale is not None:
                x = x * scale
            for p in range(planes):
                dst[depth + p, pl.ds(pl.multiple_of(b * 8, 8), 8), :] = jnp.concatenate(
                    [x[p : p + 1, i * LANES : (i + 1) * LANES] for i in range(8)], axis=0
                )
        return carry

    lax.fori_loop(0, rows // 8, unfold, 0)
    pl.semaphore_wait(barrier, n * groups - 1)

    def send_planes(buf, lo, hi, to, j):
        slot = -to
        shift = depth - (depth + planes * slot)
        return rcopy(
            buf.at[pl.ds(lo + shift, hi - lo)],
            buf.at[pl.ds(lo, hi - lo)],
            set_send.at[j, at[to]],
            set_recv.at[j, at[slot]],
            {"sub": me + to},
        )

    def first_copies(to):
        base = depth - planes * to
        lo, hi = max(base, depth - near), min(base + planes, depth + planes + near)
        out = [send_planes(fa, lo, hi, to, 0)]
        lo, hi = max(base, depth - near + 1), min(base + planes, depth + planes + near - 1)
        if hi > lo:
            out += [send_planes(buf, lo, hi, to, j + 1) for j, buf in enumerate((cx, vx, hx))]
        return out

    def rest_copies(to, which):
        base = depth - planes * to
        lo, hi = max(base, 1), min(base + planes, ext - 1)
        if to == 1:
            hi = min(hi, depth - near + 1)
        if to == -1:
            lo = max(lo, depth + planes + near - 1)
        if hi <= lo:
            return []
        return [send_planes((cx, vx, hx)[j], lo, hi, to, j + 4) for j in which]

    def surf_copies(to):
        return [
            rcopy(
                surf_all.at[reach],
                surf_all.at[reach - to],
                set_send.at[7, at[to]],
                set_recv.at[7, at[-to]],
                {"sub": me + to},
            )
        ]

    def mid_copy(to):
        return rcopy(
            fa.at[own],
            land.at[1, at[-to]],
            set_send.at[8, at[to]],
            set_recv.at[8, at[-to]],
            {"sub": me + to},
        )

    def each(ds, act):
        for d in ds:

            @pl.when(there(d))
            def _():
                act(d)

    def starts(copies):
        for c in copies:
            c.start()

    def arrivals(copies):
        for c in copies:
            c.wait_recv()

    def departures(copies):
        for c in copies:
            c.wait_send()

    beside = (-1, 1)
    each(beside, lambda d: starts(first_copies(d)))

    partner = partner_ref[grp]
    count = count_ref[0, me]
    block_row = iota((blocks, LANES), 0)
    lane_row = iota((LANES, LANES), 0)

    def block_of(x):
        return lax.shift_right_logical(x, jnp.full(x.shape, LANES.bit_length() - 1, jnp.int32))

    def lane_of(x):
        return lax.bitwise_and(x, jnp.full(x.shape, LANES - 1, jnp.int32))

    def hot(mask):
        return jnp.where(mask, 1.0, 0.0).astype(F32)

    for c in loads[7:]:
        c.wait()
    for s in range(cap):
        lanes = pl.ds(s * LANES, LANES)
        oh_cent[:, lanes] = hot(lane_row == lane_of(cent_ref[s : s + 1, :])).astype(BF16)
        oh_targ[:, lanes] = hot(block_row == block_of(targ_ref[s : s + 1, :])).astype(BF16)
        hot_targ[lanes, :] = hot(lane_row == lane_of(targ_ref[s : s + 1, :])).T.astype(BF16)
        live = jnp.where(s < count, 1.0, 0.0).astype(F32)
        hi, lo = split((maps[s] * live).T)
        maps2[s, :, pl.ds(0, LANES)] = hi.astype(BF16)
        maps2[s, :, pl.ds(LANES, LANES)] = lo.astype(BF16)

    cell_row = iota((rows, surf_here), 0)

    def plane_of(cell):
        return sum((cell >= p * rows * LANES).astype(jnp.int32) for p in range(1, planes))

    def row_of(cell):
        return block_of(cell) - plane_of(cell) * rows

    def spot_of(cell):
        return plane_of(cell) * LANES + lane_of(cell)

    def hot_rows(j):
        oh_surf[j] = hot(cell_row == row_of(surf_all[j])).astype(BF16)
        spot = spot_of(surf_all[j])
        for i in range(half):
            cols = slice(i * LANES, (i + 1) * LANES)
            for p in range(planes):
                hot_surf[j, cols, pl.ds(p * LANES, LANES)] = hot(lane_row + p * LANES == spot[:, cols]).T.astype(BF16)

    hot_rows(reach)
    oh_lane[...] = hot(iota((planes * LANES, surf_here), 0) == spot_of(surf_all[reach])).astype(BF16)

    block_of_slot = iota((blocks, cap * LANES), 0)

    def step(src, dst, k):
        for z in range(k + 1, ext - k - 1):
            c = src[z]
            dn = src[z - 1]
            lap = src[z + 1] + dn + in_plane(c) - 6.0 * c
            dst[z] = c + cx[z] * lap - vx[z] * (c - dn) + hx[z] * (1.0 + jnp.tanh(c))

    def spread(slot, inc):
        lhs = []
        for x in split(inc):
            wide = [jnp.broadcast_to(x[i : i + 1, :], (16, LANES)).astype(BF16) for i in range(half)]
            wide = jnp.concatenate(wide, axis=1)
            lhs += [oh_surf[slot, r * 16 : (r + 1) * 16, :] * wide for r in range(rows // 16)]
        r = dot_nn(jnp.concatenate(lhs, axis=0), hot_surf[slot])
        r = r[:rows] + r[rows:]
        return [r[:, p * LANES : (p + 1) * LANES] for p in range(planes)]

    def halo_copy(par, to, slot):
        return rcopy(
            fa.at[own],
            land.at[par, at[slot]],
            halo_send.at[par, at[to]],
            halo_recv.at[par, at[slot]],
            {"sub": me + to},
        )

    upper = 2 * me >= n

    def ex_copy(two, par, k, peer, sender):
        src, dst = (exp_two, land_two.at[k - 1, sender]) if two else (exp_one, land_one.at[par, k - 1, sender])
        return rcopy(
            src,
            dst,
            ex_send.at[par, k - 1, peer],
            ex_recv.at[par, k - 1, sender],
            {"grp": lax.rem(grp + k, groups), "sub": peer},
        )

    def rs_copy(two, par, k, sender):
        peer = lax.rem(me + k, n)
        if two:
            src, dst = part_two.at[peer], rs_two.at[sender]
        else:
            src, dst = part_one.at[pl.ds(peer, span)], rs_one.at[par, sender]
        return rcopy(src, dst, rs_send.at[par, k - 1], rs_recv.at[par, k - 1], {"sub": peer})

    def sample(values):
        lhs = []
        for x in values:
            lhs += split(jnp.concatenate(x, axis=1))
        got = dot_nn(jnp.concatenate(lhs, axis=0).astype(BF16), oh_lane[...])
        hit = cell_row == row_of(surf_all[reach])
        out = []
        for q in range(len(values)):
            v = got[2 * q * rows : (2 * q + 1) * rows] + got[(2 * q + 1) * rows : (2 * q + 2) * rows]
            out.append(jnp.sum(jnp.where(hit, v, 0.0), axis=0, keepdims=True))
        return out

    def patches(srcs):
        count_q = len(srcs)
        lhs = jnp.concatenate([x for v in srcs for x in split(v)], axis=0).astype(BF16)
        vals = dot_nn(lhs, oh_cent[...])
        cent = jnp.concatenate([cent_ref[s : s + 1, :] for s in range(cap)], axis=1)
        hit = block_of_slot == block_of(cent)
        cv = []
        for q in range(count_q):
            v = vals[2 * q * blocks : (2 * q + 1) * blocks] + vals[(2 * q + 1) * blocks : (2 * q + 2) * blocks]
            cv.append(jnp.sum(jnp.where(hit, v, 0.0), axis=0, keepdims=True))
        c4 = jnp.concatenate([x for v in cv for x in split(v)], axis=0).astype(BF16)
        contrib = []
        for s in range(cap):
            r = dot_nn(c4[:, s * LANES : (s + 1) * LANES], maps2[s])
            contrib.append(r[:, :LANES] + r[:, LANES:])
        r = jnp.concatenate(contrib, axis=1)
        rows_of = []
        for q in range(count_q):
            for x in split(r[2 * q : 2 * q + 1] + r[2 * q + 1 : 2 * q + 2]):
                wide = jnp.broadcast_to(x, (16, cap * LANES)).astype(BF16)
                rows_of += [oh_targ[b * 16 : (b + 1) * 16, :] * wide for b in range(blocks // 16)]
        acc = dot_nn(jnp.concatenate(rows_of, axis=0), hot_targ[...])
        return [
            acc[2 * q * blocks : (2 * q + 1) * blocks] + acc[(2 * q + 1) * blocks : (2 * q + 2) * blocks]
            for q in range(count_q)
        ]

    def advance():
        for k in range(STEPS):
            step(pair[k % 2], pair[(k + 1) % 2], k)

    def surface():
        temp = [fa[depth + p] for p in range(planes)]
        flux = [cx[depth + p] * (4.0 * t - in_plane(t)) for p, t in enumerate(temp)]
        return temp, flux

    def exchange(two, par):
        for j in range(n):
            peer = jnp.where(upper, j, n - 1 - j)
            for k in range(1, groups):
                ex_copy(two, par, k, peer, me).start()

    def chosen(two, par):
        for j in range(n):
            for k in range(1, groups):
                ex_copy(two, par, k, me, j).wait_recv()
        out = None
        for k in range(1, groups):
            got = land_two[k - 1] if two else land_one[par, k - 1]
            source = lax.rem(grp + groups - k, groups)
            out = got if out is None else jnp.where(partner == source, got, out)
        return out

    def finish(two, par):
        for j in range(n):
            for k in range(1, groups):
                ex_copy(two, par, k, j, me).wait_send()
        for k in range(1, n):
            rs_copy(two, par, k, me).wait_send()

    def couple(it, carry):
        par = lax.rem(it, 2)
        first = it == 0

        @pl.when(jnp.logical_not(first))
        def _():
            advance()

        temp, flux = surface()
        mixed = sample([[away_t * t + away_f * f for t, f in zip(temp, flux)]])[0]
        for i in range(half):
            exp_one[i : i + 1, :] = mixed[:, i * LANES : (i + 1) * LANES]
        exchange(False, par)
        for d in offs:

            @pl.when(there(d))
            def _():
                halo_copy(par, d, -d).start()

        here = sample([temp])[0]
        for i in range(half):
            own_temp[i : i + 1, :] = here[:, i * LANES : (i + 1) * LANES]

        srcs = chosen(False, par)
        part = patches([srcs.reshape(blocks, LANES)])[0].reshape(n, half, LANES)
        mine = iota((n, half, LANES), 0) == me
        part_one[pl.ds(reach, n)] = part - jnp.where(mine, gain_t * own_temp[...], 0.0)
        for k in range(1, n):
            rs_copy(False, par, k, me).start()

        @pl.when(first)
        def _():
            each(offs, lambda d: starts(rest_copies(d, (2,))))

        rs_one[par, me] = part_one[pl.ds(me, span)]

        @pl.when(first)
        def _():
            each(offs, lambda d: arrivals(surf_copies(-d)))
            for d in offs:
                hot_rows(d + reach)

        for d in offs:

            @pl.when(there(d))
            def _():
                halo_copy(par, d, -d).wait_send()
                halo_copy(par, -d, d).wait_recv()

        for k in range(1, n):
            rs_copy(False, par, k, lax.rem(me + n - k, n)).wait_recv()
        inc = rs_one[par, 0]
        for j in range(1, n):
            inc = inc + rs_one[par, j]
        sums = [spread(slot, inc[slot]) for slot in range(span)]
        for p in range(planes):
            fa[depth + p] = fa[depth + p] + sums[reach][p]
        for d in offs:
            for p in range(planes):
                fa[depth + planes * d + p] = land[par, at[d], p] + sums[d + reach][p]

        @pl.when(first)
        def _():
            each(offs, lambda d: arrivals(rest_copies(-d, (0, 1, 2))))
            each(offs, lambda d: departures(rest_copies(d, (0, 1, 2)) + surf_copies(d)))

        finish(False, par)
        return carry

    def final():
        par = (COUPLE - 1) % 2
        advance()
        got = sample(surface())
        for q in range(2):
            for i in range(half):
                exp_two[q * half + i : q * half + i + 1, :] = got[q][:, i * LANES : (i + 1) * LANES]
        exchange(True, par)
        src = chosen(True, par)
        parts = patches([src[:, q * half : (q + 1) * half].reshape(blocks, LANES) for q in range(2)])
        part_two[...] = jnp.concatenate([x.reshape(n, half, LANES) for x in parts], axis=1)
        for k in range(1, n):
            rs_copy(True, par, k, me).start()
        rs_two[me] = part_two[me]
        for k in range(1, n):
            rs_copy(True, par, k, lax.rem(me + n - k, n)).wait_recv()
        iface = rs_two[0]
        for j in range(1, n):
            iface = iface + rs_two[j]
        iface_ref[...] = iface
        inc = gain_t * (iface[:half] - exp_two[:half]) + gain_f * iface[half:]
        for p, x in enumerate(spread(reach, inc)):
            out_ref[p] = fa[depth + p] + x
        finish(True, par)

    pair = (fa, fb)
    each(beside, lambda d: arrivals(first_copies(-d)))
    each(beside, lambda d: departures(first_copies(d)))
    for k in range(near):
        step(pair[k % 2], pair[(k + 1) % 2], depth - near + k)
    each(beside, lambda d: mid_copy(d).start())
    each(offs, lambda d: starts(surf_copies(d) + rest_copies(d, (0, 1))))
    each(beside, lambda d: mid_copy(-d).wait_recv())
    for d in beside:
        fa[pl.ds(depth + planes * d, planes)] = land[1, at[d]]
    each(beside, lambda d: mid_copy(d).wait_send())
    for k in range(near):
        step(pair[k % 2], pair[(k + 1) % 2], depth - near + k)

    lax.fori_loop(0, COUPLE - 1, couple, 0)
    final()


def unpack(planes_ref, rows_ref, out_ref, iface_ref):
    planes, rows, _ = planes_ref.shape
    half = rows_ref.shape[0] // 2
    for b in range(rows // 8):
        rws = []
        for p in range(planes):
            x = planes_ref[p, b * 8 : (b + 1) * 8, :]
            rws.append(jnp.concatenate([x[i : i + 1, :] for i in range(8)], axis=1))
        out_ref[0, :, b * 8 * LANES : (b + 1) * 8 * LANES] = jnp.concatenate(rws, axis=0)
    for q in range(2):
        for i in range(half):
            iface_ref[0, q : q + 1, i * LANES : (i + 1) * LANES] = rows_ref[q * half + i : q * half + i + 1, :]


def local_of(n, groups):
    def local(
        initial_field,
        conduct,
        velocity,
        heat_release,
        group_kind,
        partner,
        surface_cell,
        patch_count,
        patch_centres,
        patch_targets,
        patch_maps,
    ):
        _, planes, cells = initial_field.shape
        rows = cells // LANES
        surf_here = surface_cell.shape[1]
        cap = patch_centres.shape[1]
        reach = -(-STEPS // planes)
        ext = planes + 2 * reach * planes
        half = surf_here // LANES
        vmem = pl.BlockSpec(memory_space=pltpu.VMEM)
        dma = pltpu.SemaphoreType.DMA
        nd = 2 * reach
        scratch = [
            pltpu.VMEM((ext, rows, LANES), F32),
            pltpu.VMEM((ext, rows, LANES), F32),
            pltpu.VMEM((ext, rows, LANES), F32),
            pltpu.VMEM((ext, rows, LANES), F32),
            pltpu.VMEM((ext, rows, LANES), F32),
            pltpu.VMEM((2, nd, planes, rows, LANES), F32),
            pltpu.VMEM((nd + 1, 1, surf_here), jnp.int32),
            pltpu.VMEM((nd + 1, rows, surf_here), BF16),
            pltpu.VMEM((nd + 1, surf_here, planes * LANES), BF16),
            pltpu.VMEM((planes * LANES, surf_here), BF16),
            pltpu.VMEM((LANES, cap * LANES), BF16),
            pltpu.VMEM((n * half, cap * LANES), BF16),
            pltpu.VMEM((cap * LANES, LANES), BF16),
            pltpu.VMEM((cap, LANES, 2 * LANES), BF16),
            pltpu.VMEM((half, LANES), F32),
            pltpu.VMEM((2 * half, LANES), F32),
            pltpu.VMEM((half, LANES), F32),
            pltpu.VMEM((2, groups - 1, n, half, LANES), F32),
            pltpu.VMEM((groups - 1, n, 2 * half, LANES), F32),
            pltpu.VMEM((n + nd, half, LANES), F32),
            pltpu.VMEM((n, 2 * half, LANES), F32),
            pltpu.VMEM((2, n, nd + 1, half, LANES), F32),
            pltpu.VMEM((n, 2 * half, LANES), F32),
            dma((9, nd)),
            dma((9, nd)),
            dma((2, groups - 1, n)),
            dma((2, groups - 1, n)),
            dma((2, n - 1)),
            dma((2, n - 1)),
            dma((2, nd)),
            dma((2, nd)),
            pltpu.SMEM(group_kind.shape, jnp.int32),
            pltpu.SMEM(partner.shape, jnp.int32),
            pltpu.SMEM(patch_count.shape, jnp.int32),
            pltpu.VMEM((planes, cells), F32),
            pltpu.VMEM((planes, cells), F32),
            pltpu.VMEM((planes, cells), F32),
            pltpu.VMEM((planes, cells), F32),
            pltpu.VMEM((cap, LANES), jnp.int32),
            pltpu.VMEM((cap, LANES), jnp.int32),
            pltpu.VMEM((cap, LANES, LANES), F32),
            dma((11,)),
        ]

        def body(*refs):
            kernel(n, groups, *refs)

        lying, tops = pl.pallas_call(
            body,
            name="coupled",
            out_shape=(
                pltpu.VMEM((planes, rows, LANES), F32),
                pltpu.VMEM((2 * half, LANES), F32),
            ),
            in_specs=[pl.BlockSpec(memory_space=pltpu.HBM)] * 11,
            out_specs=(vmem, vmem),
            scratch_shapes=scratch,
            compiler_params=pltpu.CompilerParams(
                collective_id=0, has_side_effects=True, vmem_limit_bytes=56 * 1024 * 1024
            ),
        )(
            group_kind,
            partner,
            patch_count,
            initial_field,
            conduct,
            velocity,
            heat_release,
            surface_cell,
            patch_centres[0],
            patch_targets[0],
            patch_maps[0],
        )
        return pl.pallas_call(
            unpack,
            name="unpack",
            out_shape=(
                jax.ShapeDtypeStruct(initial_field.shape, F32),
                jax.ShapeDtypeStruct((1, 2, surf_here), F32),
            ),
            in_specs=[vmem] * 2,
            out_specs=(vmem, vmem),
        )(*(pltpu.with_memory_space_constraint(x, pltpu.VMEM) for x in (lying, tops)))

    return local


def solution(mesh):
    placed = (
        P("grp", "sub", None),
        P("grp", "sub", None),
        P("grp", "sub", None),
        P("grp", "sub", None),
        P(),
        P(),
        P("grp", "sub"),
        P("grp", None),
        P("grp", "sub", None),
        P("grp", "sub", None),
        P("grp", "sub", None, None),
    )
    return jax.shard_map(
        local_of(mesh.shape["sub"], mesh.shape["grp"]),
        mesh=mesh,
        in_specs=placed,
        out_specs=(P("grp", "sub", None), P("grp", None, "sub")),
        check_vma=False,
    )
```

```python
import jax
import jax.numpy as jnp
from jax import lax
from jax.experimental import pallas as pl
from jax.experimental.pallas import tpu as pltpu
from jax.sharding import PartitionSpec as P

STEPS = 4
COUPLE = 4
LANES = 128
F32 = jnp.float32
BF16 = jnp.bfloat16


def split(x):
    hi = x.astype(BF16).astype(F32)
    return hi, x - hi


def dot_nt(a, b):
    return lax.dot_general(a, b, (((1,), (1,)), ((), ())), preferred_element_type=F32)


def dot_nn(a, b):
    return lax.dot_general(a, b, (((1,), (0,)), ((), ())), preferred_element_type=F32)


def iota(shape, dim):
    return lax.broadcasted_iota(jnp.int32, shape, dim)


def in_plane(c):
    rows, cols = c.shape
    return (
        pltpu.roll(c, 1, 0)
        + pltpu.roll(c, rows - 1, 0)
        + pltpu.roll(c, 1, 1)
        + pltpu.roll(c, cols - 1, 1)
    )


def kernel(
    n,
    groups,
    kind_hbm,
    partner_hbm,
    count_hbm,
    field_hbm,
    cond_hbm,
    vel_hbm,
    heat_hbm,
    surf_hbm,
    cent_hbm,
    targ_hbm,
    maps_hbm,
    out_ref,
    iface_ref,
    fa,
    fb,
    cx,
    vx,
    hx,
    land,
    surf_all,
    oh_surf,
    hot_surf,
    oh_lane,
    oh_cent,
    oh_targ,
    hot_targ,
    maps2,
    exp_one,
    exp_two,
    own_temp,
    land_one,
    land_two,
    part_one,
    part_two,
    rs_one,
    rs_two,
    set_send,
    set_recv,
    ex_send,
    ex_recv,
    rs_send,
    rs_recv,
    halo_send,
    halo_recv,
    kind_ref,
    partner_ref,
    count_ref,
    field_ref,
    cond_ref,
    vel_ref,
    heat_ref,
    cent_ref,
    targ_ref,
    maps,
    load_sem,
):
    planes = field_ref.shape[0]
    rows = fa.shape[1]
    near = STEPS // 2
    assert near % 2 == 0 and near <= planes
    surf_here = surf_all.shape[2]
    cap = cent_ref.shape[0]
    reach = -(-STEPS // planes)
    depth = reach * planes
    ext = planes + 2 * depth
    offs = [d for d in range(-reach, reach + 1) if d != 0]
    at = {d: i for i, d in enumerate(offs)}
    half = surf_here // LANES
    span = 2 * reach + 1
    blocks = n * half
    me = lax.axis_index("sub")
    grp = lax.axis_index("grp")

    def there(d):
        return jnp.logical_and(me + d >= 0, me + d < n)

    def rcopy(src, dst, ss, rs, dev):
        return pltpu.make_async_remote_copy(
            src_ref=src,
            dst_ref=dst,
            send_sem=ss,
            recv_sem=rs,
            device_id=dev,
            device_id_type=pl.DeviceIdType.MESH,
        )

    pairs = (
        (kind_hbm, kind_ref),
        (partner_hbm, partner_ref),
        (count_hbm, count_ref),
        (field_hbm.at[0], field_ref),
        (cond_hbm.at[0], cond_ref),
        (vel_hbm.at[0], vel_ref),
        (heat_hbm.at[0], heat_ref),
        (surf_hbm, surf_all.at[reach]),
        (cent_hbm, cent_ref),
        (targ_hbm, targ_ref),
        (maps_hbm, maps),
    )
    loads = [pltpu.make_async_copy(src, dst, load_sem.at[i]) for i, (src, dst) in enumerate(pairs)]
    for c in loads:
        c.start()

    barrier = pltpu.get_barrier_semaphore()
    for k in range(1, n):
        pl.semaphore_signal(
            barrier, inc=1, device_id={"sub": lax.rem(me + k, n)}, device_id_type=pl.DeviceIdType.MESH
        )
    for k in range(1, groups):
        for j in range(n):
            pl.semaphore_signal(
                barrier,
                inc=1,
                device_id={"grp": lax.rem(grp + k, groups), "sub": lax.rem(me + j, n)},
                device_id_type=pl.DeviceIdType.MESH,
            )

    for border in (pl.ds(0, reach), pl.ds(reach + n, reach)):
        part_one[border] = jnp.zeros((reach, half, LANES), F32)
    for d in offs:

        @pl.when(jnp.logical_not(there(d)))
        def _():
            for buf in (fa, cx, vx, hx):
                buf[pl.ds(depth + planes * d, planes)] = jnp.zeros((planes, rows, LANES), F32)
            for par in range(2):
                land[par, at[d]] = jnp.zeros((planes, rows, LANES), F32)
            surf_all[reach + d] = jnp.zeros((1, surf_here), jnp.int32)

    for c in loads[:7]:
        c.wait()
    own = pl.ds(depth, planes)
    kind = kind_ref[grp]
    gas = jnp.where(kind == 0, 1.0, 0.0).astype(F32)
    gain_t = jnp.where(kind == 0, 0.5, 0.25).astype(F32)
    gain_f = jnp.where(kind == 0, -0.25, 0.25).astype(F32)
    away_t = jnp.where(kind == 0, 0.25, 0.5).astype(F32)
    away_f = jnp.where(kind == 0, 0.25, -0.25).astype(F32)
    fetch = ((field_ref, fa, None), (cond_ref, cx, None), (vel_ref, vx, gas), (heat_ref, hx, 0.5 * gas))

    def unfold(b, carry):
        chunk = pl.ds(pl.multiple_of(b * 8 * LANES, LANES), 8 * LANES)
        for src, dst, scale in fetch:
            x = src[:, chunk]
            if scale is not None:
                x = x * scale
            for p in range(planes):
                dst[depth + p, pl.ds(pl.multiple_of(b * 8, 8), 8), :] = jnp.concatenate(
                    [x[p : p + 1, i * LANES : (i + 1) * LANES] for i in range(8)], axis=0
                )
        return carry

    lax.fori_loop(0, rows // 8, unfold, 0)
    pl.semaphore_wait(barrier, n * groups - 1)

    def send_planes(buf, lo, hi, to, j):
        slot = -to
        shift = depth - (depth + planes * slot)
        return rcopy(
            buf.at[pl.ds(lo + shift, hi - lo)],
            buf.at[pl.ds(lo, hi - lo)],
            set_send.at[j, at[to]],
            set_recv.at[j, at[slot]],
            {"sub": me + to},
        )

    def first_copies(to):
        base = depth - planes * to
        lo, hi = max(base, depth - near), min(base + planes, depth + planes + near)
        out = [send_planes(fa, lo, hi, to, 0)]
        lo, hi = max(base, depth - near + 1), min(base + planes, depth + planes + near - 1)
        if hi > lo:
            out += [send_planes(buf, lo, hi, to, j + 1) for j, buf in enumerate((cx, vx, hx))]
        return out

    def rest_copies(to, which):
        base = depth - planes * to
        lo, hi = max(base, 1), min(base + planes, ext - 1)
        if to == 1:
            hi = min(hi, depth - near + 1)
        if to == -1:
            lo = max(lo, depth + planes + near - 1)
        if hi <= lo:
            return []
        return [send_planes((cx, vx, hx)[j], lo, hi, to, j + 4) for j in which]

    sides = ((-1, 1, lax.rem(me, 2) == 0), (1, -1, lax.rem(me, 2) == 1))
    assert reach == 2 and near == planes == 2 and n % 2 == 0

    def when(mine, d, act):
        @pl.when(jnp.logical_and(mine, there(d)))
        def _():
            act()

    def rest_each(which, act):
        for x, p, mine in sides:
            for d in (x, p, 2 * p):
                when(mine, d, lambda d=d: act(rest_copies(d, which)))

    def handed_rest(x, p):
        plane = depth - 1 if x < 0 else depth + planes
        return [
            rcopy(
                buf.at[pl.ds(plane, 1)],
                buf.at[pl.ds(plane - p * planes, 1)],
                set_send.at[j + 4, at[x - p]],
                set_recv.at[j + 4, at[x - p]],
                {"sub": me + p},
            )
            for j, buf in enumerate((cx, vx, hx))
        ]

    def handed_halo(par, x, p):
        return rcopy(
            land.at[par, at[x]],
            land.at[par, at[x - p]],
            halo_send.at[par, at[x - p]],
            halo_recv.at[par, at[x - p]],
            {"sub": me + p},
        )

    def surf_copies(to):
        return [
            rcopy(
                surf_all.at[reach],
                surf_all.at[reach - to],
                set_send.at[7, at[to]],
                set_recv.at[7, at[-to]],
                {"sub": me + to},
            )
        ]

    def mid_copy(to):
        return rcopy(
            fa.at[own],
            land.at[1, at[-to]],
            set_send.at[8, at[to]],
            set_recv.at[8, at[-to]],
            {"sub": me + to},
        )

    def each(ds, act):
        for d in ds:

            @pl.when(there(d))
            def _():
                act(d)

    def starts(copies):
        for c in copies:
            c.start()

    def arrivals(copies):
        for c in copies:
            c.wait_recv()

    def departures(copies):
        for c in copies:
            c.wait_send()

    beside = (-1, 1)
    each(beside, lambda d: starts(first_copies(d)))

    partner = partner_ref[grp]
    count = count_ref[0, me]
    block_row = iota((blocks, LANES), 0)
    lane_row = iota((LANES, LANES), 0)

    def block_of(x):
        return lax.shift_right_logical(x, jnp.full(x.shape, LANES.bit_length() - 1, jnp.int32))

    def lane_of(x):
        return lax.bitwise_and(x, jnp.full(x.shape, LANES - 1, jnp.int32))

    def hot(mask):
        return jnp.where(mask, 1.0, 0.0).astype(F32)

    for c in loads[7:]:
        c.wait()
    for s in range(cap):
        lanes = pl.ds(s * LANES, LANES)
        oh_cent[:, lanes] = hot(lane_row == lane_of(cent_ref[s : s + 1, :])).astype(BF16)
        oh_targ[:, lanes] = hot(block_row == block_of(targ_ref[s : s + 1, :])).astype(BF16)
        hot_targ[lanes, :] = hot(lane_row == lane_of(targ_ref[s : s + 1, :])).T.astype(BF16)
        live = jnp.where(s < count, 1.0, 0.0).astype(F32)
        hi, lo = split((maps[s] * live).T)
        maps2[s, :, pl.ds(0, LANES)] = hi.astype(BF16)
        maps2[s, :, pl.ds(LANES, LANES)] = lo.astype(BF16)

    cell_row = iota((rows, surf_here), 0)

    def plane_of(cell):
        return sum((cell >= p * rows * LANES).astype(jnp.int32) for p in range(1, planes))

    def row_of(cell):
        return block_of(cell) - plane_of(cell) * rows

    def spot_of(cell):
        return plane_of(cell) * LANES + lane_of(cell)

    def hot_rows(j):
        oh_surf[j] = hot(cell_row == row_of(surf_all[j])).astype(BF16)
        spot = spot_of(surf_all[j])
        for i in range(half):
            cols = slice(i * LANES, (i + 1) * LANES)
            for p in range(planes):
                hot_surf[j, cols, pl.ds(p * LANES, LANES)] = hot(lane_row + p * LANES == spot[:, cols]).T.astype(BF16)

    hot_rows(reach)
    oh_lane[...] = hot(iota((planes * LANES, surf_here), 0) == spot_of(surf_all[reach])).astype(BF16)

    block_of_slot = iota((blocks, cap * LANES), 0)

    def step(src, dst, k):
        for z in range(k + 1, ext - k - 1):
            c = src[z]
            dn = src[z - 1]
            lap = src[z + 1] + dn + in_plane(c) - 6.0 * c
            dst[z] = c + cx[z] * lap - vx[z] * (c - dn) + hx[z] * (1.0 + jnp.tanh(c))

    def spread(slot, inc):
        lhs = []
        for x in split(inc):
            wide = [jnp.broadcast_to(x[i : i + 1, :], (16, LANES)).astype(BF16) for i in range(half)]
            wide = jnp.concatenate(wide, axis=1)
            lhs += [oh_surf[slot, r * 16 : (r + 1) * 16, :] * wide for r in range(rows // 16)]
        r = dot_nn(jnp.concatenate(lhs, axis=0), hot_surf[slot])
        r = r[:rows] + r[rows:]
        return [r[:, p * LANES : (p + 1) * LANES] for p in range(planes)]

    def halo_copy(par, to, slot):
        return rcopy(
            fa.at[own],
            land.at[par, at[slot]],
            halo_send.at[par, at[to]],
            halo_recv.at[par, at[slot]],
            {"sub": me + to},
        )

    upper = 2 * me >= n

    def ex_copy(two, par, k, peer, sender):
        src, dst = (exp_two, land_two.at[k - 1, sender]) if two else (exp_one, land_one.at[par, k - 1, sender])
        return rcopy(
            src,
            dst,
            ex_send.at[par, k - 1, peer],
            ex_recv.at[par, k - 1, sender],
            {"grp": lax.rem(grp + k, groups), "sub": peer},
        )

    def rs_copy(two, par, k, sender):
        peer = lax.rem(me + k, n)
        if two:
            src, dst = part_two.at[peer], rs_two.at[sender]
        else:
            src, dst = part_one.at[pl.ds(peer, span)], rs_one.at[par, sender]
        return rcopy(src, dst, rs_send.at[par, k - 1], rs_recv.at[par, k - 1], {"sub": peer})

    def sample(values):
        lhs = []
        for x in values:
            lhs += split(jnp.concatenate(x, axis=1))
        got = dot_nn(jnp.concatenate(lhs, axis=0).astype(BF16), oh_lane[...])
        hit = cell_row == row_of(surf_all[reach])
        out = []
        for q in range(len(values)):
            v = got[2 * q * rows : (2 * q + 1) * rows] + got[(2 * q + 1) * rows : (2 * q + 2) * rows]
            out.append(jnp.sum(jnp.where(hit, v, 0.0), axis=0, keepdims=True))
        return out

    def patches(srcs):
        count_q = len(srcs)
        lhs = jnp.concatenate([x for v in srcs for x in split(v)], axis=0).astype(BF16)
        vals = dot_nn(lhs, oh_cent[...])
        cent = jnp.concatenate([cent_ref[s : s + 1, :] for s in range(cap)], axis=1)
        hit = block_of_slot == block_of(cent)
        cv = []
        for q in range(count_q):
            v = vals[2 * q * blocks : (2 * q + 1) * blocks] + vals[(2 * q + 1) * blocks : (2 * q + 2) * blocks]
            cv.append(jnp.sum(jnp.where(hit, v, 0.0), axis=0, keepdims=True))
        c4 = jnp.concatenate([x for v in cv for x in split(v)], axis=0).astype(BF16)
        contrib = []
        for s in range(cap):
            r = dot_nn(c4[:, s * LANES : (s + 1) * LANES], maps2[s])
            contrib.append(r[:, :LANES] + r[:, LANES:])
        r = jnp.concatenate(contrib, axis=1)
        rows_of = []
        for q in range(count_q):
            for x in split(r[2 * q : 2 * q + 1] + r[2 * q + 1 : 2 * q + 2]):
                wide = jnp.broadcast_to(x, (16, cap * LANES)).astype(BF16)
                rows_of += [oh_targ[b * 16 : (b + 1) * 16, :] * wide for b in range(blocks // 16)]
        acc = dot_nn(jnp.concatenate(rows_of, axis=0), hot_targ[...])
        return [
            acc[2 * q * blocks : (2 * q + 1) * blocks] + acc[(2 * q + 1) * blocks : (2 * q + 2) * blocks]
            for q in range(count_q)
        ]

    def advance():
        for k in range(STEPS):
            step(pair[k % 2], pair[(k + 1) % 2], k)

    def surface():
        temp = [fa[depth + p] for p in range(planes)]
        flux = [cx[depth + p] * (4.0 * t - in_plane(t)) for p, t in enumerate(temp)]
        return temp, flux

    def exchange(two, par):
        for j in range(n):
            peer = jnp.where(upper, j, n - 1 - j)
            for k in range(1, groups):
                ex_copy(two, par, k, peer, me).start()

    def chosen(two, par):
        for j in range(n):
            for k in range(1, groups):
                ex_copy(two, par, k, me, j).wait_recv()
        out = None
        for k in range(1, groups):
            got = land_two[k - 1] if two else land_one[par, k - 1]
            source = lax.rem(grp + groups - k, groups)
            out = got if out is None else jnp.where(partner == source, got, out)
        return out

    def finish(two, par):
        for j in range(n):
            for k in range(1, groups):
                ex_copy(two, par, k, j, me).wait_send()
        for k in range(1, n):
            rs_copy(two, par, k, me).wait_send()

    def couple(it, carry):
        par = lax.rem(it, 2)
        first = it == 0

        @pl.when(jnp.logical_not(first))
        def _():
            advance()

        temp, flux = surface()
        mixed = sample([[away_t * t + away_f * f for t, f in zip(temp, flux)]])[0]
        for i in range(half):
            exp_one[i : i + 1, :] = mixed[:, i * LANES : (i + 1) * LANES]
        exchange(False, par)
        for x, p, mine in sides:
            for d in (x, p, 2 * p):
                when(mine, d, lambda d=d: halo_copy(par, d, -d).start())

        here = sample([temp])[0]
        for i in range(half):
            own_temp[i : i + 1, :] = here[:, i * LANES : (i + 1) * LANES]

        srcs = chosen(False, par)
        part = patches([srcs.reshape(blocks, LANES)])[0].reshape(n, half, LANES)
        mine = iota((n, half, LANES), 0) == me
        part_one[pl.ds(reach, n)] = part - jnp.where(mine, gain_t * own_temp[...], 0.0)
        for k in range(1, n):
            rs_copy(False, par, k, me).start()
        for x, p, mine in sides:

            def hand_on(x=x, p=p):
                halo_copy(par, -x, x).wait_recv()
                handed_halo(par, x, p).start()

            when(mine, x, hand_on)

        @pl.when(first)
        def _():
            rest_each((2,), starts)

        rs_one[par, me] = part_one[pl.ds(me, span)]

        @pl.when(first)
        def _():
            each(offs, lambda d: arrivals(surf_copies(-d)))
            for d in offs:
                hot_rows(d + reach)

        for x, p, mine in sides:
            for d in (x, p, 2 * p):
                when(mine, d, lambda d=d: halo_copy(par, d, -d).wait_send())
            when(mine, x, lambda x=x, p=p: handed_halo(par, x, p).wait_send())
            for d in (p, 2 * p, 2 * x):
                when(mine, d, lambda d=d: halo_copy(par, -d, d).wait_recv())

        for k in range(1, n):
            rs_copy(False, par, k, lax.rem(me + n - k, n)).wait_recv()
        inc = rs_one[par, 0]
        for j in range(1, n):
            inc = inc + rs_one[par, j]
        sums = [spread(slot, inc[slot]) for slot in range(span)]
        for p in range(planes):
            fa[depth + p] = fa[depth + p] + sums[reach][p]
        for d in offs:
            for p in range(planes):
                fa[depth + planes * d + p] = land[par, at[d], p] + sums[d + reach][p]

        @pl.when(first)
        def _():
            each(offs, lambda d: arrivals(rest_copies(-d, (0, 1, 2))))
            each(offs, lambda d: departures(surf_copies(d)))
            rest_each((0, 1, 2), departures)
            for x, p, mine in sides:
                when(mine, x, lambda x=x, p=p: departures(handed_rest(x, p)))

        finish(False, par)
        return carry

    def final():
        par = (COUPLE - 1) % 2
        advance()
        got = sample(surface())
        for q in range(2):
            for i in range(half):
                exp_two[q * half + i : q * half + i + 1, :] = got[q][:, i * LANES : (i + 1) * LANES]
        exchange(True, par)
        src = chosen(True, par)
        parts = patches([src[:, q * half : (q + 1) * half].reshape(blocks, LANES) for q in range(2)])
        part_two[...] = jnp.concatenate([x.reshape(n, half, LANES) for x in parts], axis=1)
        for k in range(1, n):
            rs_copy(True, par, k, me).start()
        rs_two[me] = part_two[me]
        for k in range(1, n):
            rs_copy(True, par, k, lax.rem(me + n - k, n)).wait_recv()
        iface = rs_two[0]
        for j in range(1, n):
            iface = iface + rs_two[j]
        iface_ref[...] = iface
        inc = gain_t * (iface[:half] - exp_two[:half]) + gain_f * iface[half:]
        for p, x in enumerate(spread(reach, inc)):
            out_ref[p] = fa[depth + p] + x
        finish(True, par)

    pair = (fa, fb)
    each(beside, lambda d: arrivals(first_copies(-d)))
    each(beside, lambda d: departures(first_copies(d)))
    for k in range(near):
        step(pair[k % 2], pair[(k + 1) % 2], depth - near + k)
    each(beside, lambda d: mid_copy(d).start())
    each(offs, lambda d: starts(surf_copies(d)))
    rest_each((0, 1), starts)
    for x, p, mine in sides:
        when(mine, x, lambda x=x, p=p: starts(handed_rest(x, p)))
    each(beside, lambda d: mid_copy(-d).wait_recv())
    for d in beside:
        fa[pl.ds(depth + planes * d, planes)] = land[1, at[d]]
    each(beside, lambda d: mid_copy(d).wait_send())
    for k in range(near):
        step(pair[k % 2], pair[(k + 1) % 2], depth - near + k)

    lax.fori_loop(0, COUPLE - 1, couple, 0)
    final()


def unpack(planes_ref, rows_ref, out_ref, iface_ref):
    planes, rows, _ = planes_ref.shape
    half = rows_ref.shape[0] // 2
    for b in range(rows // 8):
        rws = []
        for p in range(planes):
            x = planes_ref[p, b * 8 : (b + 1) * 8, :]
            rws.append(jnp.concatenate([x[i : i + 1, :] for i in range(8)], axis=1))
        out_ref[0, :, b * 8 * LANES : (b + 1) * 8 * LANES] = jnp.concatenate(rws, axis=0)
    for q in range(2):
        for i in range(half):
            iface_ref[0, q : q + 1, i * LANES : (i + 1) * LANES] = rows_ref[q * half + i : q * half + i + 1, :]


def local_of(n, groups):
    def local(
        initial_field,
        conduct,
        velocity,
        heat_release,
        group_kind,
        partner,
        surface_cell,
        patch_count,
        patch_centres,
        patch_targets,
        patch_maps,
    ):
        _, planes, cells = initial_field.shape
        rows = cells // LANES
        surf_here = surface_cell.shape[1]
        cap = patch_centres.shape[1]
        reach = -(-STEPS // planes)
        ext = planes + 2 * reach * planes
        half = surf_here // LANES
        vmem = pl.BlockSpec(memory_space=pltpu.VMEM)
        dma = pltpu.SemaphoreType.DMA
        nd = 2 * reach
        scratch = [
            pltpu.VMEM((ext, rows, LANES), F32),
            pltpu.VMEM((ext, rows, LANES), F32),
            pltpu.VMEM((ext, rows, LANES), F32),
            pltpu.VMEM((ext, rows, LANES), F32),
            pltpu.VMEM((ext, rows, LANES), F32),
            pltpu.VMEM((2, nd, planes, rows, LANES), F32),
            pltpu.VMEM((nd + 1, 1, surf_here), jnp.int32),
            pltpu.VMEM((nd + 1, rows, surf_here), BF16),
            pltpu.VMEM((nd + 1, surf_here, planes * LANES), BF16),
            pltpu.VMEM((planes * LANES, surf_here), BF16),
            pltpu.VMEM((LANES, cap * LANES), BF16),
            pltpu.VMEM((n * half, cap * LANES), BF16),
            pltpu.VMEM((cap * LANES, LANES), BF16),
            pltpu.VMEM((cap, LANES, 2 * LANES), BF16),
            pltpu.VMEM((half, LANES), F32),
            pltpu.VMEM((2 * half, LANES), F32),
            pltpu.VMEM((half, LANES), F32),
            pltpu.VMEM((2, groups - 1, n, half, LANES), F32),
            pltpu.VMEM((groups - 1, n, 2 * half, LANES), F32),
            pltpu.VMEM((n + nd, half, LANES), F32),
            pltpu.VMEM((n, 2 * half, LANES), F32),
            pltpu.VMEM((2, n, nd + 1, half, LANES), F32),
            pltpu.VMEM((n, 2 * half, LANES), F32),
            dma((9, nd)),
            dma((9, nd)),
            dma((2, groups - 1, n)),
            dma((2, groups - 1, n)),
            dma((2, n - 1)),
            dma((2, n - 1)),
            dma((2, nd)),
            dma((2, nd)),
            pltpu.SMEM(group_kind.shape, jnp.int32),
            pltpu.SMEM(partner.shape, jnp.int32),
            pltpu.SMEM(patch_count.shape, jnp.int32),
            pltpu.VMEM((planes, cells), F32),
            pltpu.VMEM((planes, cells), F32),
            pltpu.VMEM((planes, cells), F32),
            pltpu.VMEM((planes, cells), F32),
            pltpu.VMEM((cap, LANES), jnp.int32),
            pltpu.VMEM((cap, LANES), jnp.int32),
            pltpu.VMEM((cap, LANES, LANES), F32),
            dma((11,)),
        ]

        def body(*refs):
            kernel(n, groups, *refs)

        lying, tops = pl.pallas_call(
            body,
            name="coupled",
            out_shape=(
                pltpu.VMEM((planes, rows, LANES), F32),
                pltpu.VMEM((2 * half, LANES), F32),
            ),
            in_specs=[pl.BlockSpec(memory_space=pltpu.HBM)] * 11,
            out_specs=(vmem, vmem),
            scratch_shapes=scratch,
            compiler_params=pltpu.CompilerParams(
                collective_id=0, has_side_effects=True, vmem_limit_bytes=56 * 1024 * 1024
            ),
        )(
            group_kind,
            partner,
            patch_count,
            initial_field,
            conduct,
            velocity,
            heat_release,
            surface_cell,
            patch_centres[0],
            patch_targets[0],
            patch_maps[0],
        )
        return pl.pallas_call(
            unpack,
            name="unpack",
            out_shape=(
                jax.ShapeDtypeStruct(initial_field.shape, F32),
                jax.ShapeDtypeStruct((1, 2, surf_here), F32),
            ),
            in_specs=[vmem] * 2,
            out_specs=(vmem, vmem),
        )(*(pltpu.with_memory_space_constraint(x, pltpu.VMEM) for x in (lying, tops)))

    return local


def solution(mesh):
    placed = (
        P("grp", "sub", None),
        P("grp", "sub", None),
        P("grp", "sub", None),
        P("grp", "sub", None),
        P(),
        P(),
        P("grp", "sub"),
        P("grp", None),
        P("grp", "sub", None),
        P("grp", "sub", None),
        P("grp", "sub", None, None),
    )
    return jax.shard_map(
        local_of(mesh.shape["sub"], mesh.shape["grp"]),
        mesh=mesh,
        in_specs=placed,
        out_specs=(P("grp", "sub", None), P("grp", None, "sub")),
        check_vma=False,
    )
```

```python
import jax
import jax.numpy as jnp
from jax import lax
from jax.experimental import pallas as pl
from jax.experimental.pallas import tpu as pltpu
from jax.sharding import PartitionSpec as P

STEPS = 4
COUPLE = 4
LANES = 128
F32 = jnp.float32
BF16 = jnp.bfloat16


def split(x):
    hi = x.astype(BF16).astype(F32)
    return hi, x - hi


def dot_nt(a, b):
    return lax.dot_general(a, b, (((1,), (1,)), ((), ())), preferred_element_type=F32)


def dot_nn(a, b):
    return lax.dot_general(a, b, (((1,), (0,)), ((), ())), preferred_element_type=F32)


def iota(shape, dim):
    return lax.broadcasted_iota(jnp.int32, shape, dim)


def in_plane(c):
    rows, cols = c.shape
    return (
        pltpu.roll(c, 1, 0)
        + pltpu.roll(c, rows - 1, 0)
        + pltpu.roll(c, 1, 1)
        + pltpu.roll(c, cols - 1, 1)
    )


def kernel(
    n,
    groups,
    kind_hbm,
    partner_hbm,
    count_hbm,
    field_hbm,
    cond_hbm,
    vel_hbm,
    heat_hbm,
    surf_hbm,
    cent_hbm,
    targ_hbm,
    maps_hbm,
    out_ref,
    iface_ref,
    fa,
    fb,
    cx,
    vx,
    hx,
    land,
    surf_all,
    oh_surf,
    hot_surf,
    oh_lane,
    oh_cent,
    oh_targ,
    hot_targ,
    maps2,
    exp_one,
    exp_two,
    own_temp,
    land_one,
    land_two,
    part_one,
    part_two,
    rs_one,
    rs_two,
    set_send,
    set_recv,
    ex_send,
    ex_recv,
    rs_send,
    rs_recv,
    halo_send,
    halo_recv,
    kind_ref,
    partner_ref,
    count_ref,
    field_ref,
    cond_ref,
    vel_ref,
    heat_ref,
    cent_ref,
    targ_ref,
    maps,
    load_sem,
    ready,
):
    planes = field_ref.shape[0]
    rows = fa.shape[1]
    near = STEPS // 2
    assert near % 2 == 0 and near <= planes
    surf_here = surf_all.shape[2]
    cap = cent_ref.shape[0]
    reach = -(-STEPS // planes)
    depth = reach * planes
    ext = planes + 2 * depth
    offs = [d for d in range(-reach, reach + 1) if d != 0]
    at = {d: i for i, d in enumerate(offs)}
    half = surf_here // LANES
    span = 2 * reach + 1
    blocks = n * half
    me = lax.axis_index("sub")
    grp = lax.axis_index("grp")

    def there(d):
        return jnp.logical_and(me + d >= 0, me + d < n)

    def rcopy(src, dst, ss, rs, dev):
        return pltpu.make_async_remote_copy(
            src_ref=src,
            dst_ref=dst,
            send_sem=ss,
            recv_sem=rs,
            device_id=dev,
            device_id_type=pl.DeviceIdType.MESH,
        )

    pairs = (
        (kind_hbm, kind_ref),
        (partner_hbm, partner_ref),
        (count_hbm, count_ref),
        (field_hbm.at[0], field_ref),
        (cond_hbm.at[0], cond_ref),
        (vel_hbm.at[0], vel_ref),
        (heat_hbm.at[0], heat_ref),
        (surf_hbm, surf_all.at[reach]),
        (cent_hbm, cent_ref),
        (targ_hbm, targ_ref),
        (maps_hbm, maps),
    )
    loads = [pltpu.make_async_copy(src, dst, load_sem.at[i]) for i, (src, dst) in enumerate(pairs)]
    for c in loads:
        c.start()

    def signal(sem, dev):
        pl.semaphore_signal(sem, inc=1, device_id=dev, device_id_type=pl.DeviceIdType.MESH)

    def among(ds):
        return sum(there(d).astype(jnp.int32) for d in ds)

    def tell(sem, ds):
        for d in ds:

            @pl.when(there(d))
            def _():
                signal(sem, {"sub": me + d})

    barrier = pltpu.get_barrier_semaphore()
    tell(barrier, offs)
    for k in range(1, groups):
        signal(barrier, {"grp": lax.rem(grp + k, groups)})
    hops = [reach]
    while 2 * hops[-1] < n:
        hops.append(2 * hops[-1])

    def hear(i):
        pl.semaphore_wait(ready.at[i], among((-hops[i], hops[i])))

    def pass_on(i):
        tell(ready.at[i], (-hops[i], hops[i]))

    for border in (pl.ds(0, reach), pl.ds(reach + n, reach)):
        part_one[border] = jnp.zeros((reach, half, LANES), F32)
    for d in offs:

        @pl.when(jnp.logical_not(there(d)))
        def _():
            for buf in (fa, cx, vx, hx):
                buf[pl.ds(depth + planes * d, planes)] = jnp.zeros((planes, rows, LANES), F32)
            for par in range(2):
                land[par, at[d]] = jnp.zeros((planes, rows, LANES), F32)
            surf_all[reach + d] = jnp.zeros((1, surf_here), jnp.int32)

    for c in loads[:7]:
        c.wait()
    own = pl.ds(depth, planes)
    kind = kind_ref[grp]
    gas = jnp.where(kind == 0, 1.0, 0.0).astype(F32)
    gain_t = jnp.where(kind == 0, 0.5, 0.25).astype(F32)
    gain_f = jnp.where(kind == 0, -0.25, 0.25).astype(F32)
    away_t = jnp.where(kind == 0, 0.25, 0.5).astype(F32)
    away_f = jnp.where(kind == 0, 0.25, -0.25).astype(F32)
    fetch = ((field_ref, fa, None), (cond_ref, cx, None), (vel_ref, vx, gas), (heat_ref, hx, 0.5 * gas))

    def unfold(b, carry):
        chunk = pl.ds(pl.multiple_of(b * 8 * LANES, LANES), 8 * LANES)
        for src, dst, scale in fetch:
            x = src[:, chunk]
            if scale is not None:
                x = x * scale
            for p in range(planes):
                dst[depth + p, pl.ds(pl.multiple_of(b * 8, 8), 8), :] = jnp.concatenate(
                    [x[p : p + 1, i * LANES : (i + 1) * LANES] for i in range(8)], axis=0
                )
        return carry

    lax.fori_loop(0, rows // 8, unfold, 0)
    pl.semaphore_wait(barrier, among(offs) + groups - 1)

    def send_planes(buf, lo, hi, to, j):
        slot = -to
        shift = depth - (depth + planes * slot)
        return rcopy(
            buf.at[pl.ds(lo + shift, hi - lo)],
            buf.at[pl.ds(lo, hi - lo)],
            set_send.at[j, at[to]],
            set_recv.at[j, at[slot]],
            {"sub": me + to},
        )

    def first_copies(to):
        base = depth - planes * to
        lo, hi = max(base, depth - near), min(base + planes, depth + planes + near)
        out = [send_planes(fa, lo, hi, to, 0)]
        lo, hi = max(base, depth - near + 1), min(base + planes, depth + planes + near - 1)
        if hi > lo:
            out += [send_planes(buf, lo, hi, to, j + 1) for j, buf in enumerate((cx, vx, hx))]
        return out

    def rest_copies(to, which):
        base = depth - planes * to
        lo, hi = max(base, 1), min(base + planes, ext - 1)
        if to == 1:
            hi = min(hi, depth - near + 1)
        if to == -1:
            lo = max(lo, depth + planes + near - 1)
        if hi <= lo:
            return []
        return [send_planes((cx, vx, hx)[j], lo, hi, to, j + 4) for j in which]

    sides = ((-1, 1, lax.rem(me, 2) == 0), (1, -1, lax.rem(me, 2) == 1))
    assert reach == 2 and near == planes == 2 and n % 2 == 0

    def when(mine, d, act):
        @pl.when(jnp.logical_and(mine, there(d)))
        def _():
            act()

    def rest_each(which, act):
        for x, p, mine in sides:
            for d in (x, p, 2 * p):
                when(mine, d, lambda d=d: act(rest_copies(d, which)))

    def handed_rest(x, p):
        plane = depth - 1 if x < 0 else depth + planes
        return [
            rcopy(
                buf.at[pl.ds(plane, 1)],
                buf.at[pl.ds(plane - p * planes, 1)],
                set_send.at[j + 4, at[x - p]],
                set_recv.at[j + 4, at[x - p]],
                {"sub": me + p},
            )
            for j, buf in enumerate((cx, vx, hx))
        ]

    def handed_halo(par, x, p):
        return rcopy(
            land.at[par, at[x]],
            land.at[par, at[x - p]],
            halo_send.at[par, at[x - p]],
            halo_recv.at[par, at[x - p]],
            {"sub": me + p},
        )

    def surf_copies(to):
        return [
            rcopy(
                surf_all.at[reach],
                surf_all.at[reach - to],
                set_send.at[7, at[to]],
                set_recv.at[7, at[-to]],
                {"sub": me + to},
            )
        ]

    def mid_copy(to):
        return rcopy(
            fa.at[own],
            land.at[1, at[-to]],
            set_send.at[8, at[to]],
            set_recv.at[8, at[-to]],
            {"sub": me + to},
        )

    def each(ds, act):
        for d in ds:

            @pl.when(there(d))
            def _():
                act(d)

    def starts(copies):
        for c in copies:
            c.start()

    def arrivals(copies):
        for c in copies:
            c.wait_recv()

    def departures(copies):
        for c in copies:
            c.wait_send()

    beside = (-1, 1)
    each(beside, lambda d: starts(first_copies(d)))
    pass_on(0)

    partner = partner_ref[grp]
    count = count_ref[0, me]
    block_row = iota((blocks, LANES), 0)
    lane_row = iota((LANES, LANES), 0)

    def block_of(x):
        return lax.shift_right_logical(x, jnp.full(x.shape, LANES.bit_length() - 1, jnp.int32))

    def lane_of(x):
        return lax.bitwise_and(x, jnp.full(x.shape, LANES - 1, jnp.int32))

    def hot(mask):
        return jnp.where(mask, 1.0, 0.0).astype(F32)

    for c in loads[7:]:
        c.wait()
    for s in range(cap):
        lanes = pl.ds(s * LANES, LANES)
        oh_cent[:, lanes] = hot(lane_row == lane_of(cent_ref[s : s + 1, :])).astype(BF16)
        oh_targ[:, lanes] = hot(block_row == block_of(targ_ref[s : s + 1, :])).astype(BF16)
        hot_targ[lanes, :] = hot(lane_row == lane_of(targ_ref[s : s + 1, :])).T.astype(BF16)
        live = jnp.where(s < count, 1.0, 0.0).astype(F32)
        hi, lo = split((maps[s] * live).T)
        maps2[s, :, pl.ds(0, LANES)] = hi.astype(BF16)
        maps2[s, :, pl.ds(LANES, LANES)] = lo.astype(BF16)

    cell_row = iota((rows, surf_here), 0)

    def plane_of(cell):
        return sum((cell >= p * rows * LANES).astype(jnp.int32) for p in range(1, planes))

    def row_of(cell):
        return block_of(cell) - plane_of(cell) * rows

    def spot_of(cell):
        return plane_of(cell) * LANES + lane_of(cell)

    def hot_rows(j):
        oh_surf[j] = hot(cell_row == row_of(surf_all[j])).astype(BF16)
        spot = spot_of(surf_all[j])
        for i in range(half):
            cols = slice(i * LANES, (i + 1) * LANES)
            for p in range(planes):
                hot_surf[j, cols, pl.ds(p * LANES, LANES)] = hot(lane_row + p * LANES == spot[:, cols]).T.astype(BF16)

    hot_rows(reach)
    oh_lane[...] = hot(iota((planes * LANES, surf_here), 0) == spot_of(surf_all[reach])).astype(BF16)

    block_of_slot = iota((blocks, cap * LANES), 0)

    def step(src, dst, k):
        for z in range(k + 1, ext - k - 1):
            c = src[z]
            dn = src[z - 1]
            lap = src[z + 1] + dn + in_plane(c) - 6.0 * c
            dst[z] = c + cx[z] * lap - vx[z] * (c - dn) + hx[z] * (1.0 + jnp.tanh(c))

    def spread(slot, inc):
        lhs = []
        for x in split(inc):
            wide = [jnp.broadcast_to(x[i : i + 1, :], (16, LANES)).astype(BF16) for i in range(half)]
            wide = jnp.concatenate(wide, axis=1)
            lhs += [oh_surf[slot, r * 16 : (r + 1) * 16, :] * wide for r in range(rows // 16)]
        r = dot_nn(jnp.concatenate(lhs, axis=0), hot_surf[slot])
        r = r[:rows] + r[rows:]
        return [r[:, p * LANES : (p + 1) * LANES] for p in range(planes)]

    def halo_copy(par, to, slot):
        return rcopy(
            fa.at[own],
            land.at[par, at[slot]],
            halo_send.at[par, at[to]],
            halo_recv.at[par, at[slot]],
            {"sub": me + to},
        )

    upper = 2 * me >= n

    def ex_copy(two, par, k, peer, sender):
        src, dst = (exp_two, land_two.at[k - 1, sender]) if two else (exp_one, land_one.at[par, k - 1, sender])
        return rcopy(
            src,
            dst,
            ex_send.at[par, k - 1, peer],
            ex_recv.at[par, k - 1, sender],
            {"grp": lax.rem(grp + k, groups), "sub": peer},
        )

    def rs_copy(two, par, k, sender):
        peer = lax.rem(me + k, n)
        if two:
            src, dst = part_two.at[peer], rs_two.at[sender]
        else:
            src, dst = part_one.at[pl.ds(peer, span)], rs_one.at[par, sender]
        return rcopy(src, dst, rs_send.at[par, k - 1], rs_recv.at[par, k - 1], {"sub": peer})

    def sample(values):
        lhs = []
        for x in values:
            lhs += split(jnp.concatenate(x, axis=1))
        got = dot_nn(jnp.concatenate(lhs, axis=0).astype(BF16), oh_lane[...])
        hit = cell_row == row_of(surf_all[reach])
        out = []
        for q in range(len(values)):
            v = got[2 * q * rows : (2 * q + 1) * rows] + got[(2 * q + 1) * rows : (2 * q + 2) * rows]
            out.append(jnp.sum(jnp.where(hit, v, 0.0), axis=0, keepdims=True))
        return out

    def patches(srcs):
        count_q = len(srcs)
        lhs = jnp.concatenate([x for v in srcs for x in split(v)], axis=0).astype(BF16)
        vals = dot_nn(lhs, oh_cent[...])
        cent = jnp.concatenate([cent_ref[s : s + 1, :] for s in range(cap)], axis=1)
        hit = block_of_slot == block_of(cent)
        cv = []
        for q in range(count_q):
            v = vals[2 * q * blocks : (2 * q + 1) * blocks] + vals[(2 * q + 1) * blocks : (2 * q + 2) * blocks]
            cv.append(jnp.sum(jnp.where(hit, v, 0.0), axis=0, keepdims=True))
        c4 = jnp.concatenate([x for v in cv for x in split(v)], axis=0).astype(BF16)
        contrib = []
        for s in range(cap):
            r = dot_nn(c4[:, s * LANES : (s + 1) * LANES], maps2[s])
            contrib.append(r[:, :LANES] + r[:, LANES:])
        r = jnp.concatenate(contrib, axis=1)
        rows_of = []
        for q in range(count_q):
            for x in split(r[2 * q : 2 * q + 1] + r[2 * q + 1 : 2 * q + 2]):
                wide = jnp.broadcast_to(x, (16, cap * LANES)).astype(BF16)
                rows_of += [oh_targ[b * 16 : (b + 1) * 16, :] * wide for b in range(blocks // 16)]
        acc = dot_nn(jnp.concatenate(rows_of, axis=0), hot_targ[...])
        return [
            acc[2 * q * blocks : (2 * q + 1) * blocks] + acc[(2 * q + 1) * blocks : (2 * q + 2) * blocks]
            for q in range(count_q)
        ]

    def advance():
        for k in range(STEPS):
            step(pair[k % 2], pair[(k + 1) % 2], k)

    def surface():
        temp = [fa[depth + p] for p in range(planes)]
        flux = [cx[depth + p] * (4.0 * t - in_plane(t)) for p, t in enumerate(temp)]
        return temp, flux

    def exchange(two, par):
        for j in range(n):
            peer = jnp.where(upper, j, n - 1 - j)
            for k in range(1, groups):
                ex_copy(two, par, k, peer, me).start()

    def chosen(two, par):
        for j in range(n):
            for k in range(1, groups):
                ex_copy(two, par, k, me, j).wait_recv()
        out = None
        for k in range(1, groups):
            got = land_two[k - 1] if two else land_one[par, k - 1]
            source = lax.rem(grp + groups - k, groups)
            out = got if out is None else jnp.where(partner == source, got, out)
        return out

    def finish(two, par):
        for j in range(n):
            for k in range(1, groups):
                ex_copy(two, par, k, j, me).wait_send()
        for k in range(1, n):
            rs_copy(two, par, k, me).wait_send()

    def couple(it, carry):
        par = lax.rem(it, 2)
        first = it == 0

        @pl.when(jnp.logical_not(first))
        def _():
            advance()

        temp, flux = surface()
        mixed = sample([[away_t * t + away_f * f for t, f in zip(temp, flux)]])[0]
        for i in range(half):
            exp_one[i : i + 1, :] = mixed[:, i * LANES : (i + 1) * LANES]
        exchange(False, par)
        for x, p, mine in sides:
            for d in (x, p, 2 * p):
                when(mine, d, lambda d=d: halo_copy(par, d, -d).start())

        here = sample([temp])[0]
        for i in range(half):
            own_temp[i : i + 1, :] = here[:, i * LANES : (i + 1) * LANES]

        srcs = chosen(False, par)
        part = patches([srcs.reshape(blocks, LANES)])[0].reshape(n, half, LANES)
        mine = iota((n, half, LANES), 0) == me
        part_one[pl.ds(reach, n)] = part - jnp.where(mine, gain_t * own_temp[...], 0.0)
        for k in range(1, n):
            rs_copy(False, par, k, me).start()
        for x, p, mine in sides:

            def hand_on(x=x, p=p):
                halo_copy(par, -x, x).wait_recv()
                handed_halo(par, x, p).start()

            when(mine, x, hand_on)

        @pl.when(first)
        def _():
            rest_each((2,), starts)

        rs_one[par, me] = part_one[pl.ds(me, span)]

        @pl.when(first)
        def _():
            each(offs, lambda d: arrivals(surf_copies(-d)))
            for d in offs:
                hot_rows(d + reach)

        for x, p, mine in sides:
            for d in (x, p, 2 * p):
                when(mine, d, lambda d=d: halo_copy(par, d, -d).wait_send())
            when(mine, x, lambda x=x, p=p: handed_halo(par, x, p).wait_send())
            for d in (p, 2 * p, 2 * x):
                when(mine, d, lambda d=d: halo_copy(par, -d, d).wait_recv())

        for k in range(1, n):
            rs_copy(False, par, k, lax.rem(me + n - k, n)).wait_recv()
        inc = rs_one[par, 0]
        for j in range(1, n):
            inc = inc + rs_one[par, j]
        sums = [spread(slot, inc[slot]) for slot in range(span)]
        for p in range(planes):
            fa[depth + p] = fa[depth + p] + sums[reach][p]
        for d in offs:
            for p in range(planes):
                fa[depth + planes * d + p] = land[par, at[d], p] + sums[d + reach][p]

        @pl.when(first)
        def _():
            each(offs, lambda d: arrivals(rest_copies(-d, (0, 1, 2))))
            each(offs, lambda d: departures(surf_copies(d)))
            rest_each((0, 1, 2), departures)
            for x, p, mine in sides:
                when(mine, x, lambda x=x, p=p: departures(handed_rest(x, p)))

        finish(False, par)
        return carry

    def final():
        par = (COUPLE - 1) % 2
        advance()
        got = sample(surface())
        for q in range(2):
            for i in range(half):
                exp_two[q * half + i : q * half + i + 1, :] = got[q][:, i * LANES : (i + 1) * LANES]
        exchange(True, par)
        src = chosen(True, par)
        parts = patches([src[:, q * half : (q + 1) * half].reshape(blocks, LANES) for q in range(2)])
        part_two[...] = jnp.concatenate([x.reshape(n, half, LANES) for x in parts], axis=1)
        for k in range(1, n):
            rs_copy(True, par, k, me).start()
        rs_two[me] = part_two[me]
        for k in range(1, n):
            rs_copy(True, par, k, lax.rem(me + n - k, n)).wait_recv()
        iface = rs_two[0]
        for j in range(1, n):
            iface = iface + rs_two[j]
        iface_ref[...] = iface
        inc = gain_t * (iface[:half] - exp_two[:half]) + gain_f * iface[half:]
        for p, x in enumerate(spread(reach, inc)):
            out_ref[p] = fa[depth + p] + x
        finish(True, par)

    pair = (fa, fb)
    hear(0)
    for i in range(1, len(hops)):
        pass_on(i)
        if i < len(hops) - 1:
            hear(i)
    each(beside, lambda d: arrivals(first_copies(-d)))
    if len(hops) > 1:
        hear(len(hops) - 1)
    for k in range(1, groups):
        signal(ready.at[len(hops)], {"grp": lax.rem(grp + k, groups)})
    each(beside, lambda d: departures(first_copies(d)))
    for k in range(near):
        step(pair[k % 2], pair[(k + 1) % 2], depth - near + k)
    each(beside, lambda d: mid_copy(d).start())
    each(offs, lambda d: starts(surf_copies(d)))
    rest_each((0, 1), starts)
    for x, p, mine in sides:
        when(mine, x, lambda x=x, p=p: starts(handed_rest(x, p)))
    each(beside, lambda d: mid_copy(-d).wait_recv())
    for d in beside:
        fa[pl.ds(depth + planes * d, planes)] = land[1, at[d]]
    each(beside, lambda d: mid_copy(d).wait_send())
    for k in range(near):
        step(pair[k % 2], pair[(k + 1) % 2], depth - near + k)

    pl.semaphore_wait(ready.at[len(hops)], groups - 1)
    lax.fori_loop(0, COUPLE - 1, couple, 0)
    final()


def unpack(planes_ref, rows_ref, out_ref, iface_ref):
    planes, rows, _ = planes_ref.shape
    half = rows_ref.shape[0] // 2
    for b in range(rows // 8):
        rws = []
        for p in range(planes):
            x = planes_ref[p, b * 8 : (b + 1) * 8, :]
            rws.append(jnp.concatenate([x[i : i + 1, :] for i in range(8)], axis=1))
        out_ref[0, :, b * 8 * LANES : (b + 1) * 8 * LANES] = jnp.concatenate(rws, axis=0)
    for q in range(2):
        for i in range(half):
            iface_ref[0, q : q + 1, i * LANES : (i + 1) * LANES] = rows_ref[q * half + i : q * half + i + 1, :]


def local_of(n, groups):
    def local(
        initial_field,
        conduct,
        velocity,
        heat_release,
        group_kind,
        partner,
        surface_cell,
        patch_count,
        patch_centres,
        patch_targets,
        patch_maps,
    ):
        _, planes, cells = initial_field.shape
        rows = cells // LANES
        surf_here = surface_cell.shape[1]
        cap = patch_centres.shape[1]
        reach = -(-STEPS // planes)
        ext = planes + 2 * reach * planes
        half = surf_here // LANES
        vmem = pl.BlockSpec(memory_space=pltpu.VMEM)
        dma = pltpu.SemaphoreType.DMA
        nd = 2 * reach
        scratch = [
            pltpu.VMEM((ext, rows, LANES), F32),
            pltpu.VMEM((ext, rows, LANES), F32),
            pltpu.VMEM((ext, rows, LANES), F32),
            pltpu.VMEM((ext, rows, LANES), F32),
            pltpu.VMEM((ext, rows, LANES), F32),
            pltpu.VMEM((2, nd, planes, rows, LANES), F32),
            pltpu.VMEM((nd + 1, 1, surf_here), jnp.int32),
            pltpu.VMEM((nd + 1, rows, surf_here), BF16),
            pltpu.VMEM((nd + 1, surf_here, planes * LANES), BF16),
            pltpu.VMEM((planes * LANES, surf_here), BF16),
            pltpu.VMEM((LANES, cap * LANES), BF16),
            pltpu.VMEM((n * half, cap * LANES), BF16),
            pltpu.VMEM((cap * LANES, LANES), BF16),
            pltpu.VMEM((cap, LANES, 2 * LANES), BF16),
            pltpu.VMEM((half, LANES), F32),
            pltpu.VMEM((2 * half, LANES), F32),
            pltpu.VMEM((half, LANES), F32),
            pltpu.VMEM((2, groups - 1, n, half, LANES), F32),
            pltpu.VMEM((groups - 1, n, 2 * half, LANES), F32),
            pltpu.VMEM((n + nd, half, LANES), F32),
            pltpu.VMEM((n, 2 * half, LANES), F32),
            pltpu.VMEM((2, n, nd + 1, half, LANES), F32),
            pltpu.VMEM((n, 2 * half, LANES), F32),
            dma((9, nd)),
            dma((9, nd)),
            dma((2, groups - 1, n)),
            dma((2, groups - 1, n)),
            dma((2, n - 1)),
            dma((2, n - 1)),
            dma((2, nd)),
            dma((2, nd)),
            pltpu.SMEM(group_kind.shape, jnp.int32),
            pltpu.SMEM(partner.shape, jnp.int32),
            pltpu.SMEM(patch_count.shape, jnp.int32),
            pltpu.VMEM((planes, cells), F32),
            pltpu.VMEM((planes, cells), F32),
            pltpu.VMEM((planes, cells), F32),
            pltpu.VMEM((planes, cells), F32),
            pltpu.VMEM((cap, LANES), jnp.int32),
            pltpu.VMEM((cap, LANES), jnp.int32),
            pltpu.VMEM((cap, LANES, LANES), F32),
            dma((11,)),
            pltpu.SemaphoreType.REGULAR((n.bit_length() + 1,)),
        ]

        def body(*refs):
            kernel(n, groups, *refs)

        lying, tops = pl.pallas_call(
            body,
            name="coupled",
            out_shape=(
                pltpu.VMEM((planes, rows, LANES), F32),
                pltpu.VMEM((2 * half, LANES), F32),
            ),
            in_specs=[pl.BlockSpec(memory_space=pltpu.HBM)] * 11,
            out_specs=(vmem, vmem),
            scratch_shapes=scratch,
            compiler_params=pltpu.CompilerParams(
                collective_id=0, has_side_effects=True, vmem_limit_bytes=56 * 1024 * 1024
            ),
        )(
            group_kind,
            partner,
            patch_count,
            initial_field,
            conduct,
            velocity,
            heat_release,
            surface_cell,
            patch_centres[0],
            patch_targets[0],
            patch_maps[0],
        )
        return pl.pallas_call(
            unpack,
            name="unpack",
            out_shape=(
                jax.ShapeDtypeStruct(initial_field.shape, F32),
                jax.ShapeDtypeStruct((1, 2, surf_here), F32),
            ),
            in_specs=[vmem] * 2,
            out_specs=(vmem, vmem),
        )(*(pltpu.with_memory_space_constraint(x, pltpu.VMEM) for x in (lying, tops)))

    return local


def solution(mesh):
    placed = (
        P("grp", "sub", None),
        P("grp", "sub", None),
        P("grp", "sub", None),
        P("grp", "sub", None),
        P(),
        P(),
        P("grp", "sub"),
        P("grp", None),
        P("grp", "sub", None),
        P("grp", "sub", None),
        P("grp", "sub", None, None),
    )
    return jax.shard_map(
        local_of(mesh.shape["sub"], mesh.shape["grp"]),
        mesh=mesh,
        in_specs=placed,
        out_specs=(P("grp", "sub", None), P("grp", None, "sub")),
        check_vma=False,
    )
```

```python
import jax
import jax.numpy as jnp
from jax import lax
from jax.experimental import pallas as pl
from jax.experimental.pallas import tpu as pltpu
from jax.sharding import PartitionSpec as P

STEPS = 4
COUPLE = 4
LANES = 128
F32 = jnp.float32
BF16 = jnp.bfloat16


def split(x):
    hi = x.astype(BF16).astype(F32)
    return hi, x - hi


def dot_nt(a, b):
    return lax.dot_general(a, b, (((1,), (1,)), ((), ())), preferred_element_type=F32)


def dot_nn(a, b):
    return lax.dot_general(a, b, (((1,), (0,)), ((), ())), preferred_element_type=F32)


def iota(shape, dim):
    return lax.broadcasted_iota(jnp.int32, shape, dim)


def in_plane(c):
    rows, cols = c.shape
    return (
        pltpu.roll(c, 1, 0)
        + pltpu.roll(c, rows - 1, 0)
        + pltpu.roll(c, 1, 1)
        + pltpu.roll(c, cols - 1, 1)
    )


def kernel(
    n,
    groups,
    kind_hbm,
    partner_hbm,
    count_hbm,
    field_hbm,
    cond_hbm,
    vel_hbm,
    heat_hbm,
    surf_hbm,
    cent_hbm,
    targ_hbm,
    maps_hbm,
    out_ref,
    iface_ref,
    fa,
    fb,
    cx,
    vx,
    hx,
    land,
    surf_all,
    oh_surf,
    hot_surf,
    oh_lane,
    oh_cent,
    oh_targ,
    hot_targ,
    maps2,
    exp_one,
    exp_two,
    own_temp,
    land_one,
    land_two,
    part_one,
    part_two,
    rs_one,
    rs_two,
    set_send,
    set_recv,
    ex_send,
    ex_recv,
    rs_send,
    rs_recv,
    halo_send,
    halo_recv,
    kind_ref,
    partner_ref,
    count_ref,
    field_ref,
    cond_ref,
    vel_ref,
    heat_ref,
    cent_ref,
    targ_ref,
    maps,
    load_sem,
    ready,
):
    planes = field_ref.shape[0]
    rows = fa.shape[1]
    near = STEPS // 2
    assert near % 2 == 0 and near <= planes
    surf_here = surf_all.shape[2]
    cap = cent_ref.shape[0]
    reach = -(-STEPS // planes)
    depth = reach * planes
    ext = planes + 2 * depth
    offs = [d for d in range(-reach, reach + 1) if d != 0]
    at = {d: i for i, d in enumerate(offs)}
    half = surf_here // LANES
    span = 2 * reach + 1
    blocks = n * half
    me = lax.axis_index("sub")
    grp = lax.axis_index("grp")

    def there(d):
        return jnp.logical_and(me + d >= 0, me + d < n)

    def rcopy(src, dst, ss, rs, dev):
        return pltpu.make_async_remote_copy(
            src_ref=src,
            dst_ref=dst,
            send_sem=ss,
            recv_sem=rs,
            device_id=dev,
            device_id_type=pl.DeviceIdType.MESH,
        )

    pairs = (
        (kind_hbm, kind_ref),
        (partner_hbm, partner_ref),
        (count_hbm, count_ref),
        (field_hbm.at[0], field_ref),
        (cond_hbm.at[0], cond_ref),
        (vel_hbm.at[0], vel_ref),
        (heat_hbm.at[0], heat_ref),
        (surf_hbm, surf_all.at[reach]),
        (cent_hbm, cent_ref),
        (targ_hbm, targ_ref),
        (maps_hbm, maps),
    )
    loads = [pltpu.make_async_copy(src, dst, load_sem.at[i]) for i, (src, dst) in enumerate(pairs)]
    for c in loads:
        c.start()

    def signal(sem, dev):
        pl.semaphore_signal(sem, inc=1, device_id=dev, device_id_type=pl.DeviceIdType.MESH)

    def among(ds):
        return sum(there(d).astype(jnp.int32) for d in ds)

    def tell(sem, ds):
        for d in ds:

            @pl.when(there(d))
            def _():
                signal(sem, {"sub": me + d})

    barrier = pltpu.get_barrier_semaphore()
    tell(barrier, offs)
    for k in range(1, groups):
        signal(barrier, {"grp": lax.rem(grp + k, groups)})
    hops = [reach]
    while 2 * hops[-1] < n:
        hops.append(2 * hops[-1])

    def hear(i):
        pl.semaphore_wait(ready.at[i], among((-hops[i], hops[i])))

    def pass_on(i):
        tell(ready.at[i], (-hops[i], hops[i]))

    for border in (pl.ds(0, reach), pl.ds(reach + n, reach)):
        part_one[border] = jnp.zeros((reach, half, LANES), F32)
    for d in offs:

        @pl.when(jnp.logical_not(there(d)))
        def _():
            for buf in (fa, cx, vx, hx):
                buf[pl.ds(depth + planes * d, planes)] = jnp.zeros((planes, rows, LANES), F32)
            for par in range(2):
                land[par, at[d]] = jnp.zeros((planes, rows, LANES), F32)
            surf_all[reach + d] = jnp.zeros((1, surf_here), jnp.int32)

    for c in loads[:7]:
        c.wait()
    own = pl.ds(depth, planes)
    kind = kind_ref[grp]
    gas = jnp.where(kind == 0, 1.0, 0.0).astype(F32)
    gain_t = jnp.where(kind == 0, 0.5, 0.25).astype(F32)
    gain_f = jnp.where(kind == 0, -0.25, 0.25).astype(F32)
    away_t = jnp.where(kind == 0, 0.25, 0.5).astype(F32)
    away_f = jnp.where(kind == 0, 0.25, -0.25).astype(F32)
    fetch = ((field_ref, fa, None), (cond_ref, cx, None), (vel_ref, vx, gas), (heat_ref, hx, 0.5 * gas))

    def unfold(b, carry):
        chunk = pl.ds(pl.multiple_of(b * 8 * LANES, LANES), 8 * LANES)
        for src, dst, scale in fetch:
            x = src[:, chunk]
            if scale is not None:
                x = x * scale
            for p in range(planes):
                dst[depth + p, pl.ds(pl.multiple_of(b * 8, 8), 8), :] = jnp.concatenate(
                    [x[p : p + 1, i * LANES : (i + 1) * LANES] for i in range(8)], axis=0
                )
        return carry

    lax.fori_loop(0, rows // 8, unfold, 0)
    pl.semaphore_wait(barrier, among(offs) + groups - 1)

    def send_planes(buf, lo, hi, to, j):
        slot = -to
        shift = depth - (depth + planes * slot)
        return rcopy(
            buf.at[pl.ds(lo + shift, hi - lo)],
            buf.at[pl.ds(lo, hi - lo)],
            set_send.at[j, at[to]],
            set_recv.at[j, at[slot]],
            {"sub": me + to},
        )

    def first_copies(to):
        base = depth - planes * to
        lo, hi = max(base, depth - near), min(base + planes, depth + planes + near)
        out = [send_planes(fa, lo, hi, to, 0)]
        lo, hi = max(base, depth - near + 1), min(base + planes, depth + planes + near - 1)
        if hi > lo:
            out += [send_planes(buf, lo, hi, to, j + 1) for j, buf in enumerate((cx, vx, hx))]
        return out

    def rest_copies(to, which):
        base = depth - planes * to
        lo, hi = max(base, 1), min(base + planes, ext - 1)
        if to == 1:
            hi = min(hi, depth - near + 1)
        if to == -1:
            lo = max(lo, depth + planes + near - 1)
        if hi <= lo:
            return []
        return [send_planes((cx, vx, hx)[j], lo, hi, to, j + 4) for j in which]

    sides = ((-1, 1, lax.rem(me, 2) == 0), (1, -1, lax.rem(me, 2) == 1))
    assert reach == 2 and near == planes == 2 and n % 2 == 0

    def when(mine, d, act):
        @pl.when(jnp.logical_and(mine, there(d)))
        def _():
            act()

    def rest_each(which, act):
        for x, p, mine in sides:
            for d in (x, p, 2 * p):
                when(mine, d, lambda d=d: act(rest_copies(d, which)))

    def handed_rest(x, p):
        plane = depth - 1 if x < 0 else depth + planes
        return [
            rcopy(
                buf.at[pl.ds(plane, 1)],
                buf.at[pl.ds(plane - p * planes, 1)],
                set_send.at[j + 4, at[x - p]],
                set_recv.at[j + 4, at[x - p]],
                {"sub": me + p},
            )
            for j, buf in enumerate((cx, vx, hx))
        ]

    def handed_halo(par, x, p):
        return rcopy(
            land.at[par, at[x]],
            land.at[par, at[x - p]],
            halo_send.at[par, at[x - p]],
            halo_recv.at[par, at[x - p]],
            {"sub": me + p},
        )

    def surf_copies(to):
        return [
            rcopy(
                surf_all.at[reach],
                surf_all.at[reach - to],
                set_send.at[7, at[to]],
                set_recv.at[7, at[-to]],
                {"sub": me + to},
            )
        ]

    def mid_copy(to):
        return rcopy(
            fa.at[own],
            land.at[1, at[-to]],
            set_send.at[8, at[to]],
            set_recv.at[8, at[-to]],
            {"sub": me + to},
        )

    def each(ds, act):
        for d in ds:

            @pl.when(there(d))
            def _():
                act(d)

    def starts(copies):
        for c in copies:
            c.start()

    def arrivals(copies):
        for c in copies:
            c.wait_recv()

    def departures(copies):
        for c in copies:
            c.wait_send()

    beside = (-1, 1)
    each(beside, lambda d: starts(first_copies(d)))
    pass_on(0)

    partner = partner_ref[grp]
    count = count_ref[0, me]
    block_row = iota((blocks, LANES), 0)
    lane_row = iota((LANES, LANES), 0)

    def block_of(x):
        return lax.shift_right_logical(x, jnp.full(x.shape, LANES.bit_length() - 1, jnp.int32))

    def lane_of(x):
        return lax.bitwise_and(x, jnp.full(x.shape, LANES - 1, jnp.int32))

    def hot(mask):
        return jnp.where(mask, 1.0, 0.0).astype(F32)

    for c in loads[7:]:
        c.wait()
    for s in range(cap):
        lanes = pl.ds(s * LANES, LANES)
        oh_cent[:, lanes] = hot(lane_row == lane_of(cent_ref[s : s + 1, :])).astype(BF16)
        oh_targ[:, lanes] = hot(block_row == block_of(targ_ref[s : s + 1, :])).astype(BF16)
        hot_targ[lanes, :] = hot(lane_row == lane_of(targ_ref[s : s + 1, :])).T.astype(BF16)
        live = jnp.where(s < count, 1.0, 0.0).astype(F32)
        hi, lo = split((maps[s] * live).T)
        maps2[s, :, pl.ds(0, LANES)] = hi.astype(BF16)
        maps2[s, :, pl.ds(LANES, LANES)] = lo.astype(BF16)

    cell_row = iota((rows, surf_here), 0)

    def plane_of(cell):
        return sum((cell >= p * rows * LANES).astype(jnp.int32) for p in range(1, planes))

    def row_of(cell):
        return block_of(cell) - plane_of(cell) * rows

    def spot_of(cell):
        return plane_of(cell) * LANES + lane_of(cell)

    def hot_rows(j):
        oh_surf[j] = hot(cell_row == row_of(surf_all[j])).astype(BF16)
        spot = spot_of(surf_all[j])
        for i in range(half):
            cols = slice(i * LANES, (i + 1) * LANES)
            for p in range(planes):
                hot_surf[j, cols, pl.ds(p * LANES, LANES)] = hot(lane_row + p * LANES == spot[:, cols]).T.astype(BF16)

    hot_rows(reach)
    oh_lane[...] = hot(iota((planes * LANES, surf_here), 0) == spot_of(surf_all[reach])).astype(BF16)

    block_of_slot = iota((blocks, cap * LANES), 0)

    def step(src, dst, k):
        for z in range(k + 1, ext - k - 1):
            c = src[z]
            dn = src[z - 1]
            lap = src[z + 1] + dn + in_plane(c) - 6.0 * c
            dst[z] = c + cx[z] * lap - vx[z] * (c - dn) + hx[z] * (1.0 + jnp.tanh(c))

    def spread(slot, inc):
        lhs = []
        for x in split(inc):
            wide = [jnp.broadcast_to(x[i : i + 1, :], (16, LANES)).astype(BF16) for i in range(half)]
            wide = jnp.concatenate(wide, axis=1)
            lhs += [oh_surf[slot, r * 16 : (r + 1) * 16, :] * wide for r in range(rows // 16)]
        r = dot_nn(jnp.concatenate(lhs, axis=0), hot_surf[slot])
        r = r[:rows] + r[rows:]
        return [r[:, p * LANES : (p + 1) * LANES] for p in range(planes)]

    def halo_copy(par, to, slot):
        return rcopy(
            fa.at[own],
            land.at[par, at[slot]],
            halo_send.at[par, at[to]],
            halo_recv.at[par, at[slot]],
            {"sub": me + to},
        )

    upper = 2 * me >= n

    def ex_copy(two, par, k, peer, sender):
        src, dst = (exp_two, land_two.at[k - 1, sender]) if two else (exp_one, land_one.at[par, k - 1, sender])
        return rcopy(
            src,
            dst,
            ex_send.at[par, k - 1, peer],
            ex_recv.at[par, k - 1, sender],
            {"grp": lax.rem(grp + k, groups), "sub": peer},
        )

    def peers():
        return [lax.rem(me + jnp.where(upper, k, n - k), n) for k in range(1, n)]

    def rs_copy(two, par, peer, sender):
        if two:
            src, dst = part_two.at[peer], rs_two.at[sender]
        else:
            src, dst = part_one.at[pl.ds(peer, span)], rs_one.at[par, sender]
        return rcopy(src, dst, rs_send.at[par, peer], rs_recv.at[par, sender], {"sub": peer})

    def sample(values):
        lhs = []
        for x in values:
            lhs += split(jnp.concatenate(x, axis=1))
        got = dot_nn(jnp.concatenate(lhs, axis=0).astype(BF16), oh_lane[...])
        hit = cell_row == row_of(surf_all[reach])
        out = []
        for q in range(len(values)):
            v = got[2 * q * rows : (2 * q + 1) * rows] + got[(2 * q + 1) * rows : (2 * q + 2) * rows]
            out.append(jnp.sum(jnp.where(hit, v, 0.0), axis=0, keepdims=True))
        return out

    def patches(srcs):
        count_q = len(srcs)
        lhs = jnp.concatenate([x for v in srcs for x in split(v)], axis=0).astype(BF16)
        vals = dot_nn(lhs, oh_cent[...])
        cent = jnp.concatenate([cent_ref[s : s + 1, :] for s in range(cap)], axis=1)
        hit = block_of_slot == block_of(cent)
        cv = []
        for q in range(count_q):
            v = vals[2 * q * blocks : (2 * q + 1) * blocks] + vals[(2 * q + 1) * blocks : (2 * q + 2) * blocks]
            cv.append(jnp.sum(jnp.where(hit, v, 0.0), axis=0, keepdims=True))
        c4 = jnp.concatenate([x for v in cv for x in split(v)], axis=0).astype(BF16)
        contrib = []
        for s in range(cap):
            r = dot_nn(c4[:, s * LANES : (s + 1) * LANES], maps2[s])
            contrib.append(r[:, :LANES] + r[:, LANES:])
        r = jnp.concatenate(contrib, axis=1)
        rows_of = []
        for q in range(count_q):
            for x in split(r[2 * q : 2 * q + 1] + r[2 * q + 1 : 2 * q + 2]):
                wide = jnp.broadcast_to(x, (16, cap * LANES)).astype(BF16)
                rows_of += [oh_targ[b * 16 : (b + 1) * 16, :] * wide for b in range(blocks // 16)]
        acc = dot_nn(jnp.concatenate(rows_of, axis=0), hot_targ[...])
        return [
            acc[2 * q * blocks : (2 * q + 1) * blocks] + acc[(2 * q + 1) * blocks : (2 * q + 2) * blocks]
            for q in range(count_q)
        ]

    def advance():
        for k in range(STEPS):
            step(pair[k % 2], pair[(k + 1) % 2], k)

    def surface():
        temp = [fa[depth + p] for p in range(planes)]
        flux = [cx[depth + p] * (4.0 * t - in_plane(t)) for p, t in enumerate(temp)]
        return temp, flux

    def exchange(two, par):
        for j in range(n):
            peer = jnp.where(upper, j, n - 1 - j)
            for k in range(1, groups):
                ex_copy(two, par, k, peer, me).start()

    def chosen(two, par):
        for j in range(n):
            for k in range(1, groups):
                ex_copy(two, par, k, me, j).wait_recv()
        out = None
        for k in range(1, groups):
            got = land_two[k - 1] if two else land_one[par, k - 1]
            source = lax.rem(grp + groups - k, groups)
            out = got if out is None else jnp.where(partner == source, got, out)
        return out

    def finish(two, par):
        for j in range(n):
            for k in range(1, groups):
                ex_copy(two, par, k, j, me).wait_send()
        for peer in peers():
            rs_copy(two, par, peer, me).wait_send()

    def couple(it, carry):
        par = lax.rem(it, 2)
        first = it == 0

        @pl.when(jnp.logical_not(first))
        def _():
            advance()

        temp, flux = surface()
        mixed = sample([[away_t * t + away_f * f for t, f in zip(temp, flux)]])[0]
        for i in range(half):
            exp_one[i : i + 1, :] = mixed[:, i * LANES : (i + 1) * LANES]
        exchange(False, par)
        for x, p, mine in sides:
            for d in (x, p, 2 * p):
                when(mine, d, lambda d=d: halo_copy(par, d, -d).start())

        here = sample([temp])[0]
        for i in range(half):
            own_temp[i : i + 1, :] = here[:, i * LANES : (i + 1) * LANES]

        srcs = chosen(False, par)
        part = patches([srcs.reshape(blocks, LANES)])[0].reshape(n, half, LANES)
        mine = iota((n, half, LANES), 0) == me
        part_one[pl.ds(reach, n)] = part - jnp.where(mine, gain_t * own_temp[...], 0.0)
        for peer in peers():
            rs_copy(False, par, peer, me).start()
        for x, p, mine in sides:

            def hand_on(x=x, p=p):
                halo_copy(par, -x, x).wait_recv()
                handed_halo(par, x, p).start()

            when(mine, x, hand_on)

        @pl.when(first)
        def _():
            rest_each((2,), starts)

        rs_one[par, me] = part_one[pl.ds(me, span)]

        @pl.when(first)
        def _():
            each(offs, lambda d: arrivals(surf_copies(-d)))
            for d in offs:
                hot_rows(d + reach)

        for x, p, mine in sides:
            for d in (x, p, 2 * p):
                when(mine, d, lambda d=d: halo_copy(par, d, -d).wait_send())
            when(mine, x, lambda x=x, p=p: handed_halo(par, x, p).wait_send())
            for d in (p, 2 * p, 2 * x):
                when(mine, d, lambda d=d: halo_copy(par, -d, d).wait_recv())

        for peer in peers():
            rs_copy(False, par, me, peer).wait_recv()
        inc = rs_one[par, 0]
        for j in range(1, n):
            inc = inc + rs_one[par, j]
        sums = [spread(slot, inc[slot]) for slot in range(span)]
        for p in range(planes):
            fa[depth + p] = fa[depth + p] + sums[reach][p]
        for d in offs:
            for p in range(planes):
                fa[depth + planes * d + p] = land[par, at[d], p] + sums[d + reach][p]

        @pl.when(first)
        def _():
            each(offs, lambda d: arrivals(rest_copies(-d, (0, 1, 2))))
            each(offs, lambda d: departures(surf_copies(d)))
            rest_each((0, 1, 2), departures)
            for x, p, mine in sides:
                when(mine, x, lambda x=x, p=p: departures(handed_rest(x, p)))

        finish(False, par)
        return carry

    def final():
        par = (COUPLE - 1) % 2
        advance()
        got = sample(surface())
        for q in range(2):
            for i in range(half):
                exp_two[q * half + i : q * half + i + 1, :] = got[q][:, i * LANES : (i + 1) * LANES]
        exchange(True, par)
        src = chosen(True, par)
        parts = patches([src[:, q * half : (q + 1) * half].reshape(blocks, LANES) for q in range(2)])
        part_two[...] = jnp.concatenate([x.reshape(n, half, LANES) for x in parts], axis=1)
        for peer in peers():
            rs_copy(True, par, peer, me).start()
        rs_two[me] = part_two[me]
        for peer in peers():
            rs_copy(True, par, me, peer).wait_recv()
        iface = rs_two[0]
        for j in range(1, n):
            iface = iface + rs_two[j]
        iface_ref[...] = iface
        inc = gain_t * (iface[:half] - exp_two[:half]) + gain_f * iface[half:]
        for p, x in enumerate(spread(reach, inc)):
            out_ref[p] = fa[depth + p] + x
        finish(True, par)

    pair = (fa, fb)
    hear(0)
    for i in range(1, len(hops)):
        pass_on(i)
        if i < len(hops) - 1:
            hear(i)
    each(beside, lambda d: arrivals(first_copies(-d)))
    if len(hops) > 1:
        hear(len(hops) - 1)
    for k in range(1, groups):
        signal(ready.at[len(hops)], {"grp": lax.rem(grp + k, groups)})
    each(beside, lambda d: departures(first_copies(d)))
    for k in range(near):
        step(pair[k % 2], pair[(k + 1) % 2], depth - near + k)
    each(beside, lambda d: mid_copy(d).start())
    each(offs, lambda d: starts(surf_copies(d)))
    rest_each((0, 1), starts)
    for x, p, mine in sides:
        when(mine, x, lambda x=x, p=p: starts(handed_rest(x, p)))
    each(beside, lambda d: mid_copy(-d).wait_recv())
    for d in beside:
        fa[pl.ds(depth + planes * d, planes)] = land[1, at[d]]
    each(beside, lambda d: mid_copy(d).wait_send())
    for k in range(near):
        step(pair[k % 2], pair[(k + 1) % 2], depth - near + k)

    pl.semaphore_wait(ready.at[len(hops)], groups - 1)
    lax.fori_loop(0, COUPLE - 1, couple, 0)
    final()


def unpack(planes_ref, rows_ref, out_ref, iface_ref):
    planes, rows, _ = planes_ref.shape
    half = rows_ref.shape[0] // 2
    for b in range(rows // 8):
        rws = []
        for p in range(planes):
            x = planes_ref[p, b * 8 : (b + 1) * 8, :]
            rws.append(jnp.concatenate([x[i : i + 1, :] for i in range(8)], axis=1))
        out_ref[0, :, b * 8 * LANES : (b + 1) * 8 * LANES] = jnp.concatenate(rws, axis=0)
    for q in range(2):
        for i in range(half):
            iface_ref[0, q : q + 1, i * LANES : (i + 1) * LANES] = rows_ref[q * half + i : q * half + i + 1, :]


def local_of(n, groups):
    def local(
        initial_field,
        conduct,
        velocity,
        heat_release,
        group_kind,
        partner,
        surface_cell,
        patch_count,
        patch_centres,
        patch_targets,
        patch_maps,
    ):
        _, planes, cells = initial_field.shape
        rows = cells // LANES
        surf_here = surface_cell.shape[1]
        cap = patch_centres.shape[1]
        reach = -(-STEPS // planes)
        ext = planes + 2 * reach * planes
        half = surf_here // LANES
        vmem = pl.BlockSpec(memory_space=pltpu.VMEM)
        dma = pltpu.SemaphoreType.DMA
        nd = 2 * reach
        scratch = [
            pltpu.VMEM((ext, rows, LANES), F32),
            pltpu.VMEM((ext, rows, LANES), F32),
            pltpu.VMEM((ext, rows, LANES), F32),
            pltpu.VMEM((ext, rows, LANES), F32),
            pltpu.VMEM((ext, rows, LANES), F32),
            pltpu.VMEM((2, nd, planes, rows, LANES), F32),
            pltpu.VMEM((nd + 1, 1, surf_here), jnp.int32),
            pltpu.VMEM((nd + 1, rows, surf_here), BF16),
            pltpu.VMEM((nd + 1, surf_here, planes * LANES), BF16),
            pltpu.VMEM((planes * LANES, surf_here), BF16),
            pltpu.VMEM((LANES, cap * LANES), BF16),
            pltpu.VMEM((n * half, cap * LANES), BF16),
            pltpu.VMEM((cap * LANES, LANES), BF16),
            pltpu.VMEM((cap, LANES, 2 * LANES), BF16),
            pltpu.VMEM((half, LANES), F32),
            pltpu.VMEM((2 * half, LANES), F32),
            pltpu.VMEM((half, LANES), F32),
            pltpu.VMEM((2, groups - 1, n, half, LANES), F32),
            pltpu.VMEM((groups - 1, n, 2 * half, LANES), F32),
            pltpu.VMEM((n + nd, half, LANES), F32),
            pltpu.VMEM((n, 2 * half, LANES), F32),
            pltpu.VMEM((2, n, nd + 1, half, LANES), F32),
            pltpu.VMEM((n, 2 * half, LANES), F32),
            dma((9, nd)),
            dma((9, nd)),
            dma((2, groups - 1, n)),
            dma((2, groups - 1, n)),
            dma((2, n)),
            dma((2, n)),
            dma((2, nd)),
            dma((2, nd)),
            pltpu.SMEM(group_kind.shape, jnp.int32),
            pltpu.SMEM(partner.shape, jnp.int32),
            pltpu.SMEM(patch_count.shape, jnp.int32),
            pltpu.VMEM((planes, cells), F32),
            pltpu.VMEM((planes, cells), F32),
            pltpu.VMEM((planes, cells), F32),
            pltpu.VMEM((planes, cells), F32),
            pltpu.VMEM((cap, LANES), jnp.int32),
            pltpu.VMEM((cap, LANES), jnp.int32),
            pltpu.VMEM((cap, LANES, LANES), F32),
            dma((11,)),
            pltpu.SemaphoreType.REGULAR((n.bit_length() + 1,)),
        ]

        def body(*refs):
            kernel(n, groups, *refs)

        lying, tops = pl.pallas_call(
            body,
            name="coupled",
            out_shape=(
                pltpu.VMEM((planes, rows, LANES), F32),
                pltpu.VMEM((2 * half, LANES), F32),
            ),
            in_specs=[pl.BlockSpec(memory_space=pltpu.HBM)] * 11,
            out_specs=(vmem, vmem),
            scratch_shapes=scratch,
            compiler_params=pltpu.CompilerParams(
                collective_id=0, has_side_effects=True, vmem_limit_bytes=56 * 1024 * 1024
            ),
        )(
            group_kind,
            partner,
            patch_count,
            initial_field,
            conduct,
            velocity,
            heat_release,
            surface_cell,
            patch_centres[0],
            patch_targets[0],
            patch_maps[0],
        )
        return pl.pallas_call(
            unpack,
            name="unpack",
            out_shape=(
                jax.ShapeDtypeStruct(initial_field.shape, F32),
                jax.ShapeDtypeStruct((1, 2, surf_here), F32),
            ),
            in_specs=[vmem] * 2,
            out_specs=(vmem, vmem),
        )(*(pltpu.with_memory_space_constraint(x, pltpu.VMEM) for x in (lying, tops)))

    return local


def solution(mesh):
    placed = (
        P("grp", "sub", None),
        P("grp", "sub", None),
        P("grp", "sub", None),
        P("grp", "sub", None),
        P(),
        P(),
        P("grp", "sub"),
        P("grp", None),
        P("grp", "sub", None),
        P("grp", "sub", None),
        P("grp", "sub", None, None),
    )
    return jax.shard_map(
        local_of(mesh.shape["sub"], mesh.shape["grp"]),
        mesh=mesh,
        in_specs=placed,
        out_specs=(P("grp", "sub", None), P("grp", None, "sub")),
        check_vma=False,
    )
```

```python
import jax
import jax.numpy as jnp
from jax import lax
from jax.experimental import pallas as pl
from jax.experimental.pallas import tpu as pltpu
from jax.sharding import PartitionSpec as P

STEPS = 4
COUPLE = 4
LANES = 128
F32 = jnp.float32
BF16 = jnp.bfloat16


def split(x):
    hi = x.astype(BF16).astype(F32)
    return hi, x - hi


def dot_nt(a, b):
    return lax.dot_general(a, b, (((1,), (1,)), ((), ())), preferred_element_type=F32)


def dot_nn(a, b):
    return lax.dot_general(a, b, (((1,), (0,)), ((), ())), preferred_element_type=F32)


def iota(shape, dim):
    return lax.broadcasted_iota(jnp.int32, shape, dim)


def in_plane(c):
    rows, cols = c.shape
    return (
        pltpu.roll(c, 1, 0)
        + pltpu.roll(c, rows - 1, 0)
        + pltpu.roll(c, 1, 1)
        + pltpu.roll(c, cols - 1, 1)
    )


def kernel(
    n,
    groups,
    kind_hbm,
    partner_hbm,
    count_hbm,
    field_hbm,
    cond_hbm,
    vel_hbm,
    heat_hbm,
    surf_hbm,
    cent_hbm,
    targ_hbm,
    maps_hbm,
    out_ref,
    iface_ref,
    fa,
    fb,
    cx,
    vx,
    hx,
    land,
    surf_all,
    oh_surf,
    hot_surf,
    oh_lane,
    oh_cent,
    oh_targ,
    hot_targ,
    maps2,
    exp_one,
    exp_two,
    own_temp,
    land_one,
    land_two,
    part_one,
    part_two,
    rs_one,
    rs_two,
    set_send,
    set_recv,
    ex_send,
    ex_recv,
    rs_send,
    rs_recv,
    halo_send,
    halo_recv,
    kind_ref,
    partner_ref,
    count_ref,
    field_ref,
    cond_ref,
    vel_ref,
    heat_ref,
    cent_ref,
    targ_ref,
    maps,
    load_sem,
    ready,
):
    planes = field_ref.shape[0]
    rows = fa.shape[1]
    near = STEPS // 2
    assert near % 2 == 0 and near <= planes
    surf_here = surf_all.shape[2]
    cap = cent_ref.shape[0]
    reach = -(-STEPS // planes)
    depth = reach * planes
    ext = planes + 2 * depth
    offs = [d for d in range(-reach, reach + 1) if d != 0]
    at = {d: i for i, d in enumerate(offs)}
    half = surf_here // LANES
    span = 2 * reach + 1
    blocks = n * half
    me = lax.axis_index("sub")
    grp = lax.axis_index("grp")

    def there(d):
        return jnp.logical_and(me + d >= 0, me + d < n)

    def rcopy(src, dst, ss, rs, dev):
        return pltpu.make_async_remote_copy(
            src_ref=src,
            dst_ref=dst,
            send_sem=ss,
            recv_sem=rs,
            device_id=dev,
            device_id_type=pl.DeviceIdType.MESH,
        )

    pairs = (
        (kind_hbm, kind_ref),
        (partner_hbm, partner_ref),
        (count_hbm, count_ref),
        (field_hbm.at[0], field_ref),
        (cond_hbm.at[0], cond_ref),
        (vel_hbm.at[0], vel_ref),
        (heat_hbm.at[0], heat_ref),
        (surf_hbm, surf_all.at[reach]),
        (cent_hbm, cent_ref),
        (targ_hbm, targ_ref),
        (maps_hbm, maps),
    )
    loads = [pltpu.make_async_copy(src, dst, load_sem.at[i]) for i, (src, dst) in enumerate(pairs)]
    for c in loads:
        c.start()

    def signal(sem, dev):
        pl.semaphore_signal(sem, inc=1, device_id=dev, device_id_type=pl.DeviceIdType.MESH)

    def among(ds):
        return sum(there(d).astype(jnp.int32) for d in ds)

    def tell(sem, ds):
        for d in ds:

            @pl.when(there(d))
            def _():
                signal(sem, {"sub": me + d})

    barrier = pltpu.get_barrier_semaphore()
    tell(barrier, offs)
    for k in range(1, groups):
        signal(barrier, {"grp": lax.rem(grp + k, groups)})
    hops = [reach]
    while 2 * hops[-1] < n:
        hops.append(2 * hops[-1])

    def hear(i):
        pl.semaphore_wait(ready.at[i], among((-hops[i], hops[i])))

    def pass_on(i):
        tell(ready.at[i], (-hops[i], hops[i]))

    for border in (pl.ds(0, reach), pl.ds(reach + n, reach)):
        part_one[border] = jnp.zeros((reach, half, LANES), F32)
    for d in offs:

        @pl.when(jnp.logical_not(there(d)))
        def _():
            for buf in (fa, cx, vx, hx):
                buf[pl.ds(depth + planes * d, planes)] = jnp.zeros((planes, rows, LANES), F32)
            for par in range(2):
                land[par, at[d]] = jnp.zeros((planes, rows, LANES), F32)
            surf_all[reach + d] = jnp.zeros((1, surf_here), jnp.int32)

    for c in loads[:7]:
        c.wait()
    own = pl.ds(depth, planes)
    kind = kind_ref[grp]
    gas = jnp.where(kind == 0, 1.0, 0.0).astype(F32)
    gain_t = jnp.where(kind == 0, 0.5, 0.25).astype(F32)
    gain_f = jnp.where(kind == 0, -0.25, 0.25).astype(F32)
    away_t = jnp.where(kind == 0, 0.25, 0.5).astype(F32)
    away_f = jnp.where(kind == 0, 0.25, -0.25).astype(F32)
    fetch = ((field_ref, fa, None), (cond_ref, cx, None), (vel_ref, vx, gas), (heat_ref, hx, 0.5 * gas))

    def unfold(b, carry):
        chunk = pl.ds(pl.multiple_of(b * 8 * LANES, LANES), 8 * LANES)
        for src, dst, scale in fetch:
            x = src[:, chunk]
            if scale is not None:
                x = x * scale
            for p in range(planes):
                dst[depth + p, pl.ds(pl.multiple_of(b * 8, 8), 8), :] = jnp.concatenate(
                    [x[p : p + 1, i * LANES : (i + 1) * LANES] for i in range(8)], axis=0
                )
        return carry

    lax.fori_loop(0, rows // 8, unfold, 0)
    pl.semaphore_wait(barrier, among(offs) + groups - 1)

    def send_planes(buf, lo, hi, to, j):
        slot = -to
        shift = depth - (depth + planes * slot)
        return rcopy(
            buf.at[pl.ds(lo + shift, hi - lo)],
            buf.at[pl.ds(lo, hi - lo)],
            set_send.at[j, at[to]],
            set_recv.at[j, at[slot]],
            {"sub": me + to},
        )

    def first_copies(to):
        base = depth - planes * to
        lo, hi = max(base, depth - near), min(base + planes, depth + planes + near)
        out = [send_planes(fa, lo, hi, to, 0)]
        lo, hi = max(base, depth - near + 1), min(base + planes, depth + planes + near - 1)
        if hi > lo:
            out += [send_planes(buf, lo, hi, to, j + 1) for j, buf in enumerate((cx, vx, hx))]
        return out

    def rest_copies(to, which):
        base = depth - planes * to
        lo, hi = max(base, 1), min(base + planes, ext - 1)
        if to == 1:
            hi = min(hi, depth - near + 1)
        if to == -1:
            lo = max(lo, depth + planes + near - 1)
        if hi <= lo:
            return []
        return [send_planes((cx, vx, hx)[j], lo, hi, to, j + 4) for j in which]

    sides = ((-1, 1, lax.rem(me, 2) == 0), (1, -1, lax.rem(me, 2) == 1))
    assert reach == 2 and near == planes == 2 and n % 2 == 0

    def when(mine, d, act):
        @pl.when(jnp.logical_and(mine, there(d)))
        def _():
            act()

    def rest_each(which, act):
        for x, p, mine in sides:
            for d in (x, p, 2 * p):
                when(mine, d, lambda d=d: act(rest_copies(d, which)))

    def handed_rest(x, p):
        plane = depth - 1 if x < 0 else depth + planes
        return [
            rcopy(
                buf.at[pl.ds(plane, 1)],
                buf.at[pl.ds(plane - p * planes, 1)],
                set_send.at[j + 4, at[x - p]],
                set_recv.at[j + 4, at[x - p]],
                {"sub": me + p},
            )
            for j, buf in enumerate((cx, vx, hx))
        ]

    def handed_halo(par, x, p):
        return rcopy(
            land.at[par, at[x]],
            land.at[par, at[x - p]],
            halo_send.at[par, at[x - p]],
            halo_recv.at[par, at[x - p]],
            {"sub": me + p},
        )

    def surf_copies(to):
        return [
            rcopy(
                surf_all.at[reach],
                surf_all.at[reach - to],
                set_send.at[7, at[to]],
                set_recv.at[7, at[-to]],
                {"sub": me + to},
            )
        ]

    def mid_copy(to):
        return rcopy(
            fa.at[own],
            land.at[1, at[-to]],
            set_send.at[8, at[to]],
            set_recv.at[8, at[-to]],
            {"sub": me + to},
        )

    def each(ds, act):
        for d in ds:

            @pl.when(there(d))
            def _():
                act(d)

    def starts(copies):
        for c in copies:
            c.start()

    def arrivals(copies):
        for c in copies:
            c.wait_recv()

    def departures(copies):
        for c in copies:
            c.wait_send()

    beside = (-1, 1)
    each(beside, lambda d: starts(first_copies(d)))
    pass_on(0)

    partner = partner_ref[grp]
    count = count_ref[0, me]
    block_row = iota((blocks, LANES), 0)
    lane_row = iota((LANES, LANES), 0)

    def block_of(x):
        return lax.shift_right_logical(x, jnp.full(x.shape, LANES.bit_length() - 1, jnp.int32))

    def lane_of(x):
        return lax.bitwise_and(x, jnp.full(x.shape, LANES - 1, jnp.int32))

    def hot(mask):
        return jnp.where(mask, 1.0, 0.0).astype(F32)

    for c in loads[7:]:
        c.wait()
    for s in range(cap):
        lanes = pl.ds(s * LANES, LANES)
        oh_cent[:, lanes] = hot(lane_row == lane_of(cent_ref[s : s + 1, :])).astype(BF16)
        oh_targ[:, lanes] = hot(block_row == block_of(targ_ref[s : s + 1, :])).astype(BF16)
        hot_targ[lanes, :] = hot(lane_row == lane_of(targ_ref[s : s + 1, :])).T.astype(BF16)
        live = jnp.where(s < count, 1.0, 0.0).astype(F32)
        hi, lo = split((maps[s] * live).T)
        maps2[s, :, pl.ds(0, LANES)] = hi.astype(BF16)
        maps2[s, :, pl.ds(LANES, LANES)] = lo.astype(BF16)

    cell_row = iota((rows, surf_here), 0)

    def plane_of(cell):
        return sum((cell >= p * rows * LANES).astype(jnp.int32) for p in range(1, planes))

    def row_of(cell):
        return block_of(cell) - plane_of(cell) * rows

    def spot_of(cell):
        return plane_of(cell) * LANES + lane_of(cell)

    def hot_rows(j):
        oh_surf[j] = hot(cell_row == row_of(surf_all[j])).astype(BF16)
        spot = spot_of(surf_all[j])
        for i in range(half):
            cols = slice(i * LANES, (i + 1) * LANES)
            for p in range(planes):
                hot_surf[j, cols, pl.ds(p * LANES, LANES)] = hot(lane_row + p * LANES == spot[:, cols]).T.astype(BF16)

    hot_rows(reach)
    oh_lane[...] = hot(iota((planes * LANES, surf_here), 0) == spot_of(surf_all[reach])).astype(BF16)

    block_of_slot = iota((blocks, cap * LANES), 0)

    def step(src, dst, k):
        for z in range(k + 1, ext - k - 1):
            c = src[z]
            dn = src[z - 1]
            lap = src[z + 1] + dn + in_plane(c) - 6.0 * c
            dst[z] = c + cx[z] * lap - vx[z] * (c - dn) + hx[z] * (1.0 + jnp.tanh(c))

    def spread(slot, inc):
        lhs = []
        for x in split(inc):
            wide = [jnp.broadcast_to(x[i : i + 1, :], (16, LANES)).astype(BF16) for i in range(half)]
            wide = jnp.concatenate(wide, axis=1)
            lhs += [oh_surf[slot, r * 16 : (r + 1) * 16, :] * wide for r in range(rows // 16)]
        r = dot_nn(jnp.concatenate(lhs, axis=0), hot_surf[slot])
        r = r[:rows] + r[rows:]
        return [r[:, p * LANES : (p + 1) * LANES] for p in range(planes)]

    def halo_copy(par, to, slot):
        return rcopy(
            fa.at[own],
            land.at[par, at[slot]],
            halo_send.at[par, at[to]],
            halo_recv.at[par, at[slot]],
            {"sub": me + to},
        )

    upper = 2 * me >= n

    def ex_copy(two, par, k, peer, sender):
        src, dst = (exp_two, land_two.at[k - 1, sender]) if two else (exp_one, land_one.at[par, k - 1, sender])
        return rcopy(
            src,
            dst,
            ex_send.at[par, k - 1, peer],
            ex_recv.at[par, k - 1, sender],
            {"grp": lax.rem(grp + k, groups), "sub": peer},
        )

    def peers():
        return [lax.rem(me + jnp.where(upper, k, n - k), n) for k in range(1, n)]

    def rs_copy(two, par, peer, sender):
        if two:
            src, dst = part_two.at[peer], rs_two.at[sender]
        else:
            src, dst = part_one.at[pl.ds(peer, span)], rs_one.at[par, sender]
        return rcopy(src, dst, rs_send.at[par, peer], rs_recv.at[par, sender], {"sub": peer})

    def sample(values):
        lhs = []
        for x in values:
            lhs += split(jnp.concatenate(x, axis=1))
        got = dot_nn(jnp.concatenate(lhs, axis=0).astype(BF16), oh_lane[...])
        hit = cell_row == row_of(surf_all[reach])
        out = []
        for q in range(len(values)):
            v = got[2 * q * rows : (2 * q + 1) * rows] + got[(2 * q + 1) * rows : (2 * q + 2) * rows]
            out.append(jnp.sum(jnp.where(hit, v, 0.0), axis=0, keepdims=True))
        return out

    def patches(srcs):
        count_q = len(srcs)
        lhs = jnp.concatenate([x for v in srcs for x in split(v)], axis=0).astype(BF16)
        vals = dot_nn(lhs, oh_cent[...])
        cent = jnp.concatenate([cent_ref[s : s + 1, :] for s in range(cap)], axis=1)
        hit = block_of_slot == block_of(cent)
        cv = []
        for q in range(count_q):
            v = vals[2 * q * blocks : (2 * q + 1) * blocks] + vals[(2 * q + 1) * blocks : (2 * q + 2) * blocks]
            cv.append(jnp.sum(jnp.where(hit, v, 0.0), axis=0, keepdims=True))
        c4 = jnp.concatenate([x for v in cv for x in split(v)], axis=0).astype(BF16)
        contrib = []
        for s in range(cap):
            r = dot_nn(c4[:, s * LANES : (s + 1) * LANES], maps2[s])
            contrib.append(r[:, :LANES] + r[:, LANES:])
        r = jnp.concatenate(contrib, axis=1)
        rows_of = []
        for q in range(count_q):
            for x in split(r[2 * q : 2 * q + 1] + r[2 * q + 1 : 2 * q + 2]):
                wide = jnp.broadcast_to(x, (16, cap * LANES)).astype(BF16)
                rows_of += [oh_targ[b * 16 : (b + 1) * 16, :] * wide for b in range(blocks // 16)]
        acc = dot_nn(jnp.concatenate(rows_of, axis=0), hot_targ[...])
        return [
            acc[2 * q * blocks : (2 * q + 1) * blocks] + acc[(2 * q + 1) * blocks : (2 * q + 2) * blocks]
            for q in range(count_q)
        ]

    def advance():
        for k in range(STEPS):
            step(pair[k % 2], pair[(k + 1) % 2], k)

    def surface():
        temp = [fa[depth + p] for p in range(planes)]
        flux = [cx[depth + p] * (4.0 * t - in_plane(t)) for p, t in enumerate(temp)]
        return temp, flux

    def exchange(two, par):
        for j in range(n):
            peer = jnp.where(upper, j, n - 1 - j)
            for k in range(1, groups):
                ex_copy(two, par, k, peer, me).start()

    def chosen(two, par):
        for j in range(n):
            for k in range(1, groups):
                ex_copy(two, par, k, me, j).wait_recv()
        out = None
        for k in range(1, groups):
            got = land_two[k - 1] if two else land_one[par, k - 1]
            source = lax.rem(grp + groups - k, groups)
            out = got if out is None else jnp.where(partner == source, got, out)
        return out

    def finish(two, par):
        for j in range(n):
            for k in range(1, groups):
                ex_copy(two, par, k, j, me).wait_send()
        for peer in peers():
            rs_copy(two, par, peer, me).wait_send()

    def couple(it, carry):
        par = lax.rem(it, 2)
        first = it == 0

        @pl.when(jnp.logical_not(first))
        def _():
            advance()

        temp, flux = surface()
        mixed = sample([[away_t * t + away_f * f for t, f in zip(temp, flux)]])[0]
        for i in range(half):
            exp_one[i : i + 1, :] = mixed[:, i * LANES : (i + 1) * LANES]
        exchange(False, par)
        for x, p, mine in sides:
            for d in (x, p, 2 * p):
                when(mine, d, lambda d=d: halo_copy(par, d, -d).start())

        @pl.when(first)
        def _():
            rest_each((1,), starts)


        here = sample([temp])[0]
        for i in range(half):
            own_temp[i : i + 1, :] = here[:, i * LANES : (i + 1) * LANES]

        srcs = chosen(False, par)
        part = patches([srcs.reshape(blocks, LANES)])[0].reshape(n, half, LANES)
        mine = iota((n, half, LANES), 0) == me
        part_one[pl.ds(reach, n)] = part - jnp.where(mine, gain_t * own_temp[...], 0.0)
        for peer in peers():
            rs_copy(False, par, peer, me).start()
        for x, p, mine in sides:

            def hand_on(x=x, p=p):
                halo_copy(par, -x, x).wait_recv()
                handed_halo(par, x, p).start()

            when(mine, x, hand_on)

        @pl.when(first)
        def _():
            rest_each((2,), starts)

        rs_one[par, me] = part_one[pl.ds(me, span)]

        @pl.when(first)
        def _():
            each(offs, lambda d: arrivals(surf_copies(-d)))
            for d in offs:
                hot_rows(d + reach)

        for x, p, mine in sides:
            for d in (x, p, 2 * p):
                when(mine, d, lambda d=d: halo_copy(par, d, -d).wait_send())
            when(mine, x, lambda x=x, p=p: handed_halo(par, x, p).wait_send())
            for d in (p, 2 * p, 2 * x):
                when(mine, d, lambda d=d: halo_copy(par, -d, d).wait_recv())

        for peer in peers():
            rs_copy(False, par, me, peer).wait_recv()
        inc = rs_one[par, 0]
        for j in range(1, n):
            inc = inc + rs_one[par, j]
        sums = [spread(slot, inc[slot]) for slot in range(span)]
        for p in range(planes):
            fa[depth + p] = fa[depth + p] + sums[reach][p]
        for d in offs:
            for p in range(planes):
                fa[depth + planes * d + p] = land[par, at[d], p] + sums[d + reach][p]

        @pl.when(first)
        def _():
            each(offs, lambda d: arrivals(rest_copies(-d, (0, 1, 2))))
            each(offs, lambda d: departures(surf_copies(d)))
            rest_each((0, 1, 2), departures)
            for x, p, mine in sides:
                when(mine, x, lambda x=x, p=p: departures(handed_rest(x, p)))

        finish(False, par)
        return carry

    def final():
        par = (COUPLE - 1) % 2
        advance()
        got = sample(surface())
        for q in range(2):
            for i in range(half):
                exp_two[q * half + i : q * half + i + 1, :] = got[q][:, i * LANES : (i + 1) * LANES]
        exchange(True, par)
        src = chosen(True, par)
        parts = patches([src[:, q * half : (q + 1) * half].reshape(blocks, LANES) for q in range(2)])
        part_two[...] = jnp.concatenate([x.reshape(n, half, LANES) for x in parts], axis=1)
        for peer in peers():
            rs_copy(True, par, peer, me).start()
        rs_two[me] = part_two[me]
        for peer in peers():
            rs_copy(True, par, me, peer).wait_recv()
        iface = rs_two[0]
        for j in range(1, n):
            iface = iface + rs_two[j]
        iface_ref[...] = iface
        inc = gain_t * (iface[:half] - exp_two[:half]) + gain_f * iface[half:]
        for p, x in enumerate(spread(reach, inc)):
            out_ref[p] = fa[depth + p] + x
        finish(True, par)

    pair = (fa, fb)
    hear(0)
    for i in range(1, len(hops)):
        pass_on(i)
        if i < len(hops) - 1:
            hear(i)
    each(beside, lambda d: arrivals(first_copies(-d)))
    if len(hops) > 1:
        hear(len(hops) - 1)
    for k in range(1, groups):
        signal(ready.at[len(hops)], {"grp": lax.rem(grp + k, groups)})
    each(beside, lambda d: departures(first_copies(d)))
    for k in range(near):
        step(pair[k % 2], pair[(k + 1) % 2], depth - near + k)
    each(beside, lambda d: mid_copy(d).start())
    each(offs, lambda d: starts(surf_copies(d)))
    rest_each((0,), starts)
    for x, p, mine in sides:
        when(mine, x, lambda x=x, p=p: starts(handed_rest(x, p)))
    each(beside, lambda d: mid_copy(-d).wait_recv())
    for d in beside:
        fa[pl.ds(depth + planes * d, planes)] = land[1, at[d]]
    each(beside, lambda d: mid_copy(d).wait_send())
    for k in range(near):
        step(pair[k % 2], pair[(k + 1) % 2], depth - near + k)

    pl.semaphore_wait(ready.at[len(hops)], groups - 1)
    lax.fori_loop(0, COUPLE - 1, couple, 0)
    final()


def unpack(planes_ref, rows_ref, out_ref, iface_ref):
    planes, rows, _ = planes_ref.shape
    half = rows_ref.shape[0] // 2
    for b in range(rows // 8):
        rws = []
        for p in range(planes):
            x = planes_ref[p, b * 8 : (b + 1) * 8, :]
            rws.append(jnp.concatenate([x[i : i + 1, :] for i in range(8)], axis=1))
        out_ref[0, :, b * 8 * LANES : (b + 1) * 8 * LANES] = jnp.concatenate(rws, axis=0)
    for q in range(2):
        for i in range(half):
            iface_ref[0, q : q + 1, i * LANES : (i + 1) * LANES] = rows_ref[q * half + i : q * half + i + 1, :]


def local_of(n, groups):
    def local(
        initial_field,
        conduct,
        velocity,
        heat_release,
        group_kind,
        partner,
        surface_cell,
        patch_count,
        patch_centres,
        patch_targets,
        patch_maps,
    ):
        _, planes, cells = initial_field.shape
        rows = cells // LANES
        surf_here = surface_cell.shape[1]
        cap = patch_centres.shape[1]
        reach = -(-STEPS // planes)
        ext = planes + 2 * reach * planes
        half = surf_here // LANES
        vmem = pl.BlockSpec(memory_space=pltpu.VMEM)
        dma = pltpu.SemaphoreType.DMA
        nd = 2 * reach
        scratch = [
            pltpu.VMEM((ext, rows, LANES), F32),
            pltpu.VMEM((ext, rows, LANES), F32),
            pltpu.VMEM((ext, rows, LANES), F32),
            pltpu.VMEM((ext, rows, LANES), F32),
            pltpu.VMEM((ext, rows, LANES), F32),
            pltpu.VMEM((2, nd, planes, rows, LANES), F32),
            pltpu.VMEM((nd + 1, 1, surf_here), jnp.int32),
            pltpu.VMEM((nd + 1, rows, surf_here), BF16),
            pltpu.VMEM((nd + 1, surf_here, planes * LANES), BF16),
            pltpu.VMEM((planes * LANES, surf_here), BF16),
            pltpu.VMEM((LANES, cap * LANES), BF16),
            pltpu.VMEM((n * half, cap * LANES), BF16),
            pltpu.VMEM((cap * LANES, LANES), BF16),
            pltpu.VMEM((cap, LANES, 2 * LANES), BF16),
            pltpu.VMEM((half, LANES), F32),
            pltpu.VMEM((2 * half, LANES), F32),
            pltpu.VMEM((half, LANES), F32),
            pltpu.VMEM((2, groups - 1, n, half, LANES), F32),
            pltpu.VMEM((groups - 1, n, 2 * half, LANES), F32),
            pltpu.VMEM((n + nd, half, LANES), F32),
            pltpu.VMEM((n, 2 * half, LANES), F32),
            pltpu.VMEM((2, n, nd + 1, half, LANES), F32),
            pltpu.VMEM((n, 2 * half, LANES), F32),
            dma((9, nd)),
            dma((9, nd)),
            dma((2, groups - 1, n)),
            dma((2, groups - 1, n)),
            dma((2, n)),
            dma((2, n)),
            dma((2, nd)),
            dma((2, nd)),
            pltpu.SMEM(group_kind.shape, jnp.int32),
            pltpu.SMEM(partner.shape, jnp.int32),
            pltpu.SMEM(patch_count.shape, jnp.int32),
            pltpu.VMEM((planes, cells), F32),
            pltpu.VMEM((planes, cells), F32),
            pltpu.VMEM((planes, cells), F32),
            pltpu.VMEM((planes, cells), F32),
            pltpu.VMEM((cap, LANES), jnp.int32),
            pltpu.VMEM((cap, LANES), jnp.int32),
            pltpu.VMEM((cap, LANES, LANES), F32),
            dma((11,)),
            pltpu.SemaphoreType.REGULAR((n.bit_length() + 1,)),
        ]

        def body(*refs):
            kernel(n, groups, *refs)

        lying, tops = pl.pallas_call(
            body,
            name="coupled",
            out_shape=(
                pltpu.VMEM((planes, rows, LANES), F32),
                pltpu.VMEM((2 * half, LANES), F32),
            ),
            in_specs=[pl.BlockSpec(memory_space=pltpu.HBM)] * 11,
            out_specs=(vmem, vmem),
            scratch_shapes=scratch,
            compiler_params=pltpu.CompilerParams(
                collective_id=0, has_side_effects=True, vmem_limit_bytes=56 * 1024 * 1024
            ),
        )(
            group_kind,
            partner,
            patch_count,
            initial_field,
            conduct,
            velocity,
            heat_release,
            surface_cell,
            patch_centres[0],
            patch_targets[0],
            patch_maps[0],
        )
        return pl.pallas_call(
            unpack,
            name="unpack",
            out_shape=(
                jax.ShapeDtypeStruct(initial_field.shape, F32),
                jax.ShapeDtypeStruct((1, 2, surf_here), F32),
            ),
            in_specs=[vmem] * 2,
            out_specs=(vmem, vmem),
        )(*(pltpu.with_memory_space_constraint(x, pltpu.VMEM) for x in (lying, tops)))

    return local


def solution(mesh):
    placed = (
        P("grp", "sub", None),
        P("grp", "sub", None),
        P("grp", "sub", None),
        P("grp", "sub", None),
        P(),
        P(),
        P("grp", "sub"),
        P("grp", None),
        P("grp", "sub", None),
        P("grp", "sub", None),
        P("grp", "sub", None, None),
    )
    return jax.shard_map(
        local_of(mesh.shape["sub"], mesh.shape["grp"]),
        mesh=mesh,
        in_specs=placed,
        out_specs=(P("grp", "sub", None), P("grp", None, "sub")),
        check_vma=False,
    )
```

```python
import jax
import jax.numpy as jnp
from jax import lax
from jax.experimental import pallas as pl
from jax.experimental.pallas import tpu as pltpu
from jax.sharding import PartitionSpec as P

STEPS = 4
COUPLE = 4
LANES = 128
F32 = jnp.float32
BF16 = jnp.bfloat16


def split(x):
    hi = x.astype(BF16).astype(F32)
    return hi, x - hi


def dot_nt(a, b):
    return lax.dot_general(a, b, (((1,), (1,)), ((), ())), preferred_element_type=F32)


def dot_nn(a, b):
    return lax.dot_general(a, b, (((1,), (0,)), ((), ())), preferred_element_type=F32)


def iota(shape, dim):
    return lax.broadcasted_iota(jnp.int32, shape, dim)


def in_plane(c):
    rows, cols = c.shape
    return (
        pltpu.roll(c, 1, 0)
        + pltpu.roll(c, rows - 1, 0)
        + pltpu.roll(c, 1, 1)
        + pltpu.roll(c, cols - 1, 1)
    )


def kernel(
    n,
    groups,
    kind_hbm,
    partner_hbm,
    count_hbm,
    field_hbm,
    cond_hbm,
    vel_hbm,
    heat_hbm,
    surf_hbm,
    cent_hbm,
    targ_hbm,
    maps_hbm,
    out_ref,
    iface_ref,
    fa,
    fb,
    cx,
    vx,
    hx,
    land,
    surf_all,
    oh_surf,
    hot_surf,
    oh_lane,
    oh_cent,
    oh_targ,
    hot_targ,
    maps2,
    exp_one,
    exp_two,
    own_temp,
    land_one,
    land_two,
    part_one,
    part_two,
    rs_one,
    rs_two,
    set_send,
    set_recv,
    ex_send,
    ex_recv,
    rs_send,
    rs_recv,
    halo_send,
    halo_recv,
    kind_ref,
    partner_ref,
    count_ref,
    field_ref,
    cond_ref,
    vel_ref,
    heat_ref,
    cent_ref,
    targ_ref,
    maps,
    load_sem,
    ready,
    ax,
    bx,
):
    planes = field_ref.shape[0]
    rows = fa.shape[1]
    near = STEPS // 2
    assert near % 2 == 0 and near <= planes
    surf_here = surf_all.shape[2]
    cap = cent_ref.shape[0]
    reach = -(-STEPS // planes)
    depth = reach * planes
    ext = planes + 2 * depth
    offs = [d for d in range(-reach, reach + 1) if d != 0]
    at = {d: i for i, d in enumerate(offs)}
    half = surf_here // LANES
    span = 2 * reach + 1
    blocks = n * half
    me = lax.axis_index("sub")
    grp = lax.axis_index("grp")

    def there(d):
        return jnp.logical_and(me + d >= 0, me + d < n)

    def rcopy(src, dst, ss, rs, dev):
        return pltpu.make_async_remote_copy(
            src_ref=src,
            dst_ref=dst,
            send_sem=ss,
            recv_sem=rs,
            device_id=dev,
            device_id_type=pl.DeviceIdType.MESH,
        )

    pairs = (
        (kind_hbm, kind_ref),
        (partner_hbm, partner_ref),
        (count_hbm, count_ref),
        (field_hbm.at[0], field_ref),
        (cond_hbm.at[0], cond_ref),
        (vel_hbm.at[0], vel_ref),
        (heat_hbm.at[0], heat_ref),
        (surf_hbm, surf_all.at[reach]),
        (cent_hbm, cent_ref),
        (targ_hbm, targ_ref),
        (maps_hbm, maps),
    )
    loads = [pltpu.make_async_copy(src, dst, load_sem.at[i]) for i, (src, dst) in enumerate(pairs)]
    for c in loads:
        c.start()

    def signal(sem, dev):
        pl.semaphore_signal(sem, inc=1, device_id=dev, device_id_type=pl.DeviceIdType.MESH)

    def among(ds):
        return sum(there(d).astype(jnp.int32) for d in ds)

    def tell(sem, ds):
        for d in ds:

            @pl.when(there(d))
            def _():
                signal(sem, {"sub": me + d})

    barrier = pltpu.get_barrier_semaphore()
    tell(barrier, offs)
    for k in range(1, groups):
        signal(barrier, {"grp": lax.rem(grp + k, groups)})
    hops = [reach]
    while 2 * hops[-1] < n:
        hops.append(2 * hops[-1])

    def hear(i):
        pl.semaphore_wait(ready.at[i], among((-hops[i], hops[i])))

    def pass_on(i):
        tell(ready.at[i], (-hops[i], hops[i]))

    for border in (pl.ds(0, reach), pl.ds(reach + n, reach)):
        part_one[border] = jnp.zeros((reach, half, LANES), F32)
    for d in offs:

        @pl.when(jnp.logical_not(there(d)))
        def _():
            for buf in (fa, cx, vx, hx):
                buf[pl.ds(depth + planes * d, planes)] = jnp.zeros((planes, rows, LANES), F32)
            for par in range(2):
                land[par, at[d]] = jnp.zeros((planes, rows, LANES), F32)
            surf_all[reach + d] = jnp.zeros((1, surf_here), jnp.int32)

    for c in loads[:7]:
        c.wait()
    own = pl.ds(depth, planes)
    kind = kind_ref[grp]
    gas = jnp.where(kind == 0, 1.0, 0.0).astype(F32)
    gain_t = jnp.where(kind == 0, 0.5, 0.25).astype(F32)
    gain_f = jnp.where(kind == 0, -0.25, 0.25).astype(F32)
    away_t = jnp.where(kind == 0, 0.25, 0.5).astype(F32)
    away_f = jnp.where(kind == 0, 0.25, -0.25).astype(F32)
    fetch = ((field_ref, fa, None), (cond_ref, cx, None), (vel_ref, vx, gas), (heat_ref, hx, 0.5 * gas))

    def unfold(b, carry):
        chunk = pl.ds(pl.multiple_of(b * 8 * LANES, LANES), 8 * LANES)
        for src, dst, scale in fetch:
            x = src[:, chunk]
            if scale is not None:
                x = x * scale
            for p in range(planes):
                dst[depth + p, pl.ds(pl.multiple_of(b * 8, 8), 8), :] = jnp.concatenate(
                    [x[p : p + 1, i * LANES : (i + 1) * LANES] for i in range(8)], axis=0
                )
        return carry

    lax.fori_loop(0, rows // 8, unfold, 0)
    pl.semaphore_wait(barrier, among(offs) + groups - 1)

    def send_planes(buf, lo, hi, to, j):
        slot = -to
        shift = depth - (depth + planes * slot)
        return rcopy(
            buf.at[pl.ds(lo + shift, hi - lo)],
            buf.at[pl.ds(lo, hi - lo)],
            set_send.at[j, at[to]],
            set_recv.at[j, at[slot]],
            {"sub": me + to},
        )

    def first_copies(to):
        base = depth - planes * to
        lo, hi = max(base, depth - near), min(base + planes, depth + planes + near)
        out = [send_planes(fa, lo, hi, to, 0)]
        lo, hi = max(base, depth - near + 1), min(base + planes, depth + planes + near - 1)
        if hi > lo:
            out += [send_planes(buf, lo, hi, to, j + 1) for j, buf in enumerate((cx, vx, hx))]
        return out

    def rest_copies(to, which):
        base = depth - planes * to
        lo, hi = max(base, 1), min(base + planes, ext - 1)
        if to == 1:
            hi = min(hi, depth - near + 1)
        if to == -1:
            lo = max(lo, depth + planes + near - 1)
        if hi <= lo:
            return []
        return [send_planes((cx, vx, hx)[j], lo, hi, to, j + 4) for j in which]

    sides = ((-1, 1, lax.rem(me, 2) == 0), (1, -1, lax.rem(me, 2) == 1))
    assert reach == 2 and near == planes == 2 and n % 2 == 0

    def when(mine, d, act):
        @pl.when(jnp.logical_and(mine, there(d)))
        def _():
            act()

    def rest_each(which, act):
        for x, p, mine in sides:
            for d in (x, p, 2 * p):
                when(mine, d, lambda d=d: act(rest_copies(d, which)))

    def handed_rest(x, p):
        plane = depth - 1 if x < 0 else depth + planes
        return [
            rcopy(
                buf.at[pl.ds(plane, 1)],
                buf.at[pl.ds(plane - p * planes, 1)],
                set_send.at[j + 4, at[x - p]],
                set_recv.at[j + 4, at[x - p]],
                {"sub": me + p},
            )
            for j, buf in enumerate((cx, vx, hx))
        ]

    def handed_halo(par, x, p):
        return rcopy(
            land.at[par, at[x]],
            land.at[par, at[x - p]],
            halo_send.at[par, at[x - p]],
            halo_recv.at[par, at[x - p]],
            {"sub": me + p},
        )

    def surf_copies(to):
        return [
            rcopy(
                surf_all.at[reach],
                surf_all.at[reach - to],
                set_send.at[7, at[to]],
                set_recv.at[7, at[-to]],
                {"sub": me + to},
            )
        ]

    def mid_copy(to):
        return rcopy(
            fa.at[own],
            land.at[1, at[-to]],
            set_send.at[8, at[to]],
            set_recv.at[8, at[-to]],
            {"sub": me + to},
        )

    def each(ds, act):
        for d in ds:

            @pl.when(there(d))
            def _():
                act(d)

    def starts(copies):
        for c in copies:
            c.start()

    def arrivals(copies):
        for c in copies:
            c.wait_recv()

    def departures(copies):
        for c in copies:
            c.wait_send()

    beside = (-1, 1)
    each(beside, lambda d: starts(first_copies(d)))
    pass_on(0)

    partner = partner_ref[grp]
    count = count_ref[0, me]
    block_row = iota((blocks, LANES), 0)
    lane_row = iota((LANES, LANES), 0)

    def block_of(x):
        return lax.shift_right_logical(x, jnp.full(x.shape, LANES.bit_length() - 1, jnp.int32))

    def lane_of(x):
        return lax.bitwise_and(x, jnp.full(x.shape, LANES - 1, jnp.int32))

    def hot(mask):
        return jnp.where(mask, 1.0, 0.0).astype(F32)

    for c in loads[7:]:
        c.wait()
    for s in range(cap):
        lanes = pl.ds(s * LANES, LANES)
        oh_cent[:, lanes] = hot(lane_row == lane_of(cent_ref[s : s + 1, :])).astype(BF16)
        oh_targ[:, lanes] = hot(block_row == block_of(targ_ref[s : s + 1, :])).astype(BF16)
        hot_targ[lanes, :] = hot(lane_row == lane_of(targ_ref[s : s + 1, :])).T.astype(BF16)
        live = jnp.where(s < count, 1.0, 0.0).astype(F32)
        hi, lo = split((maps[s] * live).T)
        maps2[s, :, pl.ds(0, LANES)] = hi.astype(BF16)
        maps2[s, :, pl.ds(LANES, LANES)] = lo.astype(BF16)

    cell_row = iota((rows, surf_here), 0)

    def plane_of(cell):
        return sum((cell >= p * rows * LANES).astype(jnp.int32) for p in range(1, planes))

    def row_of(cell):
        return block_of(cell) - plane_of(cell) * rows

    def spot_of(cell):
        return plane_of(cell) * LANES + lane_of(cell)

    def hot_rows(j):
        oh_surf[j] = hot(cell_row == row_of(surf_all[j])).astype(BF16)
        spot = spot_of(surf_all[j])
        for i in range(half):
            cols = slice(i * LANES, (i + 1) * LANES)
            for p in range(planes):
                hot_surf[j, cols, pl.ds(p * LANES, LANES)] = hot(lane_row + p * LANES == spot[:, cols]).T.astype(BF16)

    hot_rows(reach)
    oh_lane[...] = hot(iota((planes * LANES, surf_here), 0) == spot_of(surf_all[reach])).astype(BF16)

    block_of_slot = iota((blocks, cap * LANES), 0)

    def gather_terms(zs):
        for z in zs:
            ax[z] = 1.0 - 6.0 * cx[z] - vx[z]
            bx[z] = cx[z] + vx[z]

    def step(src, dst, k):
        for z in range(k + 1, ext - k - 1):
            c = src[z]
            rest = hx[z] * (1.0 + jnp.tanh(c))
            dst[z] = ax[z] * c + cx[z] * (src[z + 1] + in_plane(c)) + (bx[z] * src[z - 1] + rest)

    def spread(slot, inc):
        lhs = []
        for x in split(inc):
            wide = [jnp.broadcast_to(x[i : i + 1, :], (16, LANES)).astype(BF16) for i in range(half)]
            wide = jnp.concatenate(wide, axis=1)
            lhs += [oh_surf[slot, r * 16 : (r + 1) * 16, :] * wide for r in range(rows // 16)]
        r = dot_nn(jnp.concatenate(lhs, axis=0), hot_surf[slot])
        r = r[:rows] + r[rows:]
        return [r[:, p * LANES : (p + 1) * LANES] for p in range(planes)]

    def halo_copy(par, to, slot):
        return rcopy(
            fa.at[own],
            land.at[par, at[slot]],
            halo_send.at[par, at[to]],
            halo_recv.at[par, at[slot]],
            {"sub": me + to},
        )

    upper = 2 * me >= n

    def ex_copy(two, par, k, peer, sender):
        src, dst = (exp_two, land_two.at[k - 1, sender]) if two else (exp_one, land_one.at[par, k - 1, sender])
        return rcopy(
            src,
            dst,
            ex_send.at[par, k - 1, peer],
            ex_recv.at[par, k - 1, sender],
            {"grp": lax.rem(grp + k, groups), "sub": peer},
        )

    def peers():
        return [lax.rem(me + jnp.where(upper, k, n - k), n) for k in range(1, n)]

    def rs_copy(two, par, peer, sender):
        if two:
            src, dst = part_two.at[peer], rs_two.at[sender]
        else:
            src, dst = part_one.at[pl.ds(peer, span)], rs_one.at[par, sender]
        return rcopy(src, dst, rs_send.at[par, peer], rs_recv.at[par, sender], {"sub": peer})

    def sample(values):
        lhs = []
        for x in values:
            lhs += split(jnp.concatenate(x, axis=1))
        got = dot_nn(jnp.concatenate(lhs, axis=0).astype(BF16), oh_lane[...])
        hit = cell_row == row_of(surf_all[reach])
        out = []
        for q in range(len(values)):
            v = got[2 * q * rows : (2 * q + 1) * rows] + got[(2 * q + 1) * rows : (2 * q + 2) * rows]
            out.append(jnp.sum(jnp.where(hit, v, 0.0), axis=0, keepdims=True))
        return out

    def patches(srcs):
        count_q = len(srcs)
        lhs = jnp.concatenate([x for v in srcs for x in split(v)], axis=0).astype(BF16)
        vals = dot_nn(lhs, oh_cent[...])
        cent = jnp.concatenate([cent_ref[s : s + 1, :] for s in range(cap)], axis=1)
        hit = block_of_slot == block_of(cent)
        cv = []
        for q in range(count_q):
            v = vals[2 * q * blocks : (2 * q + 1) * blocks] + vals[(2 * q + 1) * blocks : (2 * q + 2) * blocks]
            cv.append(jnp.sum(jnp.where(hit, v, 0.0), axis=0, keepdims=True))
        c4 = jnp.concatenate([x for v in cv for x in split(v)], axis=0).astype(BF16)
        contrib = []
        for s in range(cap):
            r = dot_nn(c4[:, s * LANES : (s + 1) * LANES], maps2[s])
            contrib.append(r[:, :LANES] + r[:, LANES:])
        r = jnp.concatenate(contrib, axis=1)
        rows_of = []
        for q in range(count_q):
            for x in split(r[2 * q : 2 * q + 1] + r[2 * q + 1 : 2 * q + 2]):
                wide = jnp.broadcast_to(x, (16, cap * LANES)).astype(BF16)
                rows_of += [oh_targ[b * 16 : (b + 1) * 16, :] * wide for b in range(blocks // 16)]
        acc = dot_nn(jnp.concatenate(rows_of, axis=0), hot_targ[...])
        return [
            acc[2 * q * blocks : (2 * q + 1) * blocks] + acc[(2 * q + 1) * blocks : (2 * q + 2) * blocks]
            for q in range(count_q)
        ]

    def advance():
        for k in range(STEPS):
            step(pair[k % 2], pair[(k + 1) % 2], k)

    def surface():
        temp = [fa[depth + p] for p in range(planes)]
        flux = [cx[depth + p] * (4.0 * t - in_plane(t)) for p, t in enumerate(temp)]
        return temp, flux

    def exchange(two, par):
        for j in range(n):
            peer = jnp.where(upper, j, n - 1 - j)
            for k in range(1, groups):
                ex_copy(two, par, k, peer, me).start()

    def chosen(two, par):
        for j in range(n):
            for k in range(1, groups):
                ex_copy(two, par, k, me, j).wait_recv()
        out = None
        for k in range(1, groups):
            got = land_two[k - 1] if two else land_one[par, k - 1]
            source = lax.rem(grp + groups - k, groups)
            out = got if out is None else jnp.where(partner == source, got, out)
        return out

    def finish(two, par):
        for j in range(n):
            for k in range(1, groups):
                ex_copy(two, par, k, j, me).wait_send()
        for peer in peers():
            rs_copy(two, par, peer, me).wait_send()

    def couple(it, carry):
        par = lax.rem(it, 2)
        first = it == 0

        @pl.when(jnp.logical_not(first))
        def _():
            advance()

        temp, flux = surface()
        mixed = sample([[away_t * t + away_f * f for t, f in zip(temp, flux)]])[0]
        for i in range(half):
            exp_one[i : i + 1, :] = mixed[:, i * LANES : (i + 1) * LANES]
        exchange(False, par)
        for x, p, mine in sides:
            for d in (x, p, 2 * p):
                when(mine, d, lambda d=d: halo_copy(par, d, -d).start())

        @pl.when(first)
        def _():
            rest_each((1,), starts)


        here = sample([temp])[0]
        for i in range(half):
            own_temp[i : i + 1, :] = here[:, i * LANES : (i + 1) * LANES]

        srcs = chosen(False, par)
        part = patches([srcs.reshape(blocks, LANES)])[0].reshape(n, half, LANES)
        mine = iota((n, half, LANES), 0) == me
        part_one[pl.ds(reach, n)] = part - jnp.where(mine, gain_t * own_temp[...], 0.0)
        for peer in peers():
            rs_copy(False, par, peer, me).start()
        for x, p, mine in sides:

            def hand_on(x=x, p=p):
                halo_copy(par, -x, x).wait_recv()
                handed_halo(par, x, p).start()

            when(mine, x, hand_on)

        @pl.when(first)
        def _():
            rest_each((2,), starts)

        rs_one[par, me] = part_one[pl.ds(me, span)]

        @pl.when(first)
        def _():
            each(offs, lambda d: arrivals(surf_copies(-d)))
            for d in offs:
                hot_rows(d + reach)

        for x, p, mine in sides:
            for d in (x, p, 2 * p):
                when(mine, d, lambda d=d: halo_copy(par, d, -d).wait_send())
            when(mine, x, lambda x=x, p=p: handed_halo(par, x, p).wait_send())
            for d in (p, 2 * p, 2 * x):
                when(mine, d, lambda d=d: halo_copy(par, -d, d).wait_recv())

        for peer in peers():
            rs_copy(False, par, me, peer).wait_recv()
        inc = rs_one[par, 0]
        for j in range(1, n):
            inc = inc + rs_one[par, j]
        sums = [spread(slot, inc[slot]) for slot in range(span)]
        for p in range(planes):
            fa[depth + p] = fa[depth + p] + sums[reach][p]
        for d in offs:
            for p in range(planes):
                fa[depth + planes * d + p] = land[par, at[d], p] + sums[d + reach][p]

        @pl.when(first)
        def _():
            each(offs, lambda d: arrivals(rest_copies(-d, (0, 1, 2))))
            gather_terms([z for z in range(1, ext - 1) if z not in close])
            each(offs, lambda d: departures(surf_copies(d)))
            rest_each((0, 1, 2), departures)
            for x, p, mine in sides:
                when(mine, x, lambda x=x, p=p: departures(handed_rest(x, p)))

        finish(False, par)
        return carry

    def final():
        par = (COUPLE - 1) % 2
        advance()
        got = sample(surface())
        for q in range(2):
            for i in range(half):
                exp_two[q * half + i : q * half + i + 1, :] = got[q][:, i * LANES : (i + 1) * LANES]
        exchange(True, par)
        src = chosen(True, par)
        parts = patches([src[:, q * half : (q + 1) * half].reshape(blocks, LANES) for q in range(2)])
        part_two[...] = jnp.concatenate([x.reshape(n, half, LANES) for x in parts], axis=1)
        for peer in peers():
            rs_copy(True, par, peer, me).start()
        rs_two[me] = part_two[me]
        for peer in peers():
            rs_copy(True, par, me, peer).wait_recv()
        iface = rs_two[0]
        for j in range(1, n):
            iface = iface + rs_two[j]
        iface_ref[...] = iface
        inc = gain_t * (iface[:half] - exp_two[:half]) + gain_f * iface[half:]
        for p, x in enumerate(spread(reach, inc)):
            out_ref[p] = fa[depth + p] + x
        finish(True, par)

    pair = (fa, fb)
    hear(0)
    for i in range(1, len(hops)):
        pass_on(i)
        if i < len(hops) - 1:
            hear(i)
    each(beside, lambda d: arrivals(first_copies(-d)))
    if len(hops) > 1:
        hear(len(hops) - 1)
    for k in range(1, groups):
        signal(ready.at[len(hops)], {"grp": lax.rem(grp + k, groups)})
    each(beside, lambda d: departures(first_copies(d)))
    close = range(depth - near + 1, depth + planes + near - 1)
    gather_terms(close)
    for k in range(near):
        step(pair[k % 2], pair[(k + 1) % 2], depth - near + k)
    each(beside, lambda d: mid_copy(d).start())
    each(offs, lambda d: starts(surf_copies(d)))
    rest_each((0,), starts)
    for x, p, mine in sides:
        when(mine, x, lambda x=x, p=p: starts(handed_rest(x, p)))
    each(beside, lambda d: mid_copy(-d).wait_recv())
    for d in beside:
        fa[pl.ds(depth + planes * d, planes)] = land[1, at[d]]
    each(beside, lambda d: mid_copy(d).wait_send())
    for k in range(near):
        step(pair[k % 2], pair[(k + 1) % 2], depth - near + k)

    pl.semaphore_wait(ready.at[len(hops)], groups - 1)
    lax.fori_loop(0, COUPLE - 1, couple, 0)
    final()


def unpack(planes_ref, rows_ref, out_ref, iface_ref):
    planes, rows, _ = planes_ref.shape
    half = rows_ref.shape[0] // 2
    for b in range(rows // 8):
        rws = []
        for p in range(planes):
            x = planes_ref[p, b * 8 : (b + 1) * 8, :]
            rws.append(jnp.concatenate([x[i : i + 1, :] for i in range(8)], axis=1))
        out_ref[0, :, b * 8 * LANES : (b + 1) * 8 * LANES] = jnp.concatenate(rws, axis=0)
    for q in range(2):
        for i in range(half):
            iface_ref[0, q : q + 1, i * LANES : (i + 1) * LANES] = rows_ref[q * half + i : q * half + i + 1, :]


def local_of(n, groups):
    def local(
        initial_field,
        conduct,
        velocity,
        heat_release,
        group_kind,
        partner,
        surface_cell,
        patch_count,
        patch_centres,
        patch_targets,
        patch_maps,
    ):
        _, planes, cells = initial_field.shape
        rows = cells // LANES
        surf_here = surface_cell.shape[1]
        cap = patch_centres.shape[1]
        reach = -(-STEPS // planes)
        ext = planes + 2 * reach * planes
        half = surf_here // LANES
        vmem = pl.BlockSpec(memory_space=pltpu.VMEM)
        dma = pltpu.SemaphoreType.DMA
        nd = 2 * reach
        scratch = [
            pltpu.VMEM((ext, rows, LANES), F32),
            pltpu.VMEM((ext, rows, LANES), F32),
            pltpu.VMEM((ext, rows, LANES), F32),
            pltpu.VMEM((ext, rows, LANES), F32),
            pltpu.VMEM((ext, rows, LANES), F32),
            pltpu.VMEM((2, nd, planes, rows, LANES), F32),
            pltpu.VMEM((nd + 1, 1, surf_here), jnp.int32),
            pltpu.VMEM((nd + 1, rows, surf_here), BF16),
            pltpu.VMEM((nd + 1, surf_here, planes * LANES), BF16),
            pltpu.VMEM((planes * LANES, surf_here), BF16),
            pltpu.VMEM((LANES, cap * LANES), BF16),
            pltpu.VMEM((n * half, cap * LANES), BF16),
            pltpu.VMEM((cap * LANES, LANES), BF16),
            pltpu.VMEM((cap, LANES, 2 * LANES), BF16),
            pltpu.VMEM((half, LANES), F32),
            pltpu.VMEM((2 * half, LANES), F32),
            pltpu.VMEM((half, LANES), F32),
            pltpu.VMEM((2, groups - 1, n, half, LANES), F32),
            pltpu.VMEM((groups - 1, n, 2 * half, LANES), F32),
            pltpu.VMEM((n + nd, half, LANES), F32),
            pltpu.VMEM((n, 2 * half, LANES), F32),
            pltpu.VMEM((2, n, nd + 1, half, LANES), F32),
            pltpu.VMEM((n, 2 * half, LANES), F32),
            dma((9, nd)),
            dma((9, nd)),
            dma((2, groups - 1, n)),
            dma((2, groups - 1, n)),
            dma((2, n)),
            dma((2, n)),
            dma((2, nd)),
            dma((2, nd)),
            pltpu.SMEM(group_kind.shape, jnp.int32),
            pltpu.SMEM(partner.shape, jnp.int32),
            pltpu.SMEM(patch_count.shape, jnp.int32),
            pltpu.VMEM((planes, cells), F32),
            pltpu.VMEM((planes, cells), F32),
            pltpu.VMEM((planes, cells), F32),
            pltpu.VMEM((planes, cells), F32),
            pltpu.VMEM((cap, LANES), jnp.int32),
            pltpu.VMEM((cap, LANES), jnp.int32),
            pltpu.VMEM((cap, LANES, LANES), F32),
            dma((11,)),
            pltpu.SemaphoreType.REGULAR((n.bit_length() + 1,)),
            pltpu.VMEM((ext, rows, LANES), F32),
            pltpu.VMEM((ext, rows, LANES), F32),
        ]

        def body(*refs):
            kernel(n, groups, *refs)

        lying, tops = pl.pallas_call(
            body,
            name="coupled",
            out_shape=(
                pltpu.VMEM((planes, rows, LANES), F32),
                pltpu.VMEM((2 * half, LANES), F32),
            ),
            in_specs=[pl.BlockSpec(memory_space=pltpu.HBM)] * 11,
            out_specs=(vmem, vmem),
            scratch_shapes=scratch,
            compiler_params=pltpu.CompilerParams(
                collective_id=0, has_side_effects=True, vmem_limit_bytes=56 * 1024 * 1024
            ),
        )(
            group_kind,
            partner,
            patch_count,
            initial_field,
            conduct,
            velocity,
            heat_release,
            surface_cell,
            patch_centres[0],
            patch_targets[0],
            patch_maps[0],
        )
        return pl.pallas_call(
            unpack,
            name="unpack",
            out_shape=(
                jax.ShapeDtypeStruct(initial_field.shape, F32),
                jax.ShapeDtypeStruct((1, 2, surf_here), F32),
            ),
            in_specs=[vmem] * 2,
            out_specs=(vmem, vmem),
        )(*(pltpu.with_memory_space_constraint(x, pltpu.VMEM) for x in (lying, tops)))

    return local


def solution(mesh):
    placed = (
        P("grp", "sub", None),
        P("grp", "sub", None),
        P("grp", "sub", None),
        P("grp", "sub", None),
        P(),
        P(),
        P("grp", "sub"),
        P("grp", None),
        P("grp", "sub", None),
        P("grp", "sub", None),
        P("grp", "sub", None, None),
    )
    return jax.shard_map(
        local_of(mesh.shape["sub"], mesh.shape["grp"]),
        mesh=mesh,
        in_specs=placed,
        out_specs=(P("grp", "sub", None), P("grp", None, "sub")),
        check_vma=False,
    )
```

```python
import jax
import jax.numpy as jnp
from jax import lax
from jax.experimental import pallas as pl
from jax.experimental.pallas import tpu as pltpu
from jax.sharding import PartitionSpec as P

STEPS = 4
COUPLE = 4
LANES = 128
F32 = jnp.float32
BF16 = jnp.bfloat16


def split(x):
    hi = x.astype(BF16).astype(F32)
    return hi, x - hi


def dot_nt(a, b):
    return lax.dot_general(a, b, (((1,), (1,)), ((), ())), preferred_element_type=F32)


def dot_nn(a, b):
    return lax.dot_general(a, b, (((1,), (0,)), ((), ())), preferred_element_type=F32)


def iota(shape, dim):
    return lax.broadcasted_iota(jnp.int32, shape, dim)


def in_plane(c):
    rows, cols = c.shape
    return (
        pltpu.roll(c, 1, 0)
        + pltpu.roll(c, rows - 1, 0)
        + pltpu.roll(c, 1, 1)
        + pltpu.roll(c, cols - 1, 1)
    )


def kernel(
    n,
    groups,
    kind_hbm,
    partner_hbm,
    count_hbm,
    field_hbm,
    cond_hbm,
    vel_hbm,
    heat_hbm,
    surf_hbm,
    cent_hbm,
    targ_hbm,
    maps_hbm,
    out_ref,
    iface_ref,
    fa,
    fb,
    cx,
    vx,
    hx,
    land,
    surf_all,
    oh_surf,
    hot_surf,
    oh_lane,
    oh_cent,
    oh_targ,
    hot_targ,
    maps2,
    exp_one,
    exp_two,
    own_temp,
    land_one,
    land_two,
    part_one,
    part_two,
    rs_one,
    rs_two,
    set_send,
    set_recv,
    ex_send,
    ex_recv,
    rs_send,
    rs_recv,
    halo_send,
    halo_recv,
    kind_ref,
    partner_ref,
    count_ref,
    field_ref,
    cond_ref,
    vel_ref,
    heat_ref,
    cent_ref,
    targ_ref,
    maps,
    load_sem,
    ready,
    ax,
    bx,
):
    planes = field_ref.shape[0]
    rows = fa.shape[1]
    near = STEPS // 2
    assert near % 2 == 0 and near <= planes
    surf_here = surf_all.shape[2]
    cap = cent_ref.shape[0]
    reach = -(-STEPS // planes)
    depth = reach * planes
    ext = planes + 2 * depth
    offs = [d for d in range(-reach, reach + 1) if d != 0]
    at = {d: i for i, d in enumerate(offs)}
    half = surf_here // LANES
    span = 2 * reach + 1
    blocks = n * half
    me = lax.axis_index("sub")
    grp = lax.axis_index("grp")

    def there(d):
        return jnp.logical_and(me + d >= 0, me + d < n)

    def rcopy(src, dst, ss, rs, dev):
        return pltpu.make_async_remote_copy(
            src_ref=src,
            dst_ref=dst,
            send_sem=ss,
            recv_sem=rs,
            device_id=dev,
            device_id_type=pl.DeviceIdType.MESH,
        )

    pairs = (
        (kind_hbm, kind_ref),
        (partner_hbm, partner_ref),
        (count_hbm, count_ref),
        (field_hbm.at[0], field_ref),
        (cond_hbm.at[0], cond_ref),
        (vel_hbm.at[0], vel_ref),
        (heat_hbm.at[0], heat_ref),
        (surf_hbm, surf_all.at[reach]),
        (cent_hbm, cent_ref),
        (targ_hbm, targ_ref),
        (maps_hbm, maps),
    )
    loads = [pltpu.make_async_copy(src, dst, load_sem.at[i]) for i, (src, dst) in enumerate(pairs)]
    for c in loads:
        c.start()

    def signal(sem, dev):
        pl.semaphore_signal(sem, inc=1, device_id=dev, device_id_type=pl.DeviceIdType.MESH)

    def among(ds):
        return sum(there(d).astype(jnp.int32) for d in ds)

    def tell(sem, ds):
        for d in ds:

            @pl.when(there(d))
            def _():
                signal(sem, {"sub": me + d})

    barrier = pltpu.get_barrier_semaphore()
    tell(barrier, offs)
    for k in range(1, groups):
        signal(barrier, {"grp": lax.rem(grp + k, groups)})
    hops = [reach]
    while 2 * hops[-1] < n:
        hops.append(2 * hops[-1])

    def hear(i):
        pl.semaphore_wait(ready.at[i], among((-hops[i], hops[i])))

    def pass_on(i):
        tell(ready.at[i], (-hops[i], hops[i]))

    for border in (pl.ds(0, reach), pl.ds(reach + n, reach)):
        part_one[border] = jnp.zeros((reach, half, LANES), F32)
    for d in offs:

        @pl.when(jnp.logical_not(there(d)))
        def _():
            for buf in (fa, cx, vx, hx):
                buf[pl.ds(depth + planes * d, planes)] = jnp.zeros((planes, rows, LANES), F32)
            for par in range(2):
                land[par, at[d]] = jnp.zeros((planes, rows, LANES), F32)
            surf_all[reach + d] = jnp.zeros((1, surf_here), jnp.int32)

    for c in loads[:7]:
        c.wait()
    own = pl.ds(depth, planes)
    kind = kind_ref[grp]
    gas = jnp.where(kind == 0, 1.0, 0.0).astype(F32)
    gain_t = jnp.where(kind == 0, 0.5, 0.25).astype(F32)
    gain_f = jnp.where(kind == 0, -0.25, 0.25).astype(F32)
    away_t = jnp.where(kind == 0, 0.25, 0.5).astype(F32)
    away_f = jnp.where(kind == 0, 0.25, -0.25).astype(F32)
    fetch = ((field_ref, fa, None), (cond_ref, cx, None), (vel_ref, vx, gas), (heat_ref, hx, 0.5 * gas))

    def unfold(b, carry):
        chunk = pl.ds(pl.multiple_of(b * 8 * LANES, LANES), 8 * LANES)
        for src, dst, scale in fetch:
            x = src[:, chunk]
            if scale is not None:
                x = x * scale
            for p in range(planes):
                dst[depth + p, pl.ds(pl.multiple_of(b * 8, 8), 8), :] = jnp.concatenate(
                    [x[p : p + 1, i * LANES : (i + 1) * LANES] for i in range(8)], axis=0
                )
        return carry

    lax.fori_loop(0, rows // 8, unfold, 0)
    pl.semaphore_wait(barrier, among(offs) + groups - 1)

    def send_planes(buf, lo, hi, to, j):
        slot = -to
        shift = depth - (depth + planes * slot)
        return rcopy(
            buf.at[pl.ds(lo + shift, hi - lo)],
            buf.at[pl.ds(lo, hi - lo)],
            set_send.at[j, at[to]],
            set_recv.at[j, at[slot]],
            {"sub": me + to},
        )

    def first_copies(to):
        base = depth - planes * to
        lo, hi = max(base, depth - near), min(base + planes, depth + planes + near)
        out = [send_planes(fa, lo, hi, to, 0)]
        lo, hi = max(base, depth - near + 1), min(base + planes, depth + planes + near - 1)
        if hi > lo:
            out += [send_planes(buf, lo, hi, to, j + 1) for j, buf in enumerate((cx, vx, hx))]
        return out

    def rest_copies(to, which):
        base = depth - planes * to
        lo, hi = max(base, 1), min(base + planes, ext - 1)
        if to == 1:
            hi = min(hi, depth - near + 1)
        if to == -1:
            lo = max(lo, depth + planes + near - 1)
        if hi <= lo:
            return []
        return [send_planes((cx, vx, hx)[j], lo, hi, to, j + 4) for j in which]

    sides = ((-1, 1, lax.rem(me, 2) == 0), (1, -1, lax.rem(me, 2) == 1))
    assert reach == 2 and near == planes == 2 and n % 2 == 0

    def when(mine, d, act):
        @pl.when(jnp.logical_and(mine, there(d)))
        def _():
            act()

    def rest_each(which, act):
        for x, p, mine in sides:
            for d in (x, p, 2 * p):
                when(mine, d, lambda d=d: act(rest_copies(d, which)))

    def handed_rest(x, p):
        plane = depth - 1 if x < 0 else depth + planes
        return [
            rcopy(
                buf.at[pl.ds(plane, 1)],
                buf.at[pl.ds(plane - p * planes, 1)],
                set_send.at[j + 4, at[x - p]],
                set_recv.at[j + 4, at[x - p]],
                {"sub": me + p},
            )
            for j, buf in enumerate((cx, vx, hx))
        ]

    def handed_halo(par, x, p):
        return rcopy(
            land.at[par, at[x]],
            land.at[par, at[x - p]],
            halo_send.at[par, at[x - p]],
            halo_recv.at[par, at[x - p]],
            {"sub": me + p},
        )

    def surf_copies(to):
        return [
            rcopy(
                surf_all.at[reach],
                surf_all.at[reach - to],
                set_send.at[7, at[to]],
                set_recv.at[7, at[-to]],
                {"sub": me + to},
            )
        ]

    def mid_copy(to):
        return rcopy(
            fa.at[own],
            land.at[1, at[-to]],
            set_send.at[8, at[to]],
            set_recv.at[8, at[-to]],
            {"sub": me + to},
        )

    def each(ds, act):
        for d in ds:

            @pl.when(there(d))
            def _():
                act(d)

    def starts(copies):
        for c in copies:
            c.start()

    def arrivals(copies):
        for c in copies:
            c.wait_recv()

    def departures(copies):
        for c in copies:
            c.wait_send()

    beside = (-1, 1)
    each(beside, lambda d: starts(first_copies(d)))
    pass_on(0)

    partner = partner_ref[grp]
    count = count_ref[0, me]
    block_row = iota((blocks, LANES), 0)
    lane_row = iota((LANES, LANES), 0)

    def block_of(x):
        return lax.shift_right_logical(x, jnp.full(x.shape, LANES.bit_length() - 1, jnp.int32))

    def lane_of(x):
        return lax.bitwise_and(x, jnp.full(x.shape, LANES - 1, jnp.int32))

    def hot(mask):
        return jnp.where(mask, 1.0, 0.0).astype(F32)

    for c in loads[7:]:
        c.wait()
    for s in range(cap):
        lanes = pl.ds(s * LANES, LANES)
        oh_cent[:, lanes] = hot(lane_row == lane_of(cent_ref[s : s + 1, :])).astype(BF16)
        oh_targ[:, lanes] = hot(block_row == block_of(targ_ref[s : s + 1, :])).astype(BF16)
        hot_targ[lanes, :] = hot(lane_row == lane_of(targ_ref[s : s + 1, :])).T.astype(BF16)
        live = jnp.where(s < count, 1.0, 0.0).astype(F32)
        hi, lo = split((maps[s] * live).T)
        maps2[s, :, pl.ds(0, LANES)] = hi.astype(BF16)
        maps2[s, :, pl.ds(LANES, LANES)] = lo.astype(BF16)

    cell_row = iota((rows, surf_here), 0)

    def plane_of(cell):
        return sum((cell >= p * rows * LANES).astype(jnp.int32) for p in range(1, planes))

    def row_of(cell):
        return block_of(cell) - plane_of(cell) * rows

    def spot_of(cell):
        return plane_of(cell) * LANES + lane_of(cell)

    def hot_rows(j):
        oh_surf[j] = hot(cell_row == row_of(surf_all[j])).astype(BF16)
        spot = spot_of(surf_all[j])
        for i in range(half):
            cols = slice(i * LANES, (i + 1) * LANES)
            for p in range(planes):
                hot_surf[j, cols, pl.ds(p * LANES, LANES)] = hot(lane_row + p * LANES == spot[:, cols]).T.astype(BF16)

    hot_rows(reach)
    oh_lane[...] = hot(iota((planes * LANES, surf_here), 0) == spot_of(surf_all[reach])).astype(BF16)

    block_of_slot = iota((blocks, cap * LANES), 0)

    def gather_terms(zs):
        for z in zs:
            ax[z] = 1.0 - 6.0 * cx[z] - vx[z]
            bx[z] = cx[z] + vx[z]

    def step(src, dst, k):
        for z in range(k + 1, ext - k - 1):
            c = src[z]
            rest = hx[z] * (1.0 + jnp.tanh(c))
            dst[z] = ax[z] * c + cx[z] * (src[z + 1] + in_plane(c)) + (bx[z] * src[z - 1] + rest)

    def spread(slot, inc):
        lhs = []
        for x in split(inc):
            wide = [jnp.broadcast_to(x[i : i + 1, :], (16, LANES)).astype(BF16) for i in range(half)]
            wide = jnp.concatenate(wide, axis=1)
            lhs += [oh_surf[slot, r * 16 : (r + 1) * 16, :] * wide for r in range(rows // 16)]
        r = dot_nn(jnp.concatenate(lhs, axis=0), hot_surf[slot])
        r = r[:rows] + r[rows:]
        return [r[:, p * LANES : (p + 1) * LANES] for p in range(planes)]

    def halo_copy(par, to, slot):
        return rcopy(
            fa.at[own],
            land.at[par, at[slot]],
            halo_send.at[par, at[to]],
            halo_recv.at[par, at[slot]],
            {"sub": me + to},
        )

    upper = 2 * me >= n

    def ex_copy(two, par, k, peer, sender):
        src, dst = (exp_two, land_two.at[k - 1, sender]) if two else (exp_one, land_one.at[par, k - 1, sender])
        return rcopy(
            src,
            dst,
            ex_send.at[par, k - 1, peer],
            ex_recv.at[par, k - 1, sender],
            {"grp": lax.rem(grp + k, groups), "sub": peer},
        )

    def peers():
        return [lax.rem(me + jnp.where(upper, k, n - k), n) for k in range(1, n)]

    def rs_copy(two, par, peer, sender):
        if two:
            src, dst = part_two.at[peer], rs_two.at[sender]
        else:
            src, dst = part_one.at[pl.ds(peer, span)], rs_one.at[par, sender]
        return rcopy(src, dst, rs_send.at[par, peer], rs_recv.at[par, sender], {"sub": peer})

    def sample(values):
        lhs = []
        for x in values:
            lhs += split(jnp.concatenate(x, axis=1))
        got = dot_nn(jnp.concatenate(lhs, axis=0).astype(BF16), oh_lane[...])
        hit = cell_row == row_of(surf_all[reach])
        out = []
        for q in range(len(values)):
            v = got[2 * q * rows : (2 * q + 1) * rows] + got[(2 * q + 1) * rows : (2 * q + 2) * rows]
            out.append(jnp.sum(jnp.where(hit, v, 0.0), axis=0, keepdims=True))
        return out

    def patches(srcs):
        count_q = len(srcs)
        lhs = jnp.concatenate([x for v in srcs for x in split(v)], axis=0).astype(BF16)
        vals = dot_nn(lhs, oh_cent[...])
        cent = jnp.concatenate([cent_ref[s : s + 1, :] for s in range(cap)], axis=1)
        hit = block_of_slot == block_of(cent)
        cv = []
        for q in range(count_q):
            v = vals[2 * q * blocks : (2 * q + 1) * blocks] + vals[(2 * q + 1) * blocks : (2 * q + 2) * blocks]
            cv.append(jnp.sum(jnp.where(hit, v, 0.0), axis=0, keepdims=True))
        c4 = jnp.concatenate([x for v in cv for x in split(v)], axis=0).astype(BF16)
        contrib = []
        for s in range(cap):
            r = dot_nn(c4[:, s * LANES : (s + 1) * LANES], maps2[s])
            contrib.append(r[:, :LANES] + r[:, LANES:])
        r = jnp.concatenate(contrib, axis=1)
        rows_of = []
        for q in range(count_q):
            for x in split(r[2 * q : 2 * q + 1] + r[2 * q + 1 : 2 * q + 2]):
                wide = jnp.broadcast_to(x, (16, cap * LANES)).astype(BF16)
                rows_of += [oh_targ[b * 16 : (b + 1) * 16, :] * wide for b in range(blocks // 16)]
        acc = dot_nn(jnp.concatenate(rows_of, axis=0), hot_targ[...])
        return [
            acc[2 * q * blocks : (2 * q + 1) * blocks] + acc[(2 * q + 1) * blocks : (2 * q + 2) * blocks]
            for q in range(count_q)
        ]

    def advance():
        for k in range(STEPS):
            step(pair[k % 2], pair[(k + 1) % 2], k)

    def surface():
        temp = [fa[depth + p] for p in range(planes)]
        flux = [cx[depth + p] * (4.0 * t - in_plane(t)) for p, t in enumerate(temp)]
        return temp, flux

    def exchange(two, par):
        for j in range(n):
            peer = jnp.where(upper, j, n - 1 - j)
            for k in range(1, groups):
                ex_copy(two, par, k, peer, me).start()

    def chosen(two, par):
        for j in range(n):
            for k in range(1, groups):
                ex_copy(two, par, k, me, j).wait_recv()
        out = None
        for k in range(1, groups):
            got = land_two[k - 1] if two else land_one[par, k - 1]
            source = lax.rem(grp + groups - k, groups)
            out = got if out is None else jnp.where(partner == source, got, out)
        return out

    def finish(two, par):
        for j in range(n):
            for k in range(1, groups):
                ex_copy(two, par, k, j, me).wait_send()
        for peer in peers():
            rs_copy(two, par, peer, me).wait_send()

    def couple(it, carry):
        par = lax.rem(it, 2)
        first = it == 0

        @pl.when(jnp.logical_not(first))
        def _():
            advance()

        temp, flux = surface()
        mixed = sample([[away_t * t + away_f * f for t, f in zip(temp, flux)]])[0]
        for i in range(half):
            exp_one[i : i + 1, :] = mixed[:, i * LANES : (i + 1) * LANES]
        exchange(False, par)
        for x, p, mine in sides:
            for d in (x, p, 2 * p):
                when(mine, d, lambda d=d: halo_copy(par, d, -d).start())

        @pl.when(first)
        def _():
            rest_each((1,), starts)


        here = sample([temp])[0]
        for i in range(half):
            own_temp[i : i + 1, :] = here[:, i * LANES : (i + 1) * LANES]

        srcs = chosen(False, par)
        part = patches([srcs.reshape(blocks, LANES)])[0].reshape(n, half, LANES)
        mine = iota((n, half, LANES), 0) == me
        part_one[pl.ds(reach, n)] = part - jnp.where(mine, gain_t * own_temp[...], 0.0)
        for peer in peers():
            rs_copy(False, par, peer, me).start()
        for x, p, mine in sides:

            def hand_on(x=x, p=p):
                halo_copy(par, -x, x).wait_recv()
                handed_halo(par, x, p).start()

            when(mine, x, hand_on)

        @pl.when(first)
        def _():
            rest_each((2,), starts)

        rs_one[par, me] = part_one[pl.ds(me, span)]

        @pl.when(first)
        def _():
            each(offs, lambda d: arrivals(surf_copies(-d)))
            for d in offs:
                hot_rows(d + reach)
            each(offs, lambda d: arrivals(rest_copies(-d, (0, 1))))
            gather_terms([z for z in range(1, ext - 1) if z not in close])

        for x, p, mine in sides:
            for d in (x, p, 2 * p):
                when(mine, d, lambda d=d: halo_copy(par, d, -d).wait_send())
            when(mine, x, lambda x=x, p=p: handed_halo(par, x, p).wait_send())
            for d in (p, 2 * p, 2 * x):
                when(mine, d, lambda d=d: halo_copy(par, -d, d).wait_recv())

        for peer in peers():
            rs_copy(False, par, me, peer).wait_recv()
        inc = rs_one[par, 0]
        for j in range(1, n):
            inc = inc + rs_one[par, j]
        sums = [spread(slot, inc[slot]) for slot in range(span)]
        for p in range(planes):
            fa[depth + p] = fa[depth + p] + sums[reach][p]
        for d in offs:
            for p in range(planes):
                fa[depth + planes * d + p] = land[par, at[d], p] + sums[d + reach][p]

        @pl.when(first)
        def _():
            each(offs, lambda d: arrivals(rest_copies(-d, (2,))))
            each(offs, lambda d: departures(surf_copies(d)))
            rest_each((0, 1, 2), departures)
            for x, p, mine in sides:
                when(mine, x, lambda x=x, p=p: departures(handed_rest(x, p)))

        finish(False, par)
        return carry

    def final():
        par = (COUPLE - 1) % 2
        advance()
        got = sample(surface())
        for q in range(2):
            for i in range(half):
                exp_two[q * half + i : q * half + i + 1, :] = got[q][:, i * LANES : (i + 1) * LANES]
        exchange(True, par)
        src = chosen(True, par)
        parts = patches([src[:, q * half : (q + 1) * half].reshape(blocks, LANES) for q in range(2)])
        part_two[...] = jnp.concatenate([x.reshape(n, half, LANES) for x in parts], axis=1)
        for peer in peers():
            rs_copy(True, par, peer, me).start()
        rs_two[me] = part_two[me]
        for peer in peers():
            rs_copy(True, par, me, peer).wait_recv()
        iface = rs_two[0]
        for j in range(1, n):
            iface = iface + rs_two[j]
        iface_ref[...] = iface
        inc = gain_t * (iface[:half] - exp_two[:half]) + gain_f * iface[half:]
        for p, x in enumerate(spread(reach, inc)):
            out_ref[p] = fa[depth + p] + x
        finish(True, par)

    pair = (fa, fb)
    hear(0)
    for i in range(1, len(hops)):
        pass_on(i)
        if i < len(hops) - 1:
            hear(i)
    each(beside, lambda d: arrivals(first_copies(-d)))
    if len(hops) > 1:
        hear(len(hops) - 1)
    for k in range(1, groups):
        signal(ready.at[len(hops)], {"grp": lax.rem(grp + k, groups)})
    each(beside, lambda d: departures(first_copies(d)))
    close = range(depth - near + 1, depth + planes + near - 1)
    gather_terms(close)
    for k in range(near):
        step(pair[k % 2], pair[(k + 1) % 2], depth - near + k)
    each(beside, lambda d: mid_copy(d).start())
    each(offs, lambda d: starts(surf_copies(d)))
    rest_each((0,), starts)
    for x, p, mine in sides:
        when(mine, x, lambda x=x, p=p: starts(handed_rest(x, p)))
    each(beside, lambda d: mid_copy(-d).wait_recv())
    for d in beside:
        fa[pl.ds(depth + planes * d, planes)] = land[1, at[d]]
    each(beside, lambda d: mid_copy(d).wait_send())
    for k in range(near):
        step(pair[k % 2], pair[(k + 1) % 2], depth - near + k)

    pl.semaphore_wait(ready.at[len(hops)], groups - 1)
    lax.fori_loop(0, COUPLE - 1, couple, 0)
    final()


def unpack(planes_ref, rows_ref, out_ref, iface_ref):
    planes, rows, _ = planes_ref.shape
    half = rows_ref.shape[0] // 2
    for b in range(rows // 8):
        rws = []
        for p in range(planes):
            x = planes_ref[p, b * 8 : (b + 1) * 8, :]
            rws.append(jnp.concatenate([x[i : i + 1, :] for i in range(8)], axis=1))
        out_ref[0, :, b * 8 * LANES : (b + 1) * 8 * LANES] = jnp.concatenate(rws, axis=0)
    for q in range(2):
        for i in range(half):
            iface_ref[0, q : q + 1, i * LANES : (i + 1) * LANES] = rows_ref[q * half + i : q * half + i + 1, :]


def local_of(n, groups):
    def local(
        initial_field,
        conduct,
        velocity,
        heat_release,
        group_kind,
        partner,
        surface_cell,
        patch_count,
        patch_centres,
        patch_targets,
        patch_maps,
    ):
        _, planes, cells = initial_field.shape
        rows = cells // LANES
        surf_here = surface_cell.shape[1]
        cap = patch_centres.shape[1]
        reach = -(-STEPS // planes)
        ext = planes + 2 * reach * planes
        half = surf_here // LANES
        vmem = pl.BlockSpec(memory_space=pltpu.VMEM)
        dma = pltpu.SemaphoreType.DMA
        nd = 2 * reach
        scratch = [
            pltpu.VMEM((ext, rows, LANES), F32),
            pltpu.VMEM((ext, rows, LANES), F32),
            pltpu.VMEM((ext, rows, LANES), F32),
            pltpu.VMEM((ext, rows, LANES), F32),
            pltpu.VMEM((ext, rows, LANES), F32),
            pltpu.VMEM((2, nd, planes, rows, LANES), F32),
            pltpu.VMEM((nd + 1, 1, surf_here), jnp.int32),
            pltpu.VMEM((nd + 1, rows, surf_here), BF16),
            pltpu.VMEM((nd + 1, surf_here, planes * LANES), BF16),
            pltpu.VMEM((planes * LANES, surf_here), BF16),
            pltpu.VMEM((LANES, cap * LANES), BF16),
            pltpu.VMEM((n * half, cap * LANES), BF16),
            pltpu.VMEM((cap * LANES, LANES), BF16),
            pltpu.VMEM((cap, LANES, 2 * LANES), BF16),
            pltpu.VMEM((half, LANES), F32),
            pltpu.VMEM((2 * half, LANES), F32),
            pltpu.VMEM((half, LANES), F32),
            pltpu.VMEM((2, groups - 1, n, half, LANES), F32),
            pltpu.VMEM((groups - 1, n, 2 * half, LANES), F32),
            pltpu.VMEM((n + nd, half, LANES), F32),
            pltpu.VMEM((n, 2 * half, LANES), F32),
            pltpu.VMEM((2, n, nd + 1, half, LANES), F32),
            pltpu.VMEM((n, 2 * half, LANES), F32),
            dma((9, nd)),
            dma((9, nd)),
            dma((2, groups - 1, n)),
            dma((2, groups - 1, n)),
            dma((2, n)),
            dma((2, n)),
            dma((2, nd)),
            dma((2, nd)),
            pltpu.SMEM(group_kind.shape, jnp.int32),
            pltpu.SMEM(partner.shape, jnp.int32),
            pltpu.SMEM(patch_count.shape, jnp.int32),
            pltpu.VMEM((planes, cells), F32),
            pltpu.VMEM((planes, cells), F32),
            pltpu.VMEM((planes, cells), F32),
            pltpu.VMEM((planes, cells), F32),
            pltpu.VMEM((cap, LANES), jnp.int32),
            pltpu.VMEM((cap, LANES), jnp.int32),
            pltpu.VMEM((cap, LANES, LANES), F32),
            dma((11,)),
            pltpu.SemaphoreType.REGULAR((n.bit_length() + 1,)),
            pltpu.VMEM((ext, rows, LANES), F32),
            pltpu.VMEM((ext, rows, LANES), F32),
        ]

        def body(*refs):
            kernel(n, groups, *refs)

        lying, tops = pl.pallas_call(
            body,
            name="coupled",
            out_shape=(
                pltpu.VMEM((planes, rows, LANES), F32),
                pltpu.VMEM((2 * half, LANES), F32),
            ),
            in_specs=[pl.BlockSpec(memory_space=pltpu.HBM)] * 11,
            out_specs=(vmem, vmem),
            scratch_shapes=scratch,
            compiler_params=pltpu.CompilerParams(
                collective_id=0, has_side_effects=True, vmem_limit_bytes=56 * 1024 * 1024
            ),
        )(
            group_kind,
            partner,
            patch_count,
            initial_field,
            conduct,
            velocity,
            heat_release,
            surface_cell,
            patch_centres[0],
            patch_targets[0],
            patch_maps[0],
        )
        return pl.pallas_call(
            unpack,
            name="unpack",
            out_shape=(
                jax.ShapeDtypeStruct(initial_field.shape, F32),
                jax.ShapeDtypeStruct((1, 2, surf_here), F32),
            ),
            in_specs=[vmem] * 2,
            out_specs=(vmem, vmem),
        )(*(pltpu.with_memory_space_constraint(x, pltpu.VMEM) for x in (lying, tops)))

    return local


def solution(mesh):
    placed = (
        P("grp", "sub", None),
        P("grp", "sub", None),
        P("grp", "sub", None),
        P("grp", "sub", None),
        P(),
        P(),
        P("grp", "sub"),
        P("grp", None),
        P("grp", "sub", None),
        P("grp", "sub", None),
        P("grp", "sub", None, None),
    )
    return jax.shard_map(
        local_of(mesh.shape["sub"], mesh.shape["grp"]),
        mesh=mesh,
        in_specs=placed,
        out_specs=(P("grp", "sub", None), P("grp", None, "sub")),
        check_vma=False,
    )
```
